128 devices in a mesh: az: 16 (over z, y), rg: 8 (over x, core).
Axes of the slice: x: 4, y: 4, z: 4, core: 2. Of those that a mesh axis runs over, the one named last changes fastest.
Arguments:
- ref_image: float32 [2048, 6144], P('az', 'rg'), may hold values from 0.2 to 5
- sec_image: float32 [2048, 6144], P('az', 'rg'), may hold values from 0.2 to 5
- off_az: int32 [32], P('az'), may hold values from -15 to 15, as said below
- off_rg: int32 [32], P('az'), may hold values from -15 to 15, as said below
Outputs:
- surfaces: float32 [32, 96, 128, 128], P('az', 'rg')
The draws below stay inside these ranges and needn't reach their ends.
Inputs may be any that keep to these rules, and one draw needn't show every extreme that they name: off_az is monotone over the chip rows, changes by 0 or 1 between neighbouring chip rows, and runs from one end of its range to the other. off_rg is monotone over the chip rows, changes by 0 or 1 between neighbouring chip rows, and runs from one end of its range to the other.
All inputs are finite; a program needn't handle non-finite values.
Results may differ from the reference program's by a relative error of at most 0.0003.
Values sent between devices are 32-bit elements; how exact they have to be, the bound alone decides.
A program may use at most 64 MiB of HBM per device.

```python
import math
import jax
import jax.numpy as jnp
from jax import lax

CHIP = 128
SPACE = 64
SEARCH = 192
LAGS = 64
A_DEV = 128
NA = 2048
NR = 6144
NKA = 32
OFFAZ = 15
OFFRG = 15


def monotone_path(key, count, reach):
    order = jax.random.permutation(key, count - 1)
    steps = (order < 2 * reach).astype(jnp.int32)
    path = jnp.concatenate([jnp.zeros((1,), jnp.int32), jnp.cumsum(steps).astype(jnp.int32)]) - reach
    flip = jax.random.randint(jax.random.fold_in(key, 5), (), 0, 2, dtype=jnp.int32)
    return jnp.where(flip == 1, -path, path).astype(jnp.int32)


def draw_off_az(key, part):
    return monotone_path(jax.random.fold_in(key, 11), NKA, OFFAZ)


def draw_off_rg(key, part):
    return monotone_path(jax.random.fold_in(key, 23), NKA, OFFRG)


def block_levels(rng, dims, split, least, largest):
    loudness = 1.0
    for position, shards_of in split:
        steps = jax.random.uniform(jax.random.fold_in(jax.random.fold_in(rng, 6), position), (shards_of,), jnp.float32, least / len(split), largest / len(split))
        loudness = loudness * jnp.repeat(jnp.exp(steps), dims[position] // shards_of).reshape((-1,) + (1,) * (len(dims) - 1 - position))
    return loudness


def setup_inputs(seed: int = 0) -> dict:
    keys = jax.random.split(jax.random.key(seed), 5)
    ref_image = jnp.clip(jnp.exp(math.log(5.0) - 3.218876 * jax.random.uniform(keys[0], (NA, NR), jnp.float32) ** block_levels(keys[0], (NA, NR), ((0, 16), (1, 8)), -0.2, 0.2)), 0.2, 5.0)
    sec_image = jnp.clip(jnp.exp(math.log(5.0) - 3.218876 * jax.random.uniform(keys[1], (NA, NR), jnp.float32) ** block_levels(keys[1], (NA, NR), ((0, 16), (1, 8)), -0.2, 0.2)), 0.2, 5.0)
    off_az = draw_off_az(jax.random.fold_in(keys[4], 71), 0)
    off_rg = draw_off_rg(jax.random.fold_in(keys[4], 71), 0)
    return {"ref_image": ref_image, "sec_image": sec_image, "off_az": off_az, "off_rg": off_rg}


EPSILON = 1e-06
HIGH = lax.Precision.HIGHEST

def box_matrix():
    lag_index = lax.iota(jnp.int32, LAGS)[:, None]
    cell_index = lax.iota(jnp.int32, SEARCH)[None, :]
    return ((cell_index >= lag_index) & (cell_index < lag_index + CHIP)).astype(jnp.float32)

def cubic_matrix():
    out_index = lax.iota(jnp.int32, 2 * LAGS)[:, None]
    sample = lax.iota(jnp.int32, LAGS)[None, :]
    base = out_index // 2

    def pick(where):
        return (jnp.clip(where, 0, LAGS - 1) == sample).astype(jnp.float32)
    even_part = pick(base)
    odd_part = (9.0 * (pick(base) + pick(base + 1)) - (pick(base - 1) + pick(base + 2))) / 16.0
    return jnp.where(out_index % 2 == 1, odd_part, even_part)

def cut_chips(band, count):
    blocks = band.reshape(band.shape[0], count + 1, SPACE)
    joined = jnp.concatenate([blocks[:, :-1], blocks[:, 1:]], axis=2)
    return jnp.transpose(joined, (1, 0, 2))

def cut_windows(band, count):
    blocks = band.reshape(band.shape[0], count + 2, SPACE)
    joined = jnp.concatenate([blocks[:, :-2], blocks[:, 1:-1], blocks[:, 2:]], axis=2)
    return jnp.transpose(joined, (1, 0, 2))

def finish(corr, centered, windows):
    box_sum = box_matrix()
    first = jnp.einsum('pr,nrs->nps', box_sum, windows, precision=HIGH)
    first = jnp.einsum('nps,qs->npq', first, box_sum, precision=HIGH)
    second = jnp.einsum('pr,nrs->nps', box_sum, windows * windows, precision=HIGH)
    second = jnp.einsum('nps,qs->npq', second, box_sum, precision=HIGH)
    area = float(CHIP * CHIP)
    var_sum = second - first * first / area
    energy = lax.optimization_barrier(jnp.sum(centered * centered, axis=(1, 2)))
    score = CHIP * (corr / area) / jnp.sqrt(energy[:, None, None] / area * (var_sum / area) + EPSILON)
    oversample = cubic_matrix()
    lifted = jnp.einsum('ap,npq->naq', oversample, score, precision=HIGH)
    return jnp.einsum('naq,bq->nab', lifted, oversample, precision=HIGH)

def reference(ref_image, sec_image, off_az, off_rg):
    quarter = CHIP // 4
    half_chip = CHIP // 2
    ref_pad = jnp.pad(ref_image, quarter)
    sec_pad = jnp.pad(sec_image, ((A_DEV, A_DEV), (CHIP, CHIP)))
    total_rows = ref_image.shape[0] // SPACE
    chip_cols = ref_image.shape[1] // SPACE

    def one_row(inputs):
        row_index, shift_az, shift_rg = inputs
        ref_band = lax.dynamic_slice_in_dim(ref_pad, row_index * SPACE, CHIP, 0)
        chips = cut_chips(ref_band, chip_cols)
        sec_rows = lax.dynamic_slice_in_dim(sec_pad, row_index * SPACE + shift_az - half_chip + A_DEV, SEARCH, 0)
        sec_band = lax.dynamic_slice_in_dim(sec_rows, shift_rg + half_chip, chip_cols * SPACE + CHIP, 1)
        windows = cut_windows(sec_band, chip_cols)
        centered = chips - lax.optimization_barrier(jnp.mean(chips, axis=(1, 2), keepdims=True))
        padded = jnp.pad(centered, ((0, 0), (0, SEARCH - CHIP), (0, SEARCH - CHIP)))
        spectrum = jnp.conj(jnp.fft.fft2(padded)) * jnp.fft.fft2(windows)
        corr = jnp.real(jnp.fft.ifft2(spectrum))[:, :LAGS, :LAGS]
        return finish(corr, centered, windows)
    row_list = lax.iota(jnp.int32, total_rows)
    return lax.map(one_row, (row_list, off_az, off_rg))
```

```python
import functools

import jax
import jax.numpy as jnp
import numpy as np
from jax import lax
from jax.experimental import pallas as pl
from jax.experimental.pallas import tpu as pltpu
from jax.sharding import PartitionSpec as P

CHIP = 128
SPACE = 64
LAGS = 64
AREA = float(CHIP * CHIP)
EPSILON = 1e-06
ROWS = 128
COLS = 768
CHIPS = COLS // SPACE
PAIRS = CHIPS // 2
BLOCKS = CHIPS + 2
ROW_HALO = 80
REF_HALO = 32
LANE = 128
F32 = jnp.float32
BF16 = jnp.bfloat16


def halves(table):
    high = table.astype(jnp.bfloat16)
    low = (table - high.astype(np.float64)).astype(jnp.bfloat16)
    return high, low


def row_tables():
    freq = np.arange(64)[:, None] + 0.5
    out = []
    for j in range(4):
        angle = 2 * np.pi * freq * (64 * j + np.arange(64))[None, :] / 128
        high, low = halves(np.concatenate([np.cos(angle), -np.sin(angle)], axis=0))
        out.append(np.concatenate([high, high, low], axis=1))
    return np.stack(out)


def column_tables():
    angle = 2 * np.pi * np.arange(64)[:, None] * np.arange(128)[None, :] / 128
    c, s = np.cos(angle), np.sin(angle)
    sign = np.where(np.arange(256) % 2 == 0, 1.0, -1.0)[None, :]
    even = np.concatenate([np.concatenate([c, -s], 1), np.concatenate([s, c], 1)], 0)
    odd = np.concatenate([np.concatenate([s, c], 1), np.concatenate([c, -s], 1)], 0) * sign
    out = []
    for table in (even, odd):
        high, low = halves(table)
        out.append(np.concatenate([high, high, low], axis=0))
    return np.stack(out)


def back_tables():
    angle = 2 * np.pi * np.arange(64)[:, None] * (np.arange(64)[None, :] + 0.5) / 128
    c, s = np.cos(angle), np.sin(angle)
    high, low = halves(np.concatenate([np.concatenate([c, -s], 1), np.concatenate([s, c], 1)], 0))
    rows = np.concatenate([high, high, low], axis=1)
    angle = 2 * np.pi * np.arange(128)[:, None] * np.arange(64)[None, :] / 128
    high, low = halves(np.concatenate([np.cos(angle), -np.sin(angle)], 0) * (2.0 / AREA))
    none = np.zeros_like(high)
    first = np.concatenate([high, none, low, none], axis=1)
    second = np.concatenate([none, high, none, low], axis=1)
    return rows, np.stack([first, second])


def box_tables():
    lower = (np.arange(64)[None, :] < np.arange(64)[:, None]).astype(np.float64)
    none = np.zeros_like(lower)
    rows = np.concatenate(
        [np.concatenate([lower, lower, none, none], 1), np.concatenate([none, none, lower, lower], 1)], 0
    )
    cell = np.arange(256)[:, None]
    lag = np.arange(128)[None, :]
    start = np.where(lag < 64, lag, lag - 64 + 64)
    columns = ((cell >= start) & (cell < start + 128)).astype(np.float64)
    return rows.astype(jnp.bfloat16), columns.astype(jnp.bfloat16)


def cubic_tables():
    table = np.zeros((128, 64))
    for m in range(64):
        table[2 * m, m] = 1.0
        for step, weight in ((0, 9.0), (1, 9.0), (-1, -1.0), (2, -1.0)):
            table[2 * m + 1, min(max(m + step, 0), 63)] += weight / 16.0
    left = np.concatenate([table, table], axis=1)
    none = np.zeros((64, 128))
    right = np.concatenate(
        [np.concatenate([table.T, none], 1), np.concatenate([none, table.T], 1)], axis=0
    )
    return left.astype(jnp.bfloat16), right.astype(jnp.bfloat16)


def split(x):
    high = x.astype(BF16)
    return high, (x - high.astype(F32)).astype(BF16)


def dot(a, b):
    return jnp.dot(a, b, preferred_element_type=F32)


def shifted(x, shift, width):
    lane = lax.broadcasted_iota(jnp.int32, (x.shape[0], LANE), 1)
    turned = [
        pltpu.roll(x[:, i : i + LANE], LANE - shift, axis=1) for i in range(0, width + LANE, LANE)
    ]
    keep = lane < LANE - shift
    return jnp.concatenate(
        [jnp.where(keep, a, b) for a, b in zip(turned[:-1], turned[1:])], axis=1
    )


def lowered(x, shift):
    turn = lax.rem(8 - shift, 8)
    row = lax.broadcasted_iota(jnp.int32, (8, x.shape[1]), 0)
    turned = [pltpu.roll(x[i : i + 8], turn, axis=0) for i in range(0, 200, 8)]
    keep = row < 8 - shift
    return jnp.concatenate([jnp.where(keep, a, b) for a, b in zip(turned[:-1], turned[1:])], axis=0)


def range_spectra(rows_out, col_ref):
    lane = lax.broadcasted_iota(jnp.int32, (64, LANE), 1)
    low_half = lane < 64
    even, odd = [], []
    for x in rows_out:
        for i in range(0, x.shape[1], LANE):
            re = x[:64, i : i + LANE]
            im = pltpu.roll(x[64:, i : i + LANE], 64, axis=1)
            even.append(jnp.where(low_half, re, im))
            odd.append(jnp.where(low_half, im, re))
    out = []
    for parity, parts in enumerate((even, odd)):
        high, low = split(jnp.concatenate(parts, axis=0))
        got = dot(jnp.concatenate([high, low], axis=1), col_ref[parity, :256])
        got = got + dot(high, col_ref[parity, 256:])
        out.append(got)
    count = rows_out[0].shape[1] // LANE
    result = []
    for a in range(len(rows_out)):
        blocks = []
        for i in range(count):
            at = (a * count + i) * 64
            blocks += [out[0][at : at + 64], out[1][at : at + 64]]
        result.append(blocks)
    return result


def azimuth_spectra(x, row_ref, first):
    high, low = split(x)
    out = []
    for j in range(3):
        at = slice(64 * j, 64 * j + 64)
        stack = jnp.concatenate([high[at], low[at], high[at]], axis=0)
        out.append(dot(row_ref[first + j], stack))
    return out


def kernel(
    off_az,
    off_rg,
    ref_ref,
    sec_ref,
    row_ref,
    col_ref,
    back_row_ref,
    back_col_ref,
    box_row_ref,
    box_col_ref,
    up_left_ref,
    up_right_ref,
    out_ref,
    quads,
    windows,
    boxes,
    stats,
    strips,
    staged,
    sem,
):
    ref_mean = jnp.mean(ref_ref[REF_HALO : REF_HALO + ROWS, LANE : LANE + COLS], keepdims=True)
    sec_mean = jnp.mean(sec_ref[ROW_HALO : ROW_HALO + ROWS, LANE : LANE + COLS], keepdims=True)

    def reference_group(lane, width):
        x = ref_ref[:, pl.ds(lane, width + LANE)]
        x = shifted(x, LANE - REF_HALO, width) - ref_mean
        square = x * x
        sums = [jnp.sum(x[64 * m : 64 * m + 64], axis=0, keepdims=True) for m in range(3)]
        squares = [jnp.sum(square[64 * m : 64 * m + 64], axis=0, keepdims=True) for m in range(3)]
        rows = [sums[0] + sums[1], squares[0] + squares[1], sums[1] + sums[2], squares[1] + squares[2]]
        stats[:, pl.ds(lane, width)] = jnp.concatenate(rows + rows, axis=0)
        spectra = range_spectra(azimuth_spectra(x, row_ref, 0), col_ref)
        for m in range(3):
            for i, value in enumerate(spectra[m]):
                quads[m, lane // 64 + i] = value

    def window_group(k, lane, width):
        start = ROW_HALO - 64 + 64 * k + off_az[k]
        base = pl.multiple_of(start // 8 * 8, 8)
        w = sec_ref[pl.ds(base, 200), pl.ds(lane, width + LANE)]
        w = lowered(shifted(w, 64 + off_rg[k], width), start - base) - sec_mean
        parts = azimuth_spectra(w, row_ref, k)
        spectra = range_spectra([parts[0] + parts[1], parts[1] + parts[2]], col_ref)
        for m in range(2):
            for i, value in enumerate(spectra[m]):
                windows[k, m, lane // 64 + i] = value
        square = w * w
        tops = [
            jnp.broadcast_to(jnp.sum(v[:128], axis=0, keepdims=True), (64, width)) for v in (w, square)
        ]
        steps = [split(v[128:] - v[:64]) for v in (w, square)]
        stack = jnp.concatenate([steps[0][0], steps[0][1], steps[1][0], steps[1][1]], axis=0)
        boxes[k, :, pl.ds(lane, width)] = dot(box_row_ref[...], stack) + jnp.concatenate(tops, axis=0)

    def strip(k, n):
        re, im = 0.0, 0.0
        for m in range(2):
            q = quads[k + m, n]
            x = windows[k, m, n] + windows[k, m, n + 1]
            qr, qi, xr, xi = q[:, :128], q[:, 128:], x[:, :128], x[:, 128:]
            re = re + (qr * xr + qi * xi)
            im = im + (qr * xi - qi * xr)
        return jnp.concatenate([re, im], axis=0)

    def finish_pair(k, s):
        left = strips[k]
        middle = strip(k, 2 * s + 1)
        right = strip(k, 2 * s + 2)
        strips[k] = right
        high, low = split(jnp.concatenate([left + middle, middle + right], axis=1))
        y = dot(back_row_ref[:, :256], jnp.concatenate([high, low], axis=0))
        y = y + dot(back_row_ref[:, 256:], high)
        corr = 0.0
        for i in range(2):
            one = jnp.concatenate([y[:64, LANE * i : LANE * i + LANE], y[64:, LANE * i : LANE * i + LANE]], axis=1)
            high, low = split(one)
            wide = dot(high, back_col_ref[i])
            corr = corr + (wide[:, :128] + wide[:, 128:]) + dot(low, back_col_ref[i, :, :128])
        lane = s * LANE if isinstance(s, int) else pl.multiple_of(s * LANE, LANE)
        high, low = split(boxes[k, :, pl.ds(lane, 256)])
        box = dot(high, box_col_ref[...]) + dot(low, box_col_ref[...])
        first, second = box[:64], box[64:]
        stat = stats[:, pl.ds(lane, 256)]
        place = lax.broadcasted_iota(jnp.int32, stat.shape, 1)
        a = jnp.sum(stat[:, :128], axis=1, keepdims=True)
        b = jnp.sum(jnp.where((place >= 64) & (place < 192), stat, 0.0), axis=1, keepdims=True)
        both = jnp.where(place[:, :128] < 64, a, b)
        total, power = both[2 * k : 2 * k + 1], both[2 * k + 1 : 2 * k + 2]
        mean = total / AREA
        energy = power - total * mean
        centered = corr - mean * first
        var_sum = jnp.maximum(second - first * first / AREA, 0.0)
        score = (CHIP / AREA) * centered * lax.rsqrt((energy / AREA) * (var_sum / AREA) + EPSILON)
        high, low = split(score)
        lifted = dot(up_left_ref[...], jnp.concatenate([high, low], axis=0))
        high, low = split(lifted)
        both = dot(high, up_right_ref[...]) + dot(low, up_right_ref[...])
        at = k * CHIPS + 2 * s
        staged[at] = both[:, :128]
        staged[at + 1] = both[:, 128:]
        pltpu.make_async_copy(staged.at[pl.ds(at, 2)], out_ref.at[pl.ds(at, 2)], sem).start()

    def group(g, carry):
        lane = pl.multiple_of(g * 256, 256)
        reference_group(lane, 256)
        for k in range(2):
            window_group(k, lane, 256)
        return carry

    lax.fori_loop(0, 3, group, 0)
    reference_group(768, 128)
    for k in range(2):
        window_group(k, 768, 128)

    for k in range(2):
        strips[k] = strip(k, 0)

    def pair(s, carry):
        for k in range(2):
            finish_pair(k, s)
        return carry

    lax.fori_loop(0, PAIRS, pair, 0)
    pltpu.make_async_copy(staged, out_ref, sem).wait()


def extended(value, sides):
    for axis, dim, width in sides:
        size, length = lax.axis_size(axis), value.shape[dim]
        up = [(i, i + 1) for i in range(size - 1)]
        down = [(j, i) for i, j in up]
        last = lax.slice_in_dim(value, length - width, length, axis=dim)
        leading = lax.slice_in_dim(value, 0, width, axis=dim)
        before = lax.ppermute(last, axis, up)
        after = lax.ppermute(leading, axis, down)
        value = jnp.concatenate([before, value, after], axis=dim)
    return value


def body(ref_image, sec_image, off_az, off_rg):
    ref_ext = extended(ref_image, (("az", 0, REF_HALO), ("rg", 1, LANE)))
    sec_ext = extended(sec_image, (("az", 0, ROW_HALO), ("rg", 1, LANE)))
    back_rows, back_cols = back_tables()
    box_rows, box_cols = box_tables()
    left, right = cubic_tables()
    tables = [row_tables(), column_tables(), back_rows, back_cols, box_rows, box_cols, left, right]
    vmem = pl.BlockSpec(memory_space=pltpu.VMEM)
    smem = pl.BlockSpec(memory_space=pltpu.SMEM)
    out = pl.pallas_call(
        kernel,
        out_shape=jax.ShapeDtypeStruct((2 * CHIPS, 128, 128), F32),
        in_specs=[smem, smem] + [vmem] * 10,
        out_specs=pl.BlockSpec(memory_space=pl.ANY),
        scratch_shapes=[
            pltpu.VMEM((3, BLOCKS, 64, 256), F32),
            pltpu.VMEM((2, 2, BLOCKS, 64, 256), F32),
            pltpu.VMEM((2, 128, BLOCKS * 64), F32),
            pltpu.VMEM((8, BLOCKS * 64), F32),
            pltpu.VMEM((2, 128, 128), F32),
            pltpu.VMEM((2 * CHIPS, 128, 128), F32),
            pltpu.SemaphoreType.DMA,
        ],
    )(off_az, off_rg, ref_ext, sec_ext, *[jnp.asarray(t) for t in tables])
    return out.reshape(2, CHIPS, 128, 128)


def solution(mesh):
    return jax.shard_map(
        body,
        mesh=mesh,
        in_specs=(P("az", "rg"), P("az", "rg"), P("az"), P("az")),
        out_specs=P("az", "rg", None, None),
        check_vma=False,
    )
```

```python
import functools

import jax
import jax.numpy as jnp
import numpy as np
from jax import lax
from jax.experimental import pallas as pl
from jax.experimental.pallas import tpu as pltpu
from jax.sharding import PartitionSpec as P

CHIP = 128
SPACE = 64
LAGS = 64
AREA = float(CHIP * CHIP)
EPSILON = 1e-06
ROWS = 128
COLS = 768
CHIPS = COLS // SPACE
PAIRS = CHIPS // 2
BLOCKS = CHIPS + 2
WIDE = BLOCKS * SPACE
ROW_HALO = 80
REF_HALO = 32
NEAR = 16
FAR = 64
REACH = 160
LANE = 128
MESH = pl.DeviceIdType.MESH
F32 = jnp.float32
BF16 = jnp.bfloat16


def halves(table):
    high = table.astype(jnp.bfloat16)
    low = (table - high.astype(np.float64)).astype(jnp.bfloat16)
    return high, low


def azimuth_table(first, count):
    angle = 2 * np.pi * (np.arange(64)[:, None] + 0.5) * (first + np.arange(count))[None, :] / 128
    high, low = halves(np.concatenate([np.cos(angle), -np.sin(angle)], axis=0))
    return np.concatenate([high, high, low], axis=1)


def box_table():
    cell = np.arange(256)[:, None]
    lag = np.arange(128)[None, :]
    return ((cell >= lag) & (cell < lag + 128)).astype(jnp.bfloat16)


def column_tables():
    angle = 2 * np.pi * np.arange(64)[:, None] * np.arange(128)[None, :] / 128
    c, s = np.cos(angle), np.sin(angle)
    sign = np.where(np.arange(256) % 2 == 0, 1.0, -1.0)[None, :]
    even = np.concatenate([np.concatenate([c, -s], 1), np.concatenate([s, c], 1)], 0)
    odd = np.concatenate([np.concatenate([s, c], 1), np.concatenate([c, -s], 1)], 0) * sign
    out = []
    for table in (even, odd):
        high, low = halves(table)
        out.append(np.concatenate([high, high, low], axis=0))
    return np.stack(out)


def back_tables():
    angle = 2 * np.pi * np.arange(64)[:, None] * (np.arange(64)[None, :] + 0.5) / 128
    c, s = np.cos(angle), np.sin(angle)
    high, low = halves(np.concatenate([np.concatenate([c, -s], 1), np.concatenate([s, c], 1)], 0))
    rows = np.concatenate([high, high, low], axis=1)
    angle = 2 * np.pi * np.arange(128)[:, None] * np.arange(64)[None, :] / 128
    high, low = halves(np.concatenate([np.cos(angle), -np.sin(angle)], 0) * (2.0 / AREA))
    none = np.zeros_like(high)
    first = np.concatenate([high, none, low, none], axis=1)
    second = np.concatenate([none, high, none, low], axis=1)
    return rows, np.stack([first, second])


def cubic_tables():
    table = np.zeros((128, 64))
    for m in range(64):
        table[2 * m, m] = 1.0
        for step, weight in ((0, 9.0), (1, 9.0), (-1, -1.0), (2, -1.0)):
            table[2 * m + 1, min(max(m + step, 0), 63)] += weight / 16.0
    left = np.concatenate([table, table], axis=1)
    none = np.zeros((64, 128))
    right = np.concatenate(
        [np.concatenate([table.T, none], 1), np.concatenate([none, table.T], 1)], axis=0
    )
    return left.astype(jnp.bfloat16), right.astype(jnp.bfloat16)


def split(x):
    high = x.astype(BF16)
    return high, (x - high.astype(F32)).astype(BF16)


def dot(a, b):
    return jnp.dot(a, b, preferred_element_type=F32)


def shifted(x, shift, width):
    lane = lax.broadcasted_iota(jnp.int32, (x.shape[0], LANE), 1)
    turned = [
        pltpu.roll(x[:, i : i + LANE], LANE - shift, axis=1) for i in range(0, width + LANE, LANE)
    ]
    keep = lane < LANE - shift
    return jnp.concatenate(
        [jnp.where(keep, a, b) for a, b in zip(turned[:-1], turned[1:])], axis=1
    )


def range_spectra(rows_out, col_ref):
    lane = lax.broadcasted_iota(jnp.int32, (64, LANE), 1)
    low_half = lane < 64
    even, odd = [], []
    for x in rows_out:
        for i in range(0, x.shape[1], LANE):
            re = x[:64, i : i + LANE]
            im = pltpu.roll(x[64:, i : i + LANE], 64, axis=1)
            even.append(jnp.where(low_half, re, im))
            odd.append(jnp.where(low_half, im, re))
    out = []
    for parity, parts in enumerate((even, odd)):
        high, low = split(jnp.concatenate(parts, axis=0))
        got = dot(jnp.concatenate([high, low], axis=1), col_ref[parity, :256])
        got = got + dot(high, col_ref[parity, 256:])
        out.append(got)
    count = rows_out[0].shape[1] // LANE
    result = []
    for a in range(len(rows_out)):
        blocks = []
        for i in range(count):
            at = (a * count + i) * 64
            blocks += [out[0][at : at + 64], out[1][at : at + 64]]
        result.append(blocks)
    return result


def ones_where(condition):
    return jnp.where(condition, 1.0, 0.0).astype(BF16)


class Exchange:
    def __init__(self, tiles, bufs, tile_sems, send_sems, recv_sems):
        az, rg = lax.axis_index("az"), lax.axis_index("rg")
        last_az, last_rg = lax.axis_size("az") - 1, lax.axis_size("rg") - 1
        self.up = ("az", az - 1, az > 0)
        self.down = ("az", az + 1, az < last_az)
        self.left = ("rg", rg - 1, rg > 0)
        self.right = ("rg", rg + 1, rg < last_rg)
        self.sides = (self.up, self.down, self.left, self.right)
        self.bufs, self.send_sems, self.recv_sems, self.count = bufs, send_sems, recv_sems, 0
        self.all = []
        self.loads = []
        for i, (tile, (buf, halo)) in enumerate(zip(tiles, bufs)):
            own = buf.at[pl.ds(halo, ROWS), pl.ds(LANE, COLS)]
            self.loads.append(pltpu.make_async_copy(tile, own, tile_sems.at[i]))

    def greet(self):
        for load in self.loads:
            load.start()
        barrier = pltpu.get_barrier_semaphore()
        for axis, place, there in self.sides:

            @pl.when(there)
            def _(axis=axis, place=place):
                pl.semaphore_signal(barrier, inc=1, device_id={axis: place}, device_id_type=MESH)

    def clear(self):
        up, down, left, right = self.sides
        for buf, halo in self.bufs:
            for side, rows, lanes in (
                (up, slice(0, halo), slice(None)),
                (down, slice(halo + ROWS, 2 * halo + ROWS), slice(None)),
                (left, slice(None), slice(0, LANE)),
                (right, slice(None), slice(LANE + COLS, 2 * LANE + COLS)),
            ):

                @pl.when(jnp.logical_not(side[2]))
                def _(buf=buf, rows=rows, lanes=lanes):
                    shape = [n if c == slice(None) else c.stop - c.start for n, c in zip(buf.shape, (rows, lanes))]
                    buf[rows, lanes] = jnp.zeros(shape, F32)

    def meet(self):
        barrier = pltpu.get_barrier_semaphore()
        peers = sum(there.astype(jnp.int32) for _, _, there in self.sides)
        pl.semaphore_wait(barrier, peers)

    def copy(self, buf, rows, lanes, to_rows, to_lanes, side, back, have=None):
        index = self.count
        self.count += 1
        axis, place, sends = side
        comes = back[2]
        if have is not None:
            sends, comes = sends & have, comes & have
        transfer = pltpu.make_async_remote_copy(
            src_ref=buf.at[pl.ds(*rows), pl.ds(*lanes)],
            dst_ref=buf.at[pl.ds(*to_rows), pl.ds(*to_lanes)],
            send_sem=self.send_sems.at[index],
            recv_sem=self.recv_sems.at[index],
            device_id={axis: place},
            device_id_type=MESH,
        )
        entry = (transfer, sends, comes)
        self.all.append(entry)
        return entry

    def along_azimuth(self, buf, halo, near, far, lanes):
        count = far - near
        end = halo + ROWS
        return [
            self.copy(buf, (halo + near, count), lanes, (end + near, count), lanes, self.up, self.down),
            self.copy(buf, (end - far, count), lanes, (halo - far, count), lanes, self.down, self.up),
        ]

    def along_range(self, buf, rows, have=None):
        return [
            self.copy(buf, rows, (LANE, LANE), rows, (LANE + COLS, LANE), self.left, self.right, have),
            self.copy(buf, rows, (COLS, LANE), rows, (0, LANE), self.right, self.left, have),
        ]

    def corners(self, buf, halo, near, far):
        count = far - near
        return self.along_range(buf, (halo - far, count), self.up[2]) + self.along_range(
            buf, (halo + ROWS + near, count), self.down[2]
        )

    @staticmethod
    def start(entries):
        for transfer, sends, _ in entries:

            @pl.when(sends)
            def _(transfer=transfer):
                transfer.start()

    @staticmethod
    def arrive(entries):
        for transfer, _, comes in entries:

            @pl.when(comes)
            def _(transfer=transfer):
                transfer.wait_recv()

    def close(self):
        for transfer, sends, _ in self.all:

            @pl.when(sends)
            def _(transfer=transfer):
                transfer.wait_send()


def kernel(
    off_az,
    off_rg,
    ref_tile,
    sec_tile,
    ref_row_ref,
    sec_row_ref,
    col_ref,
    back_row_ref,
    back_col_ref,
    box_col_ref,
    up_left_ref,
    up_right_ref,
    out_ref,
    ref_buf,
    sec_buf,
    row_mats,
    box_mid,
    box_far,
    sec_high,
    sec_low,
    quads,
    windows,
    boxes,
    stats,
    strips,
    staged,
    sem,
    tile_sems,
    send_sems,
    recv_sems,
):
    halo = Exchange(
        (ref_tile, sec_tile),
        ((ref_buf, REF_HALO), (sec_buf, ROW_HALO)),
        tile_sems,
        send_sems,
        recv_sems,
    )
    everything = (LANE, COLS)
    near = halo.along_azimuth(sec_buf, ROW_HALO, 0, NEAR, everything)
    beside = halo.along_range(sec_buf, (ROW_HALO, ROWS)) + halo.along_range(ref_buf, (REF_HALO, ROWS))
    far = {}
    order = (1, 6, 2, 5, 3, 4)
    for b in order:
        lanes = (LANE * b, LANE)
        far[b] = halo.along_azimuth(sec_buf, ROW_HALO, NEAR, ROW_HALO, lanes)
        far[b] += halo.along_azimuth(ref_buf, REF_HALO, 0, REF_HALO, lanes)
    near_corners = halo.corners(sec_buf, ROW_HALO, 0, NEAR)
    far_corners = halo.corners(sec_buf, ROW_HALO, NEAR, ROW_HALO)
    far_corners += halo.corners(ref_buf, REF_HALO, 0, REF_HALO)

    halo.greet()
    halo.clear()
    for k in range(2):
        first = NEAR + off_az[k]
        at = lax.broadcasted_iota(jnp.int32, (384, 3 * REACH), 0)
        to = lax.broadcasted_iota(jnp.int32, (384, 3 * REACH), 1)
        at = at + (at // 128) * (REACH - 128)
        move = ones_where(to == at + first)
        for m in range(2):
            row_mats[k, m] = dot(sec_row_ref[k + m], move).astype(BF16)
        lag = lax.broadcasted_iota(jnp.int32, (64, 2 * REACH), 0)
        cell = lax.broadcasted_iota(jnp.int32, (64, 2 * REACH), 1)
        cell = jnp.where(cell < REACH, cell, cell - REACH) + (64 - 64 * k) - first - lag
        box_mid[k] = ones_where((cell >= 0) & (cell < CHIP))
        lag = lax.broadcasted_iota(jnp.int32, (64, 2 * FAR), 0)
        cell = lax.broadcasted_iota(jnp.int32, (64, 2 * FAR), 1)
        cell = jnp.where(cell < FAR, cell, cell - FAR) + REACH * k - first - lag
        box_far[k] = ones_where((cell >= 0) & (cell < CHIP))

    for load in halo.loads:
        load.wait()
    halo.meet()
    halo.start(near)
    halo.start(beside)
    for b in order:
        halo.start(far[b])

    own = pl.ds(LANE, COLS)
    ref_mean = jnp.mean(ref_buf[pl.ds(REF_HALO, ROWS), own], keepdims=True)
    sec_mean = jnp.mean(sec_buf[pl.ds(ROW_HALO, ROWS), own], keepdims=True)

    def reference_lines(m, pairs):
        parts = [ref_buf[64 * m : 64 * m + 64, LANE * p : LANE * p + 256] for p in pairs]
        parts = [shifted(x, LANE - REF_HALO, LANE) - ref_mean for x in parts]
        for p, x in zip(pairs, parts):
            place = pl.ds(LANE * p, LANE)
            stats[2 * m : 2 * m + 1, place] = jnp.sum(x, axis=0, keepdims=True)
            stats[2 * m + 1 : 2 * m + 2, place] = jnp.sum(x * x, axis=0, keepdims=True)
        high, low = split(jnp.concatenate(parts, axis=1))
        return dot(ref_row_ref[m], jnp.concatenate([high, low, high], axis=0))

    def window_lines(k, first, count, pairs, box_ref):
        parts = [sec_buf[first : first + count, LANE * p : LANE * p + 256] for p in pairs]
        parts = [shifted(x, 64 + off_rg[k], LANE) - sec_mean for x in parts]
        sums = []
        for p, x in zip(pairs, parts):
            high, low = split(x)
            square_high, square_low = split(x * x)
            place = pl.ds(LANE * p, LANE)
            sec_high[k, first : first + count, place] = high
            sec_low[k, first : first + count, place] = low
            stack = jnp.concatenate(
                [
                    jnp.concatenate([high, square_high], axis=1),
                    jnp.concatenate([low, square_low], axis=1),
                ],
                axis=0,
            )
            sums.append(dot(box_ref[k], stack))
        return sums

    def window_transform(k, m, pairs):
        rows = slice(64 * (k + m), 64 * (k + m) + REACH)
        high = jnp.concatenate([sec_high[k, rows, LANE * p : LANE * p + LANE] for p in pairs], axis=1)
        low = jnp.concatenate([sec_low[k, rows, LANE * p : LANE * p + LANE] for p in pairs], axis=1)
        return dot(row_mats[k, m], jnp.concatenate([high, low, high], axis=0))

    def store(target, pairs, blocks):
        for i, p in enumerate(pairs):
            for half in range(2):
                target[2 * p + half] = blocks[2 * i + half]

    def middle(pairs):
        rows_out = [reference_lines(1, pairs)]
        for k in range(2):
            for p, sums in zip(pairs, window_lines(k, 64, REACH, pairs, box_mid)):
                boxes[k, :64, pl.ds(LANE * p, LANE)] = sums[:, :128]
                boxes[k, 64:, pl.ds(LANE * p, LANE)] = sums[:, 128:]
            rows_out.append(window_transform(k, 1 - k, pairs))
        got = range_spectra(rows_out, col_ref)
        store(quads.at[1], pairs, got[0])
        store(windows.at[0, 1], pairs, got[1])
        store(windows.at[1, 0], pairs, got[2])

    def outer(pairs):
        for k in range(2):
            rows_out = [reference_lines(2 * k, pairs)]
            for p, sums in zip(pairs, window_lines(k, 224 * k, FAR, pairs, box_far)):
                boxes[k, :64, pl.ds(LANE * p, LANE)] += sums[:, :128]
                boxes[k, 64:, pl.ds(LANE * p, LANE)] += sums[:, 128:]
            rows_out.append(window_transform(k, k, pairs))
            got = range_spectra(rows_out, col_ref)
            store(quads.at[2 * k], pairs, got[0])
            store(windows.at[k, k], pairs, got[1])

    def strip(k, n):
        re, im = 0.0, 0.0
        for m in range(2):
            q = quads[k + m, n]
            x = windows[k, m, n] + windows[k, m, n + 1]
            qr, qi, xr, xi = q[:, :128], q[:, 128:], x[:, :128], x[:, 128:]
            re = re + (qr * xr + qi * xi)
            im = im + (qr * xi - qi * xr)
        return jnp.concatenate([re, im], axis=0)

    def finish(s):
        lane = s * LANE
        stat = stats[:, lane : lane + 256]
        place = lax.broadcasted_iota(jnp.int32, stat.shape, 1)
        a = jnp.sum(stat[:, :128], axis=1, keepdims=True)
        b = jnp.sum(jnp.where((place >= 64) & (place < 192), stat, 0.0), axis=1, keepdims=True)
        both = jnp.where(place[:, :128] < 64, a, b)
        for k in range(2):
            left, middle_, right = [strip(k, 2 * s + i) for i in range(3)]
            high, low = split(jnp.concatenate([left + middle_, middle_ + right], axis=1))
            y = dot(back_row_ref[:, :256], jnp.concatenate([high, low], axis=0))
            y = y + dot(back_row_ref[:, 256:], high)
            corr = 0.0
            for i in range(2):
                lanes = slice(LANE * i, LANE * i + LANE)
                high, low = split(jnp.concatenate([y[:64, lanes], y[64:, lanes]], axis=1))
                wide = dot(high, back_col_ref[i])
                corr = corr + (wide[:, :128] + wide[:, 128:]) + dot(low, back_col_ref[i, :, :128])
            high, low = split(boxes[k, :, lane : lane + 256])
            box = dot(high, box_col_ref[...]) + dot(low, box_col_ref[...])
            first, second = box[:64], box[64:]
            total = both[2 * k : 2 * k + 1] + both[2 * k + 2 : 2 * k + 3]
            power = both[2 * k + 1 : 2 * k + 2] + both[2 * k + 3 : 2 * k + 4]
            mean = total / AREA
            energy = power - total * mean
            centered = corr - mean * first
            var_sum = jnp.maximum(second - first * first / AREA, 0.0)
            score = (CHIP / AREA) * centered * lax.rsqrt((energy / AREA) * (var_sum / AREA) + EPSILON)
            high, low = split(score)
            lifted = dot(up_left_ref[...], jnp.concatenate([high, low], axis=0))
            high, low = split(lifted)
            wide = dot(high, up_right_ref[...]) + dot(low, up_right_ref[...])
            at = k * CHIPS + 2 * s
            staged[at] = wide[:, :128]
            staged[at + 1] = wide[:, 128:]
            pltpu.make_async_copy(staged.at[pl.ds(at, 2)], out_ref.at[pl.ds(at, 2)], sem).start()

    halo.arrive(near)
    halo.start(near_corners)
    middle((1, 2))
    middle((3, 4))
    halo.arrive(far[1] + far[6])
    halo.start(far_corners)
    middle((5,))
    halo.arrive(beside + near_corners)
    middle((0, 6))
    halo.arrive(far[2] + far[5])
    outer((1, 5))
    halo.arrive(far_corners)
    outer((0, 6))
    finish(0)
    finish(5)
    halo.arrive(far[3] + far[4])
    outer((2,))
    finish(1)
    outer((3, 4))
    finish(2)
    finish(3)
    finish(4)
    halo.close()
    pltpu.make_async_copy(staged, out_ref, sem).wait()


def body(ref_image, sec_image, off_az, off_rg):
    back_rows, back_cols = back_tables()
    left, right = cubic_tables()
    tables = [
        np.stack([azimuth_table(64 * m, 64) for m in range(3)]),
        np.stack([azimuth_table(64 * j, 128) for j in range(3)]),
        column_tables(),
        back_rows,
        back_cols,
        box_table(),
        left,
        right,
    ]
    vmem = pl.BlockSpec(memory_space=pltpu.VMEM)
    smem = pl.BlockSpec(memory_space=pltpu.SMEM)
    out = pl.pallas_call(
        kernel,
        out_shape=jax.ShapeDtypeStruct((2 * CHIPS, 128, 128), F32),
        in_specs=[smem, smem] + [pl.BlockSpec(memory_space=pl.ANY)] * 2 + [vmem] * len(tables),
        out_specs=pl.BlockSpec(memory_space=pl.ANY),
        scratch_shapes=[
            pltpu.VMEM((ROWS + 2 * REF_HALO, COLS + 2 * LANE), F32),
            pltpu.VMEM((ROWS + 2 * ROW_HALO, COLS + 2 * LANE), F32),
            pltpu.VMEM((2, 2, 128, 3 * REACH), BF16),
            pltpu.VMEM((2, 64, 2 * REACH), BF16),
            pltpu.VMEM((2, 64, 2 * FAR), BF16),
            pltpu.VMEM((2, ROWS + 2 * ROW_HALO, WIDE), BF16),
            pltpu.VMEM((2, ROWS + 2 * ROW_HALO, WIDE), BF16),
            pltpu.VMEM((3, BLOCKS, 64, 256), F32),
            pltpu.VMEM((2, 2, BLOCKS, 64, 256), F32),
            pltpu.VMEM((2, 128, WIDE), F32),
            pltpu.VMEM((8, WIDE), F32),
            pltpu.VMEM((2, 128, 128), F32),
            pltpu.VMEM((2 * CHIPS, 128, 128), F32),
            pltpu.SemaphoreType.DMA,
            pltpu.SemaphoreType.DMA((2,)),
            pltpu.SemaphoreType.DMA((48,)),
            pltpu.SemaphoreType.DMA((48,)),
        ],
        compiler_params=pltpu.CompilerParams(collective_id=0, has_side_effects=True),
    )(off_az, off_rg, ref_image, sec_image, *[jnp.asarray(t) for t in tables])
    return out.reshape(2, CHIPS, 128, 128)


def solution(mesh):
    return jax.shard_map(
        body,
        mesh=mesh,
        in_specs=(P("az", "rg"), P("az", "rg"), P("az"), P("az")),
        out_specs=P("az", "rg", None, None),
        check_vma=False,
    )
```

```python
import functools

import jax
import jax.numpy as jnp
import numpy as np
from jax import lax
from jax.experimental import pallas as pl
from jax.experimental.pallas import tpu as pltpu
from jax.sharding import PartitionSpec as P

CHIP = 128
SPACE = 64
LAGS = 64
AREA = float(CHIP * CHIP)
EPSILON = 1e-06
ROWS = 128
COLS = 768
CHIPS = COLS // SPACE
PAIRS = CHIPS // 2
BLOCKS = CHIPS + 2
WIDE = BLOCKS * SPACE
ROW_HALO = 80
REF_HALO = 32
NEAR = 16
FAR = 64
REACH = 160
LANE = 128
MESH = pl.DeviceIdType.MESH
F32 = jnp.float32
BF16 = jnp.bfloat16


def halves(table):
    high = table.astype(jnp.bfloat16)
    low = (table - high.astype(np.float64)).astype(jnp.bfloat16)
    return high, low


def azimuth_table(first, count):
    angle = 2 * np.pi * (np.arange(64)[:, None] + 0.5) * (first + np.arange(count))[None, :] / 128
    high, low = halves(np.concatenate([np.cos(angle), -np.sin(angle)], axis=0))
    return np.concatenate([high, high, low], axis=1)


def box_table():
    cell = np.arange(256)[:, None]
    lag = np.arange(128)[None, :]
    return ((cell >= lag) & (cell < lag + 128)).astype(jnp.bfloat16)


def column_tables():
    angle = 2 * np.pi * np.arange(64)[:, None] * np.arange(128)[None, :] / 128
    c, s = np.cos(angle), np.sin(angle)
    sign = np.where(np.arange(256) % 2 == 0, 1.0, -1.0)[None, :]
    even = np.concatenate([np.concatenate([c, -s], 1), np.concatenate([s, c], 1)], 0)
    odd = np.concatenate([np.concatenate([s, c], 1), np.concatenate([c, -s], 1)], 0) * sign
    out = []
    for table in (even, odd):
        high, low = halves(table)
        out.append(np.concatenate([high, high, low], axis=0))
    return np.stack(out)


def back_tables():
    angle = 2 * np.pi * np.arange(64)[:, None] * (np.arange(64)[None, :] + 0.5) / 128
    c, s = np.cos(angle), np.sin(angle)
    high, low = halves(np.concatenate([np.concatenate([c, -s], 1), np.concatenate([s, c], 1)], 0))
    rows = np.concatenate([high, high, low], axis=1)
    angle = 2 * np.pi * np.arange(128)[:, None] * np.arange(64)[None, :] / 128
    high, low = halves(np.concatenate([np.cos(angle), -np.sin(angle)], 0) * (2.0 / AREA))
    none = np.zeros_like(high)
    first = np.concatenate([high, none, low, none], axis=1)
    second = np.concatenate([none, high, none, low], axis=1)
    return rows, np.stack([first, second])


def cubic_tables():
    table = np.zeros((128, 64))
    for m in range(64):
        table[2 * m, m] = 1.0
        for step, weight in ((0, 9.0), (1, 9.0), (-1, -1.0), (2, -1.0)):
            table[2 * m + 1, min(max(m + step, 0), 63)] += weight / 16.0
    left = np.concatenate([table, table], axis=1)
    none = np.zeros((64, 128))
    right = np.concatenate(
        [np.concatenate([table.T, none], 1), np.concatenate([none, table.T], 1)], axis=0
    )
    return left.astype(jnp.bfloat16), right.astype(jnp.bfloat16)


def split(x):
    high = x.astype(BF16)
    return high, (x - high.astype(F32)).astype(BF16)


def dot(a, b):
    return jnp.dot(a, b, preferred_element_type=F32)


def shifted(x, shift, width):
    lane = lax.broadcasted_iota(jnp.int32, (x.shape[0], LANE), 1)
    turned = [
        pltpu.roll(x[:, i : i + LANE], LANE - shift, axis=1) for i in range(0, width + LANE, LANE)
    ]
    keep = lane < LANE - shift
    return jnp.concatenate(
        [jnp.where(keep, a, b) for a, b in zip(turned[:-1], turned[1:])], axis=1
    )


def range_spectra(rows_out, col_ref):
    lane = lax.broadcasted_iota(jnp.int32, (64, LANE), 1)
    low_half = lane < 64
    even, odd = [], []
    for x in rows_out:
        for i in range(0, x.shape[1], LANE):
            re = x[:64, i : i + LANE]
            im = pltpu.roll(x[64:, i : i + LANE], 64, axis=1)
            even.append(jnp.where(low_half, re, im))
            odd.append(jnp.where(low_half, im, re))
    out = []
    for parity, parts in enumerate((even, odd)):
        high, low = split(jnp.concatenate(parts, axis=0))
        got = dot(jnp.concatenate([high, low], axis=1), col_ref[parity, :256])
        got = got + dot(high, col_ref[parity, 256:])
        out.append(got)
    count = rows_out[0].shape[1] // LANE
    result = []
    for a in range(len(rows_out)):
        blocks = []
        for i in range(count):
            at = (a * count + i) * 64
            blocks += [out[0][at : at + 64], out[1][at : at + 64]]
        result.append(blocks)
    return result


def ones_where(condition):
    return jnp.where(condition, 1.0, 0.0).astype(BF16)


class Exchange:
    def __init__(self, tiles, bufs, tile_sems, send_sems, recv_sems):
        az, rg = lax.axis_index("az"), lax.axis_index("rg")
        last_az, last_rg = lax.axis_size("az") - 1, lax.axis_size("rg") - 1
        self.up = ("az", az - 1, az > 0)
        self.down = ("az", az + 1, az < last_az)
        self.left = ("rg", rg - 1, rg > 0)
        self.right = ("rg", rg + 1, rg < last_rg)
        self.sides = (self.up, self.down, self.left, self.right)
        self.bufs, self.send_sems, self.recv_sems, self.count = bufs, send_sems, recv_sems, 0
        self.all = []
        self.loads = []
        for i, (tile, (buf, halo)) in enumerate(zip(tiles, bufs)):
            own = buf.at[pl.ds(halo, ROWS), pl.ds(LANE, COLS)]
            self.loads.append(pltpu.make_async_copy(tile, own, tile_sems.at[i]))

    def greet(self):
        for load in self.loads:
            load.start()
        barrier = pltpu.get_barrier_semaphore()
        for axis, place, there in self.sides:

            @pl.when(there)
            def _(axis=axis, place=place):
                pl.semaphore_signal(barrier, inc=1, device_id={axis: place}, device_id_type=MESH)

    def clear(self):
        up, down, left, right = self.sides
        for buf, halo in self.bufs:
            for side, rows, lanes in (
                (up, slice(0, halo), slice(None)),
                (down, slice(halo + ROWS, 2 * halo + ROWS), slice(None)),
                (left, slice(None), slice(0, LANE)),
                (right, slice(None), slice(LANE + COLS, 2 * LANE + COLS)),
            ):

                @pl.when(jnp.logical_not(side[2]))
                def _(buf=buf, rows=rows, lanes=lanes):
                    shape = [n if c == slice(None) else c.stop - c.start for n, c in zip(buf.shape, (rows, lanes))]
                    buf[rows, lanes] = jnp.zeros(shape, F32)

    def meet(self):
        barrier = pltpu.get_barrier_semaphore()
        peers = sum(there.astype(jnp.int32) for _, _, there in self.sides)
        pl.semaphore_wait(barrier, peers)

    def copy(self, buf, rows, lanes, to_rows, to_lanes, side, back, have=None):
        index = self.count
        self.count += 1
        axis, place, sends = side
        comes = back[2]
        if have is not None:
            sends, comes = sends & have, comes & have
        transfer = pltpu.make_async_remote_copy(
            src_ref=buf.at[pl.ds(*rows), pl.ds(*lanes)],
            dst_ref=buf.at[pl.ds(*to_rows), pl.ds(*to_lanes)],
            send_sem=self.send_sems.at[index],
            recv_sem=self.recv_sems.at[index],
            device_id={axis: place},
            device_id_type=MESH,
        )
        entry = (transfer, sends, comes)
        self.all.append(entry)
        return entry

    def along_azimuth(self, buf, halo, near, far, lanes):
        count = far - near
        end = halo + ROWS
        return [
            self.copy(buf, (halo + near, count), lanes, (end + near, count), lanes, self.up, self.down),
            self.copy(buf, (end - far, count), lanes, (halo - far, count), lanes, self.down, self.up),
        ]

    def along_range(self, buf, rows, have=None):
        return [
            self.copy(buf, rows, (LANE, LANE), rows, (LANE + COLS, LANE), self.left, self.right, have),
            self.copy(buf, rows, (COLS, LANE), rows, (0, LANE), self.right, self.left, have),
        ]

    def corners(self, buf, halo, near, far):
        count = far - near
        return self.along_range(buf, (halo - far, count), self.up[2]) + self.along_range(
            buf, (halo + ROWS + near, count), self.down[2]
        )

    @staticmethod
    def start(entries):
        for transfer, sends, _ in entries:

            @pl.when(sends)
            def _(transfer=transfer):
                transfer.start()

    @staticmethod
    def arrive(entries):
        for transfer, _, comes in entries:

            @pl.when(comes)
            def _(transfer=transfer):
                transfer.wait_recv()

    def close(self):
        for transfer, sends, _ in self.all:

            @pl.when(sends)
            def _(transfer=transfer):
                transfer.wait_send()


def kernel(off_az, off_rg, ref_tile, sec_tile, *refs):
    table_hbm, out_ref, tables = refs[:8], refs[8], refs[9:17]
    ref_row_ref, sec_row_ref, col_ref, back_row_ref, back_col_ref, box_col_ref, up_left_ref, up_right_ref = tables
    ref_buf, sec_buf, row_mats, box_mid, box_far, sec_high, sec_low, square_high, square_low = refs[17:26]
    quads, windows, boxes, stats, staged, sem, tile_sems, table_sems, send_sems, recv_sems = refs[26:]
    halo = Exchange(
        (ref_tile, sec_tile),
        ((ref_buf, REF_HALO), (sec_buf, ROW_HALO)),
        tile_sems,
        send_sems,
        recv_sems,
    )
    everything = (LANE, COLS)
    near = halo.along_azimuth(sec_buf, ROW_HALO, 0, NEAR, everything)
    beside = halo.along_range(sec_buf, (ROW_HALO, ROWS)) + halo.along_range(ref_buf, (REF_HALO, ROWS))
    far = {}
    order = (1, 6, 2, 5, 3, 4)
    for b in order:
        lanes = (LANE * b, LANE)
        far[b] = halo.along_azimuth(sec_buf, ROW_HALO, NEAR, ROW_HALO, lanes)
        far[b] += halo.along_azimuth(ref_buf, REF_HALO, 0, REF_HALO, lanes)
    near_corners = halo.corners(sec_buf, ROW_HALO, 0, NEAR)
    far_corners = halo.corners(sec_buf, ROW_HALO, NEAR, ROW_HALO)
    far_corners += halo.corners(ref_buf, REF_HALO, 0, REF_HALO)

    halo.greet()
    fetches = [
        pltpu.make_async_copy(source, target, table_sems.at[i])
        for i, (source, target) in enumerate(zip(table_hbm, tables))
    ]
    for fetch in fetches:
        fetch.start()
    halo.clear()
    for load in halo.loads:
        load.wait()
    halo.meet()
    halo.start(near)
    halo.start(beside)
    for b in order:
        halo.start(far[b])

    own = pl.ds(LANE, COLS)
    ref_mean = jnp.mean(ref_buf[pl.ds(REF_HALO, ROWS), own], keepdims=True)
    sec_mean = jnp.mean(sec_buf[pl.ds(ROW_HALO, ROWS), own], keepdims=True)

    for fetch in fetches:
        fetch.wait()
    lane = lax.broadcasted_iota(jnp.int32, (128, LANE), 1)
    for k in range(2):
        first = NEAR + off_az[k]
        for m in range(2):
            turned = [
                pltpu.roll(sec_row_ref[k + m, :, i : i + LANE], first, axis=1)
                for i in range(0, 512, LANE)
            ]
            moved = [jnp.where(lane < first, turned[i - 1], turned[i]) for i in range(4)]
            row_mats[k, m] = jnp.concatenate(moved, axis=1)[:, : 3 * REACH].astype(BF16)
        lag = lax.broadcasted_iota(jnp.int32, (64, 2 * REACH), 0)
        cell = lax.broadcasted_iota(jnp.int32, (64, 2 * REACH), 1)
        cell = jnp.where(cell < REACH, cell, cell - REACH) + (64 - 64 * k) - first - lag
        box_mid[k] = ones_where((cell >= 0) & (cell < CHIP))
        lag = lax.broadcasted_iota(jnp.int32, (64, 2 * FAR), 0)
        cell = lax.broadcasted_iota(jnp.int32, (64, 2 * FAR), 1)
        cell = jnp.where(cell < FAR, cell, cell - FAR) + REACH * k - first - lag
        box_far[k] = ones_where((cell >= 0) & (cell < CHIP))

    def reference_lines(m, pairs):
        parts = [ref_buf[64 * m : 64 * m + 64, LANE * p : LANE * p + 256] for p in pairs]
        parts = [shifted(x, LANE - REF_HALO, LANE) - ref_mean for x in parts]
        for p, x in zip(pairs, parts):
            place = pl.ds(LANE * p, LANE)
            stats[2 * m : 2 * m + 1, place] = jnp.sum(x, axis=0, keepdims=True)
            stats[2 * m + 1 : 2 * m + 2, place] = jnp.sum(x * x, axis=0, keepdims=True)
        high, low = split(jnp.concatenate(parts, axis=1))
        return dot(ref_row_ref[m], jnp.concatenate([high, low, high], axis=0))

    def take_lines(k, spans, pairs):
        for p in pairs:
            place = slice(LANE * p, LANE * p + LANE)
            for first, count in spans:
                rows = slice(first, first + count)
                x = shifted(sec_buf[rows, LANE * p : LANE * p + 256], 64 + off_rg[k], LANE) - sec_mean
                sec_high[k, rows, place], sec_low[k, rows, place] = split(x)
                square_high[k, rows, place], square_low[k, rows, place] = split(x * x)

    def box_lines(k, first, count, p, box_ref):
        rows, place = slice(first, first + count), slice(LANE * p, LANE * p + LANE)
        stack = jnp.concatenate(
            [
                jnp.concatenate([sec_high[k, rows, place], square_high[k, rows, place]], axis=1),
                jnp.concatenate([sec_low[k, rows, place], square_low[k, rows, place]], axis=1),
            ],
            axis=0,
        )
        return dot(box_ref[k], stack)

    def window_transform(k, m, pairs):
        rows = slice(64 * (k + m), 64 * (k + m) + REACH)
        high = jnp.concatenate([sec_high[k, rows, LANE * p : LANE * p + LANE] for p in pairs], axis=1)
        low = jnp.concatenate([sec_low[k, rows, LANE * p : LANE * p + LANE] for p in pairs], axis=1)
        return dot(row_mats[k, m], jnp.concatenate([high, low, high], axis=0))

    def store(target, pairs, blocks):
        for i, p in enumerate(pairs):
            for half in range(2):
                target[2 * p + half] = blocks[2 * i + half]

    def middle_quadrants(*groups):
        rows_out = [reference_lines(1, pairs) for pairs in groups]
        for pairs, x in zip(groups, rows_out):
            store(quads.at[1], pairs, range_spectra([x], col_ref)[0])

    def middle_windows(*groups):
        rows_out = [[window_transform(k, 1 - k, pairs) for k in range(2)] for pairs in groups]
        for pairs in groups:
            for k in range(2):
                for p in pairs:
                    sums = box_lines(k, 64, REACH, p, box_mid)
                    boxes[k, :64, LANE * p : LANE * p + LANE] = sums[:, :128]
                    boxes[k, 64:, LANE * p : LANE * p + LANE] = sums[:, 128:]
        for pairs, x in zip(groups, rows_out):
            got = range_spectra(x, col_ref)
            store(windows.at[0, 1], pairs, got[0])
            store(windows.at[1, 0], pairs, got[1])

    def outer(*groups):
        for pairs in groups:
            take_lines(0, ((0, FAR),), pairs)
            take_lines(1, ((224, FAR),), pairs)
        rows_out = [
            [
                [reference_lines(2 * k, pairs), window_transform(k, k, pairs)]
                for k in range(2)
            ]
            for pairs in groups
        ]
        for pairs in groups:
            for k in range(2):
                for p in pairs:
                    sums = box_lines(k, 224 * k, FAR, p, box_far)
                    boxes[k, :64, LANE * p : LANE * p + LANE] += sums[:, :128]
                    boxes[k, 64:, LANE * p : LANE * p + LANE] += sums[:, 128:]
        for pairs, x in zip(groups, rows_out):
            for k in range(2):
                got = range_spectra(x[k], col_ref)
                store(quads.at[2 * k], pairs, got[0])
                store(windows.at[k, k], pairs, got[1])

    def strip(k, n):
        re, im = 0.0, 0.0
        for m in range(2):
            q = quads[k + m, n]
            x = windows[k, m, n] + windows[k, m, n + 1]
            qr, qi, xr, xi = q[:, :128], q[:, 128:], x[:, :128], x[:, 128:]
            re = re + (qr * xr + qi * xi)
            im = im + (qr * xi - qi * xr)
        return jnp.concatenate([re, im], axis=0)

    def finish(*pairs):
        items = [(k, s) for s in pairs for k in range(2)]
        moments = {}
        for s in pairs:
            stat = stats[:, s * LANE : s * LANE + 256]
            place = lax.broadcasted_iota(jnp.int32, stat.shape, 1)
            a = jnp.sum(stat[:, :128], axis=1, keepdims=True)
            b = jnp.sum(jnp.where((place >= 64) & (place < 192), stat, 0.0), axis=1, keepdims=True)
            moments[s] = jnp.where(place[:, :128] < 64, a, b)
        sums = {}
        for k, s in items:
            for n in range(2 * s, 2 * s + 3):
                if (k, n) not in sums:
                    sums[k, n] = strip(k, n)
        inner = {}
        for k, s in items:
            left, middle_, right = [sums[k, 2 * s + i] for i in range(3)]
            high, low = split(jnp.concatenate([left + middle_, middle_ + right], axis=1))
            y = dot(back_row_ref[:, :256], jnp.concatenate([high, low], axis=0))
            inner[k, s] = y + dot(back_row_ref[:, 256:], high)
        scores = {}
        for k, s in items:
            y = inner[k, s]
            corr = 0.0
            for i in range(2):
                lanes = slice(LANE * i, LANE * i + LANE)
                high, low = split(jnp.concatenate([y[:64, lanes], y[64:, lanes]], axis=1))
                wide = dot(high, back_col_ref[i])
                corr = corr + (wide[:, :128] + wide[:, 128:]) + dot(low, back_col_ref[i, :, :128])
            high, low = split(boxes[k, :, s * LANE : s * LANE + 256])
            box = dot(high, box_col_ref[...]) + dot(low, box_col_ref[...])
            first, second = box[:64], box[64:]
            both = moments[s]
            total = both[2 * k : 2 * k + 1] + both[2 * k + 2 : 2 * k + 3]
            power = both[2 * k + 1 : 2 * k + 2] + both[2 * k + 3 : 2 * k + 4]
            mean = total / AREA
            energy = power - total * mean
            centered = corr - mean * first
            var_sum = jnp.maximum(second - first * first / AREA, 0.0)
            scores[k, s] = (CHIP / AREA) * centered * lax.rsqrt(
                (energy / AREA) * (var_sum / AREA) + EPSILON
            )
        lifted = {}
        for k, s in items:
            high, low = split(scores[k, s])
            lifted[k, s] = dot(up_left_ref[...], jnp.concatenate([high, low], axis=0))
        for k, s in items:
            high, low = split(lifted[k, s])
            wide = dot(high, up_right_ref[...]) + dot(low, up_right_ref[...])
            at = k * CHIPS + 2 * s
            staged[at] = wide[:, :128]
            staged[at + 1] = wide[:, 128:]
        for k, s in items:
            at = k * CHIPS + 2 * s
            pltpu.make_async_copy(staged.at[pl.ds(at, 2)], out_ref.at[pl.ds(at, 2)], sem).start()

    inside = (1, 2, 3, 4, 5)
    near_lines = ((ROW_HALO - NEAR, NEAR), (ROW_HALO + ROWS, NEAR))
    middle_quadrants((1, 2), (3, 4), (5,))
    for k in range(2):
        take_lines(k, ((ROW_HALO, ROWS),), inside)
    halo.arrive(near)
    halo.start(near_corners)
    for k in range(2):
        take_lines(k, near_lines, inside)
    middle_windows((1, 2), (3, 4), (5,))
    halo.arrive(far[1] + far[6])
    halo.start(far_corners)
    halo.arrive(beside)
    middle_quadrants((0, 6))
    halo.arrive(near_corners)
    for k in range(2):
        take_lines(k, near_lines + ((ROW_HALO, ROWS),), (0, 6))
    middle_windows((0, 6))
    halo.arrive(far[2] + far[5])
    outer((1, 5))
    halo.arrive(far_corners)
    outer((0, 6))
    finish(0, 5)
    halo.arrive(far[3] + far[4])
    outer((2,), (3, 4))
    finish(1, 2, 3, 4)
    halo.close()
    pltpu.make_async_copy(staged, out_ref, sem).wait()


def spread(table):
    room = np.zeros((128, REACH - 128))
    parts = [np.concatenate([table[:, i : i + 128].astype(np.float64), room], 1) for i in (0, 128, 256)]
    return np.concatenate(parts + [room], axis=1).astype(np.float32)


def body(ref_image, sec_image, off_az, off_rg):
    back_rows, back_cols = back_tables()
    left, right = cubic_tables()
    tables = [
        np.stack([azimuth_table(64 * m, 64) for m in range(3)]),
        np.stack([spread(azimuth_table(64 * j, 128)) for j in range(3)]),
        column_tables(),
        back_rows,
        back_cols,
        box_table(),
        left,
        right,
    ]
    smem = pl.BlockSpec(memory_space=pltpu.SMEM)
    out = pl.pallas_call(
        kernel,
        out_shape=jax.ShapeDtypeStruct((2 * CHIPS, 128, 128), F32),
        in_specs=[smem, smem] + [pl.BlockSpec(memory_space=pl.ANY)] * (2 + len(tables)),
        out_specs=pl.BlockSpec(memory_space=pl.ANY),
        scratch_shapes=[pltpu.VMEM(t.shape, t.dtype) for t in tables]
        + [
            pltpu.VMEM((ROWS + 2 * REF_HALO, COLS + 2 * LANE), F32),
            pltpu.VMEM((ROWS + 2 * ROW_HALO, COLS + 2 * LANE), F32),
            pltpu.VMEM((2, 2, 128, 3 * REACH), BF16),
            pltpu.VMEM((2, 64, 2 * REACH), BF16),
            pltpu.VMEM((2, 64, 2 * FAR), BF16),
            pltpu.VMEM((2, ROWS + 2 * ROW_HALO, WIDE), BF16),
            pltpu.VMEM((2, ROWS + 2 * ROW_HALO, WIDE), BF16),
            pltpu.VMEM((2, ROWS + 2 * ROW_HALO, WIDE), BF16),
            pltpu.VMEM((2, ROWS + 2 * ROW_HALO, WIDE), BF16),
            pltpu.VMEM((3, BLOCKS, 64, 256), F32),
            pltpu.VMEM((2, 2, BLOCKS, 64, 256), F32),
            pltpu.VMEM((2, 128, WIDE), F32),
            pltpu.VMEM((8, WIDE), F32),
            pltpu.VMEM((2 * CHIPS, 128, 128), F32),
            pltpu.SemaphoreType.DMA,
            pltpu.SemaphoreType.DMA((2,)),
            pltpu.SemaphoreType.DMA((8,)),
            pltpu.SemaphoreType.DMA((48,)),
            pltpu.SemaphoreType.DMA((48,)),
        ],
        compiler_params=pltpu.CompilerParams(collective_id=0, has_side_effects=True),
    )(off_az, off_rg, ref_image, sec_image, *[jnp.asarray(t) for t in tables])
    return out.reshape(2, CHIPS, 128, 128)


def solution(mesh):
    return jax.shard_map(
        body,
        mesh=mesh,
        in_specs=(P("az", "rg"), P("az", "rg"), P("az"), P("az")),
        out_specs=P("az", "rg", None, None),
        check_vma=False,
    )
```

```python
import functools

import jax
import jax.numpy as jnp
import numpy as np
from jax import lax
from jax.experimental import pallas as pl
from jax.experimental.pallas import tpu as pltpu
from jax.sharding import PartitionSpec as P

CHIP = 128
SPACE = 64
LAGS = 64
AREA = float(CHIP * CHIP)
EPSILON = 1e-06
ROWS = 128
COLS = 768
CHIPS = COLS // SPACE
PAIRS = CHIPS // 2
BLOCKS = CHIPS + 2
WIDE = BLOCKS * SPACE
ROW_HALO = 80
REF_HALO = 32
NEAR = 16
FAR = 64
REACH = 160
LANE = 128
MESH = pl.DeviceIdType.MESH
F32 = jnp.float32
BF16 = jnp.bfloat16


def halves(table):
    high = table.astype(jnp.bfloat16)
    low = (table - high.astype(np.float64)).astype(jnp.bfloat16)
    return high, low


def azimuth_table(first, count):
    angle = 2 * np.pi * (np.arange(64)[:, None] + 0.5) * (first + np.arange(count))[None, :] / 128
    high, low = halves(np.concatenate([np.cos(angle), -np.sin(angle)], axis=0))
    return np.concatenate([high, high, low], axis=1)


def box_table():
    cell = np.arange(256)[:, None]
    lag = np.arange(128)[None, :]
    return ((cell >= lag) & (cell < lag + 128)).astype(jnp.bfloat16)


def column_tables():
    angle = 2 * np.pi * np.arange(64)[:, None] * np.arange(128)[None, :] / 128
    c, s = np.cos(angle), np.sin(angle)
    sign = np.where(np.arange(256) % 2 == 0, 1.0, -1.0)[None, :]
    even = np.concatenate([np.concatenate([c, -s], 1), np.concatenate([s, c], 1)], 0)
    odd = np.concatenate([np.concatenate([s, c], 1), np.concatenate([c, -s], 1)], 0) * sign
    out = []
    for table in (even, odd):
        high, low = halves(table)
        out.append(np.concatenate([high, high, low], axis=0))
    return np.stack(out)


def back_tables():
    angle = 2 * np.pi * np.arange(64)[:, None] * (np.arange(64)[None, :] + 0.5) / 128
    c, s = np.cos(angle), np.sin(angle)
    high, low = halves(np.concatenate([np.concatenate([c, -s], 1), np.concatenate([s, c], 1)], 0))
    rows = np.concatenate([high, high, low], axis=1)
    angle = 2 * np.pi * np.arange(128)[:, None] * np.arange(64)[None, :] / 128
    high, low = halves(np.concatenate([np.cos(angle), -np.sin(angle)], 0) * (2.0 / AREA))
    none = np.zeros_like(high)
    first = np.concatenate([high, none, low, none], axis=1)
    second = np.concatenate([none, high, none, low], axis=1)
    return rows, np.stack([first, second])


def split(x):
    high = x.astype(BF16)
    return high, (x - high.astype(F32)).astype(BF16)


def dot(a, b):
    return jnp.dot(a, b, preferred_element_type=F32)


def shifted(x, shift, width):
    lane = lax.broadcasted_iota(jnp.int32, (x.shape[0], LANE), 1)
    turned = [
        pltpu.roll(x[:, i : i + LANE], LANE - shift, axis=1) for i in range(0, width + LANE, LANE)
    ]
    keep = lane < LANE - shift
    return jnp.concatenate(
        [jnp.where(keep, a, b) for a, b in zip(turned[:-1], turned[1:])], axis=1
    )


def range_spectra(rows_out, col_ref):
    lane = lax.broadcasted_iota(jnp.int32, (64, LANE), 1)
    low_half = lane < 64
    even, odd = [], []
    for x in rows_out:
        for i in range(0, x.shape[1], LANE):
            re = x[:64, i : i + LANE]
            im = pltpu.roll(x[64:, i : i + LANE], 64, axis=1)
            even.append(jnp.where(low_half, re, im))
            odd.append(jnp.where(low_half, im, re))
    out = []
    for parity, parts in enumerate((even, odd)):
        high, low = split(jnp.concatenate(parts, axis=0))
        got = dot(jnp.concatenate([high, low], axis=1), col_ref[parity, :256])
        got = got + dot(high, col_ref[parity, 256:])
        out.append(got)
    count = rows_out[0].shape[1] // LANE
    result = []
    for a in range(len(rows_out)):
        blocks = []
        for i in range(count):
            at = (a * count + i) * 64
            blocks += [out[0][at : at + 64], out[1][at : at + 64]]
        result.append(blocks)
    return result


def ones_where(condition):
    return jnp.where(condition, 1.0, 0.0).astype(BF16)


class Exchange:
    def __init__(self, tiles, bufs, tile_sems, send_sems, recv_sems):
        az, rg = lax.axis_index("az"), lax.axis_index("rg")
        last_az, last_rg = lax.axis_size("az") - 1, lax.axis_size("rg") - 1
        self.up = ("az", az - 1, az > 0)
        self.down = ("az", az + 1, az < last_az)
        self.left = ("rg", rg - 1, rg > 0)
        self.right = ("rg", rg + 1, rg < last_rg)
        self.sides = (self.up, self.down, self.left, self.right)
        self.bufs, self.send_sems, self.recv_sems, self.count = bufs, send_sems, recv_sems, 0
        self.all = []
        self.loads = []
        for i, (tile, (buf, halo)) in enumerate(zip(tiles, bufs)):
            own = buf.at[pl.ds(halo, ROWS), pl.ds(LANE, COLS)]
            self.loads.append(pltpu.make_async_copy(tile, own, tile_sems.at[i]))

    def greet(self):
        for load in self.loads:
            load.start()
        barrier = pltpu.get_barrier_semaphore()
        for axis, place, there in self.sides:

            @pl.when(there)
            def _(axis=axis, place=place):
                pl.semaphore_signal(barrier, inc=1, device_id={axis: place}, device_id_type=MESH)

    def clear(self):
        up, down, left, right = self.sides
        for buf, halo in self.bufs:
            for side, rows, lanes in (
                (up, slice(0, halo), slice(None)),
                (down, slice(halo + ROWS, 2 * halo + ROWS), slice(None)),
                (left, slice(None), slice(0, LANE)),
                (right, slice(None), slice(LANE + COLS, 2 * LANE + COLS)),
            ):

                @pl.when(jnp.logical_not(side[2]))
                def _(buf=buf, rows=rows, lanes=lanes):
                    shape = [n if c == slice(None) else c.stop - c.start for n, c in zip(buf.shape, (rows, lanes))]
                    buf[rows, lanes] = jnp.zeros(shape, F32)

    def meet(self):
        barrier = pltpu.get_barrier_semaphore()
        peers = sum(there.astype(jnp.int32) for _, _, there in self.sides)
        pl.semaphore_wait(barrier, peers)

    def copy(self, buf, rows, lanes, to_rows, to_lanes, side, back, have=None):
        index = self.count
        self.count += 1
        axis, place, sends = side
        comes = back[2]
        if have is not None:
            sends, comes = sends & have, comes & have
        transfer = pltpu.make_async_remote_copy(
            src_ref=buf.at[pl.ds(*rows), pl.ds(*lanes)],
            dst_ref=buf.at[pl.ds(*to_rows), pl.ds(*to_lanes)],
            send_sem=self.send_sems.at[index],
            recv_sem=self.recv_sems.at[index],
            device_id={axis: place},
            device_id_type=MESH,
        )
        entry = (transfer, sends, comes)
        self.all.append(entry)
        return entry

    def along_azimuth(self, buf, halo, near, far, lanes):
        count = far - near
        end = halo + ROWS
        return [
            self.copy(buf, (halo + near, count), lanes, (end + near, count), lanes, self.up, self.down),
            self.copy(buf, (end - far, count), lanes, (halo - far, count), lanes, self.down, self.up),
        ]

    def along_range(self, buf, rows, have=None):
        return [
            self.copy(buf, rows, (LANE, LANE), rows, (LANE + COLS, LANE), self.left, self.right, have),
            self.copy(buf, rows, (COLS, LANE), rows, (0, LANE), self.right, self.left, have),
        ]

    def corners(self, buf, halo, near, far):
        count = far - near
        return self.along_range(buf, (halo - far, count), self.up[2]) + self.along_range(
            buf, (halo + ROWS + near, count), self.down[2]
        )

    @staticmethod
    def start(entries):
        for transfer, sends, _ in entries:

            @pl.when(sends)
            def _(transfer=transfer):
                transfer.start()

    @staticmethod
    def arrive(entries):
        for transfer, _, comes in entries:

            @pl.when(comes)
            def _(transfer=transfer):
                transfer.wait_recv()

    def close(self):
        for transfer, sends, _ in self.all:

            @pl.when(sends)
            def _(transfer=transfer):
                transfer.wait_send()


def kernel(off_az_hbm, off_rg_hbm, ref_tile, sec_tile, *refs):
    table_hbm, score_ref, tables = refs[:6], refs[6], refs[7:13]
    ref_row_ref, sec_row_ref, col_ref, back_row_ref, back_col_ref, box_col_ref = tables
    off_az, off_rg, ref_buf, sec_buf, row_mats, box_mid, box_far = refs[13:20]
    sec_high, sec_low, square_high, square_low = refs[20:24]
    quads, windows, strips, boxes, stats, tile_sems, table_sems, send_sems, recv_sems = refs[24:]
    halo = Exchange(
        (ref_tile, sec_tile),
        ((ref_buf, REF_HALO), (sec_buf, ROW_HALO)),
        tile_sems,
        send_sems,
        recv_sems,
    )
    everything = (LANE, COLS)
    near = halo.along_azimuth(sec_buf, ROW_HALO, 0, NEAR, everything)
    beside = halo.along_range(sec_buf, (ROW_HALO, ROWS)) + halo.along_range(ref_buf, (REF_HALO, ROWS))
    order = (1, 6, 2, 5, 3, 4)
    sec_far, ref_far = {}, {}
    for b in order:
        sec_far[b] = halo.along_azimuth(sec_buf, ROW_HALO, NEAR, ROW_HALO, (LANE * b, LANE))
    for b, lanes in ((1, (LANE, LANE)), (6, (COLS, LANE)), (2, (2 * LANE, 4 * LANE))):
        ref_far[b] = halo.along_azimuth(ref_buf, REF_HALO, 0, REF_HALO, lanes)
    near_corners = halo.corners(sec_buf, ROW_HALO, 0, NEAR)
    sec_corners = halo.corners(sec_buf, ROW_HALO, NEAR, ROW_HALO)
    ref_corners = halo.corners(ref_buf, REF_HALO, 0, REF_HALO)

    halo.greet()
    fetches = [
        pltpu.make_async_copy(source, target, table_sems.at[i])
        for i, (source, target) in enumerate(
            zip((off_az_hbm, off_rg_hbm) + table_hbm, (off_az, off_rg) + tables)
        )
    ]
    for fetch in fetches:
        fetch.start()
    halo.clear()
    for load in halo.loads:
        load.wait()
    halo.meet()
    halo.start(near)
    halo.start(beside)
    halo.start(sec_far[1] + sec_far[6])
    halo.start(ref_far[1] + ref_far[6] + ref_far[2])
    for b in order[2:]:
        halo.start(sec_far[b])

    own = pl.ds(LANE, COLS)
    ref_mean = jnp.mean(ref_buf[pl.ds(REF_HALO, ROWS), own], keepdims=True)
    sec_mean = jnp.mean(sec_buf[pl.ds(ROW_HALO, ROWS), own], keepdims=True)

    for fetch in fetches:
        fetch.wait()
    lane = lax.broadcasted_iota(jnp.int32, (128, LANE), 1)
    for k in range(2):
        first = NEAR + off_az[k]
        for m in range(2):
            turned = [
                pltpu.roll(sec_row_ref[k + m, :, i : i + LANE], first, axis=1)
                for i in range(0, 512, LANE)
            ]
            moved = [jnp.where(lane < first, turned[i - 1], turned[i]) for i in range(4)]
            row_mats[k, m] = jnp.concatenate(moved, axis=1)[:, : 3 * REACH].astype(BF16)
        lag = lax.broadcasted_iota(jnp.int32, (64, 2 * REACH), 0)
        cell = lax.broadcasted_iota(jnp.int32, (64, 2 * REACH), 1)
        cell = jnp.where(cell < REACH, cell, cell - REACH) + (64 - 64 * k) - first - lag
        box_mid[k] = ones_where((cell >= 0) & (cell < CHIP))
        lag = lax.broadcasted_iota(jnp.int32, (64, 2 * FAR), 0)
        cell = lax.broadcasted_iota(jnp.int32, (64, 2 * FAR), 1)
        cell = jnp.where(cell < FAR, cell, cell - FAR) + REACH * k - first - lag
        box_far[k] = ones_where((cell >= 0) & (cell < CHIP))

    def reference_lines(m, pairs):
        parts = [ref_buf[64 * m : 64 * m + 64, LANE * p : LANE * p + 256] for p in pairs]
        parts = [shifted(x, LANE - REF_HALO, LANE) - ref_mean for x in parts]
        for p, x in zip(pairs, parts):
            place = pl.ds(LANE * p, LANE)
            stats[2 * m : 2 * m + 1, place] = jnp.sum(x, axis=0, keepdims=True)
            stats[2 * m + 1 : 2 * m + 2, place] = jnp.sum(x * x, axis=0, keepdims=True)
        high, low = split(jnp.concatenate(parts, axis=1))
        return dot(ref_row_ref[m], jnp.concatenate([high, low, high], axis=0))

    def take_lines(k, spans, pairs):
        for p in pairs:
            place = slice(LANE * p, LANE * p + LANE)
            for first, count in spans:
                rows = slice(first, first + count)
                x = shifted(sec_buf[rows, LANE * p : LANE * p + 256], 64 + off_rg[k], LANE) - sec_mean
                sec_high[k, rows, place], sec_low[k, rows, place] = split(x)
                square_high[k, rows, place], square_low[k, rows, place] = split(x * x)

    def box_lines(k, first, count, p, box_ref):
        rows, place = slice(first, first + count), slice(LANE * p, LANE * p + LANE)
        stack = jnp.concatenate(
            [
                jnp.concatenate([sec_high[k, rows, place], square_high[k, rows, place]], axis=1),
                jnp.concatenate([sec_low[k, rows, place], square_low[k, rows, place]], axis=1),
            ],
            axis=0,
        )
        return dot(box_ref[k], stack)

    def window_transform(k, m, pairs):
        rows = slice(64 * (k + m), 64 * (k + m) + REACH)
        high = jnp.concatenate([sec_high[k, rows, LANE * p : LANE * p + LANE] for p in pairs], axis=1)
        low = jnp.concatenate([sec_low[k, rows, LANE * p : LANE * p + LANE] for p in pairs], axis=1)
        return dot(row_mats[k, m], jnp.concatenate([high, low, high], axis=0))

    def store(target, pairs, blocks):
        for i, p in enumerate(pairs):
            for half in range(2):
                target[2 * p + half] = blocks[2 * i + half]

    def middle_quadrants(*groups):
        rows_out = [reference_lines(1, pairs) for pairs in groups]
        for pairs, x in zip(groups, rows_out):
            store(quads.at[1], pairs, range_spectra([x], col_ref)[0])

    def middle_windows(*groups):
        rows_out = [[window_transform(k, 1 - k, pairs) for k in range(2)] for pairs in groups]
        for pairs in groups:
            for k in range(2):
                for p in pairs:
                    sums = box_lines(k, 64, REACH, p, box_mid)
                    boxes[k, :64, LANE * p : LANE * p + LANE] = sums[:, :128]
                    boxes[k, 64:, LANE * p : LANE * p + LANE] = sums[:, 128:]
        for pairs, x in zip(groups, rows_out):
            got = range_spectra(x, col_ref)
            store(windows.at[0, 1], pairs, got[0])
            store(windows.at[1, 0], pairs, got[1])

    def outer_quadrants(*groups):
        rows_out = [[reference_lines(m, pairs) for m in (0, 2)] for pairs in groups]
        for pairs, x in zip(groups, rows_out):
            got = range_spectra(x, col_ref)
            store(quads.at[0], pairs, got[0])
            store(quads.at[2], pairs, got[1])

    def outer_windows(*groups):
        for pairs in groups:
            take_lines(0, ((0, FAR),), pairs)
            take_lines(1, ((224, FAR),), pairs)
        rows_out = [[window_transform(k, k, pairs) for k in range(2)] for pairs in groups]
        for pairs in groups:
            for k in range(2):
                for p in pairs:
                    sums = box_lines(k, 224 * k, FAR, p, box_far)
                    boxes[k, :64, LANE * p : LANE * p + LANE] += sums[:, :128]
                    boxes[k, 64:, LANE * p : LANE * p + LANE] += sums[:, 128:]
        for pairs, x in zip(groups, rows_out):
            got = range_spectra(x, col_ref)
            for k in range(2):
                store(windows.at[k, k], pairs, got[k])

    def product(k, m, n):
        q = quads[k + m, n]
        x = windows[k, m, n] + windows[k, m, n + 1]
        qr, qi, xr, xi = q[:, :128], q[:, 128:], x[:, :128], x[:, 128:]
        return jnp.concatenate([qr * xr + qi * xi, qr * xi - qi * xr], axis=0)

    def middle_strips(*numbers):
        for n in numbers:
            for k in range(2):
                strips[k, n] = product(k, 1 - k, n)

    done = {}

    def strip(k, n):
        if (k, n) not in done:
            done[k, n] = True
            strips[k, n] += product(k, k, n)
        return strips[k, n]

    def finish(*pairs):
        items = [(k, s) for s in pairs for k in range(2)]
        moments = {}
        for s in pairs:
            stat = stats[:, s * LANE : s * LANE + 256]
            place = lax.broadcasted_iota(jnp.int32, stat.shape, 1)
            a = jnp.sum(stat[:, :128], axis=1, keepdims=True)
            b = jnp.sum(jnp.where((place >= 64) & (place < 192), stat, 0.0), axis=1, keepdims=True)
            moments[s] = jnp.where(place[:, :128] < 64, a, b)
        sums = {(k, n): strip(k, n) for k, s in items for n in range(2 * s, 2 * s + 3)}
        inner = {}
        for k, s in items:
            left, middle_, right = [sums[k, 2 * s + i] for i in range(3)]
            high, low = split(jnp.concatenate([left + middle_, middle_ + right], axis=1))
            y = dot(back_row_ref[:, :256], jnp.concatenate([high, low], axis=0))
            inner[k, s] = y + dot(back_row_ref[:, 256:], high)
        for k, s in items:
            y = inner[k, s]
            corr = 0.0
            for i in range(2):
                lanes = slice(LANE * i, LANE * i + LANE)
                high, low = split(jnp.concatenate([y[:64, lanes], y[64:, lanes]], axis=1))
                wide = dot(high, back_col_ref[i])
                corr = corr + (wide[:, :128] + wide[:, 128:]) + dot(low, back_col_ref[i, :, :128])
            high, low = split(boxes[k, :, s * LANE : s * LANE + 256])
            box = dot(high, box_col_ref[...]) + dot(low, box_col_ref[...])
            first, second = box[:64], box[64:]
            both = moments[s]
            total = both[2 * k : 2 * k + 1] + both[2 * k + 2 : 2 * k + 3]
            power = both[2 * k + 1 : 2 * k + 2] + both[2 * k + 3 : 2 * k + 4]
            mean = total / AREA
            energy = power - total * mean
            centered = corr - mean * first
            var_sum = jnp.maximum(second - first * first / AREA, 0.0)
            score_ref[k, s] = (CHIP / AREA) * centered * lax.rsqrt(
                (energy / AREA) * (var_sum / AREA) + EPSILON
            )

    inside = (1, 2, 3, 4, 5)
    near_lines = ((ROW_HALO - NEAR, NEAR), (ROW_HALO + ROWS, NEAR))
    middle_quadrants((1, 2), (3, 4), (5,))
    for k in range(2):
        take_lines(k, ((ROW_HALO, ROWS),), inside)
    halo.arrive(near)
    halo.start(near_corners)
    for k in range(2):
        take_lines(k, near_lines, inside)
    middle_windows((1, 2), (3, 4), (5,))
    halo.arrive(sec_far[1] + sec_far[6])
    halo.start(sec_corners)
    halo.arrive(beside)
    middle_quadrants((0, 6))
    halo.arrive(ref_far[1] + ref_far[6])
    halo.start(ref_corners)
    halo.arrive(near_corners)
    for k in range(2):
        take_lines(k, near_lines + ((ROW_HALO, ROWS),), (0, 6))
    middle_windows((0, 6))
    middle_strips(*range(BLOCKS - 1))
    halo.arrive(ref_far[2])
    outer_quadrants((1, 2), (3, 4), (5,))
    halo.arrive(ref_corners)
    outer_quadrants((0, 6))
    halo.arrive(sec_far[2] + sec_far[5] + sec_corners)
    outer_windows((1, 5), (0, 6))
    halo.arrive(sec_far[3])
    outer_windows((2,))
    finish(0, 1, 5)
    halo.arrive(sec_far[4])
    outer_windows((3, 4))
    finish(2, 3, 4)
    halo.close()


def oversample(score_ref, out_ref, staged, sem):
    def cubic(out_index, sample):
        base = out_index // 2

        def pick(step):
            return jnp.where(jnp.clip(base + step, 0, LAGS - 1) == sample, 1.0, 0.0)

        odd = (9.0 * (pick(0) + pick(1)) - (pick(-1) + pick(2))) / 16.0
        return jnp.where(out_index % 2 == 1, odd, pick(0))

    row = lax.broadcasted_iota(jnp.int32, (128, 128), 0)
    lane = lax.broadcasted_iota(jnp.int32, (128, 128), 1)
    left = cubic(row, lane % LAGS).astype(BF16)
    right = cubic(lane, row % LAGS)
    right = jnp.concatenate(
        [jnp.where(row < LAGS, right, 0.0), jnp.where(row < LAGS, 0.0, right)], axis=1
    ).astype(BF16)
    items = [(k, s) for k in range(2) for s in range(PAIRS)]
    for some in (items[:4], items[4:8], items[8:]):
        lifted = []
        for k, s in some:
            high, low = split(score_ref[k, s])
            lifted.append(dot(left, jnp.concatenate([high, low], axis=0)))
        for (k, s), value in zip(some, lifted):
            high, low = split(value)
            wide = dot(high, right) + dot(low, right)
            at = k * CHIPS + 2 * s
            staged[at] = wide[:, :128]
            staged[at + 1] = wide[:, 128:]
        for k, s in some:
            part = pl.ds(k * CHIPS + 2 * s, 2)
            pltpu.make_async_copy(staged.at[part], out_ref.at[part], sem).start()
    pltpu.make_async_copy(staged, out_ref, sem).wait()


def spread(table):
    room = np.zeros((128, REACH - 128))
    parts = [np.concatenate([table[:, i : i + 128].astype(np.float64), room], 1) for i in (0, 128, 256)]
    return np.concatenate(parts + [room], axis=1).astype(np.float32)


def body(ref_image, sec_image, off_az, off_rg):
    back_rows, back_cols = back_tables()
    tables = [
        np.stack([azimuth_table(64 * m, 64) for m in range(3)]),
        np.stack([spread(azimuth_table(64 * j, 128)) for j in range(3)]),
        column_tables(),
        back_rows,
        back_cols,
        box_table(),
    ]
    anywhere = pl.BlockSpec(memory_space=pl.ANY)
    vmem = pl.BlockSpec(memory_space=pltpu.VMEM)
    scores = pl.pallas_call(
        kernel,
        out_shape=pltpu.VMEM((2, PAIRS, LAGS, 2 * LAGS), F32),
        in_specs=[pl.BlockSpec(memory_space=pltpu.HBM)] * (4 + len(tables)),
        out_specs=vmem,
        scratch_shapes=[pltpu.VMEM(t.shape, t.dtype) for t in tables]
        + [
            pltpu.SMEM((2,), jnp.int32),
            pltpu.SMEM((2,), jnp.int32),
            pltpu.VMEM((ROWS + 2 * REF_HALO, COLS + 2 * LANE), F32),
            pltpu.VMEM((ROWS + 2 * ROW_HALO, COLS + 2 * LANE), F32),
            pltpu.VMEM((2, 2, 128, 3 * REACH), BF16),
            pltpu.VMEM((2, 64, 2 * REACH), BF16),
            pltpu.VMEM((2, 64, 2 * FAR), BF16),
        ]
        + [pltpu.VMEM((2, ROWS + 2 * ROW_HALO, WIDE), BF16)] * 4
        + [
            pltpu.VMEM((3, BLOCKS, 64, 256), F32),
            pltpu.VMEM((2, 2, BLOCKS, 64, 256), F32),
            pltpu.VMEM((2, BLOCKS - 1, 128, 128), F32),
            pltpu.VMEM((2, 128, WIDE), F32),
            pltpu.VMEM((8, WIDE), F32),
            pltpu.SemaphoreType.DMA((2,)),
            pltpu.SemaphoreType.DMA((8,)),
            pltpu.SemaphoreType.DMA((48,)),
            pltpu.SemaphoreType.DMA((48,)),
        ],
        compiler_params=pltpu.CompilerParams(
            collective_id=0, has_side_effects=True
        ),
    )(off_az, off_rg, ref_image, sec_image, *[jnp.asarray(t) for t in tables])
    out = pl.pallas_call(
        oversample,
        out_shape=jax.ShapeDtypeStruct((2 * CHIPS, 128, 128), F32),
        in_specs=[vmem],
        out_specs=anywhere,
        scratch_shapes=[pltpu.VMEM((2 * CHIPS, 128, 128), F32), pltpu.SemaphoreType.DMA],
        compiler_params=pltpu.CompilerParams(vmem_limit_bytes=8 << 20),
    )(scores)
    return out.reshape(2, CHIPS, 128, 128)


def solution(mesh):
    return jax.shard_map(
        body,
        mesh=mesh,
        in_specs=(P("az", "rg"), P("az", "rg"), P("az"), P("az")),
        out_specs=P("az", "rg", None, None),
        check_vma=False,
    )
```

```python
import functools

import jax
import jax.numpy as jnp
import numpy as np
from jax import lax
from jax.experimental import pallas as pl
from jax.experimental.pallas import tpu as pltpu
from jax.sharding import PartitionSpec as P

CHIP = 128
SPACE = 64
LAGS = 64
AREA = float(CHIP * CHIP)
EPSILON = 1e-06
ROWS = 128
COLS = 768
CHIPS = COLS // SPACE
PAIRS = CHIPS // 2
BLOCKS = CHIPS + 2
WIDE = BLOCKS * SPACE
ROW_HALO = 80
REF_HALO = 32
NEAR = 16
FAR = 64
REACH = 160
LANE = 128
MESH = pl.DeviceIdType.MESH
F32 = jnp.float32
BF16 = jnp.bfloat16


def halves(table):
    high = table.astype(jnp.bfloat16)
    low = (table - high.astype(np.float64)).astype(jnp.bfloat16)
    return high, low


def azimuth_table(first, count):
    angle = 2 * np.pi * (np.arange(64)[:, None] + 0.5) * (first + np.arange(count))[None, :] / 128
    high, low = halves(np.concatenate([np.cos(angle), -np.sin(angle)], axis=0))
    return np.concatenate([high, high, low], axis=1)


def box_table():
    cell = np.arange(256)[:, None]
    lag = np.arange(128)[None, :]
    return ((cell >= lag) & (cell < lag + 128)).astype(jnp.bfloat16)


def column_tables():
    angle = 2 * np.pi * np.arange(64)[:, None] * np.arange(128)[None, :] / 128
    c, s = np.cos(angle), np.sin(angle)
    sign = np.where(np.arange(256) % 2 == 0, 1.0, -1.0)[None, :]
    even = np.concatenate([np.concatenate([c, -s], 1), np.concatenate([s, c], 1)], 0)
    odd = np.concatenate([np.concatenate([s, c], 1), np.concatenate([c, -s], 1)], 0) * sign
    out = []
    for table in (even, odd):
        high, low = halves(table)
        out.append(np.concatenate([high, high, low], axis=0))
    return np.stack(out)


def back_tables():
    angle = 2 * np.pi * np.arange(64)[:, None] * (np.arange(64)[None, :] + 0.5) / 128
    c, s = np.cos(angle), np.sin(angle)
    high, low = halves(np.concatenate([np.concatenate([c, -s], 1), np.concatenate([s, c], 1)], 0))
    rows = np.concatenate([high, high, low], axis=1)
    angle = 2 * np.pi * np.arange(128)[:, None] * np.arange(64)[None, :] / 128
    high, low = halves(np.concatenate([np.cos(angle), -np.sin(angle)], 0) * (2.0 / AREA))
    none = np.zeros_like(high)
    first = np.concatenate([high, none, low, none], axis=1)
    second = np.concatenate([none, high, none, low], axis=1)
    return rows, np.stack([first, second])


def split(x):
    high = x.astype(BF16)
    return high, (x - high.astype(F32)).astype(BF16)


def dot(a, b):
    return jnp.dot(a, b, preferred_element_type=F32)


def shifted(x, shift, width):
    lane = lax.broadcasted_iota(jnp.int32, (x.shape[0], LANE), 1)
    turned = [
        pltpu.roll(x[:, i : i + LANE], LANE - shift, axis=1) for i in range(0, width + LANE, LANE)
    ]
    keep = lane < LANE - shift
    return jnp.concatenate(
        [jnp.where(keep, a, b) for a, b in zip(turned[:-1], turned[1:])], axis=1
    )


def range_spectra(rows_out, col_ref):
    lane = lax.broadcasted_iota(jnp.int32, (64, LANE), 1)
    low_half = lane < 64
    even, odd = [], []
    for x in rows_out:
        for i in range(0, x.shape[1], LANE):
            re = x[:64, i : i + LANE]
            im = pltpu.roll(x[64:, i : i + LANE], 64, axis=1)
            even.append(jnp.where(low_half, re, im))
            odd.append(jnp.where(low_half, im, re))
    out = []
    for parity, parts in enumerate((even, odd)):
        high, low = split(jnp.concatenate(parts, axis=0))
        got = dot(jnp.concatenate([high, low], axis=1), col_ref[parity, :256])
        got = got + dot(high, col_ref[parity, 256:])
        out.append(got)
    count = rows_out[0].shape[1] // LANE
    result = []
    for a in range(len(rows_out)):
        blocks = []
        for i in range(count):
            at = (a * count + i) * 64
            blocks += [out[0][at : at + 64], out[1][at : at + 64]]
        result.append(blocks)
    return result


def ones_where(condition):
    return jnp.where(condition, 1.0, 0.0).astype(BF16)


class Exchange:
    def __init__(self, tiles, bufs, tile_sems, send_sems, recv_sems):
        az, rg = lax.axis_index("az"), lax.axis_index("rg")
        last_az, last_rg = lax.axis_size("az") - 1, lax.axis_size("rg") - 1
        self.up = ("az", az - 1, az > 0)
        self.down = ("az", az + 1, az < last_az)
        self.left = ("rg", rg - 1, rg > 0)
        self.right = ("rg", rg + 1, rg < last_rg)
        self.sides = (self.up, self.down, self.left, self.right)
        self.bufs, self.send_sems, self.recv_sems, self.count = bufs, send_sems, recv_sems, 0
        self.all = []
        self.loads = []
        for i, (tile, (buf, halo)) in enumerate(zip(tiles, bufs)):
            own = buf.at[pl.ds(halo, ROWS), pl.ds(LANE, COLS)]
            self.loads.append(pltpu.make_async_copy(tile, own, tile_sems.at[i]))

    def greet(self):
        for load in self.loads:
            load.start()
        barrier = pltpu.get_barrier_semaphore()
        for axis, place, there in self.sides:

            @pl.when(there)
            def _(axis=axis, place=place):
                pl.semaphore_signal(barrier, inc=1, device_id={axis: place}, device_id_type=MESH)

    def clear(self):
        up, down, left, right = self.sides
        for buf, halo in self.bufs:
            for side, rows, lanes in (
                (up, slice(0, halo), slice(None)),
                (down, slice(halo + ROWS, 2 * halo + ROWS), slice(None)),
                (left, slice(None), slice(0, LANE)),
                (right, slice(None), slice(LANE + COLS, 2 * LANE + COLS)),
            ):

                @pl.when(jnp.logical_not(side[2]))
                def _(buf=buf, rows=rows, lanes=lanes):
                    shape = [n if c == slice(None) else c.stop - c.start for n, c in zip(buf.shape, (rows, lanes))]
                    buf[rows, lanes] = jnp.zeros(shape, F32)

    def meet(self):
        barrier = pltpu.get_barrier_semaphore()
        peers = sum(there.astype(jnp.int32) for _, _, there in self.sides)
        pl.semaphore_wait(barrier, peers)

    def copy(self, buf, rows, lanes, to_rows, to_lanes, side, back, have=None):
        index = self.count
        self.count += 1
        axis, place, sends = side
        comes = back[2]
        if have is not None:
            sends, comes = sends & have, comes & have
        transfer = pltpu.make_async_remote_copy(
            src_ref=buf.at[pl.ds(*rows), pl.ds(*lanes)],
            dst_ref=buf.at[pl.ds(*to_rows), pl.ds(*to_lanes)],
            send_sem=self.send_sems.at[index],
            recv_sem=self.recv_sems.at[index],
            device_id={axis: place},
            device_id_type=MESH,
        )
        entry = (transfer, sends, comes)
        self.all.append(entry)
        return entry

    def along_azimuth(self, buf, halo, near, far, lanes):
        count = far - near
        end = halo + ROWS
        return [
            self.copy(buf, (halo + near, count), lanes, (end + near, count), lanes, self.up, self.down),
            self.copy(buf, (end - far, count), lanes, (halo - far, count), lanes, self.down, self.up),
        ]

    def along_range(self, buf, rows, have=None):
        return [
            self.copy(buf, rows, (LANE, LANE), rows, (LANE + COLS, LANE), self.left, self.right, have),
            self.copy(buf, rows, (COLS, LANE), rows, (0, LANE), self.right, self.left, have),
        ]

    def corners(self, buf, halo, near, far):
        count = far - near
        return self.along_range(buf, (halo - far, count), self.up[2]) + self.along_range(
            buf, (halo + ROWS + near, count), self.down[2]
        )

    @staticmethod
    def start(entries):
        for transfer, sends, _ in entries:

            @pl.when(sends)
            def _(transfer=transfer):
                transfer.start()

    @staticmethod
    def arrive(entries):
        for transfer, _, comes in entries:

            @pl.when(comes)
            def _(transfer=transfer):
                transfer.wait_recv()

    def close(self):
        for transfer, sends, _ in self.all:

            @pl.when(sends)
            def _(transfer=transfer):
                transfer.wait_send()


def kernel(off_az_hbm, off_rg_hbm, ref_tile, sec_tile, *refs):
    table_hbm, score_ref, tables = refs[:6], refs[6], refs[7:13]
    ref_row_ref, sec_row_ref, col_ref, back_row_ref, back_col_ref, box_col_ref = tables
    off_az, off_rg, ref_buf, sec_buf, row_mats, box_mid, box_far = refs[13:20]
    sec_high, sec_low, square_high, square_low = refs[20:24]
    quads, windows, strips, boxes, stats, tile_sems, table_sems, send_sems, recv_sems = refs[24:]
    halo = Exchange(
        (ref_tile, sec_tile),
        ((ref_buf, REF_HALO), (sec_buf, ROW_HALO)),
        tile_sems,
        send_sems,
        recv_sems,
    )
    everything = (LANE, COLS)
    near = halo.along_azimuth(sec_buf, ROW_HALO, 0, NEAR, everything)
    beside = halo.along_range(sec_buf, (ROW_HALO, ROWS)) + halo.along_range(ref_buf, (REF_HALO, ROWS))
    order = (1, 6, 2, 3, 4, 5)
    sec_far, ref_far = {}, {}
    for b in order:
        lanes = (LANE * b, LANE)
        sec_far[b] = halo.along_azimuth(sec_buf, ROW_HALO, NEAR, ROW_HALO, lanes)
        ref_far[b] = halo.along_azimuth(ref_buf, REF_HALO, 0, REF_HALO, lanes)
    near_corners = halo.corners(sec_buf, ROW_HALO, 0, NEAR)
    sec_corners = halo.corners(sec_buf, ROW_HALO, NEAR, ROW_HALO)
    ref_corners = halo.corners(ref_buf, REF_HALO, 0, REF_HALO)

    halo.greet()
    fetches = [
        pltpu.make_async_copy(source, target, table_sems.at[i])
        for i, (source, target) in enumerate(
            zip((off_az_hbm, off_rg_hbm) + table_hbm, (off_az, off_rg) + tables)
        )
    ]
    for fetch in fetches:
        fetch.start()
    halo.clear()
    for load in halo.loads:
        load.wait()
    halo.meet()
    halo.start(near)
    halo.start(beside)
    halo.start(sec_far[1] + sec_far[6])
    halo.start(ref_far[1] + ref_far[6])
    for b in order[2:]:
        halo.start(sec_far[b] + ref_far[b])

    own = pl.ds(LANE, COLS)
    ref_mean = jnp.mean(ref_buf[pl.ds(REF_HALO, ROWS), own], keepdims=True)
    sec_mean = jnp.mean(sec_buf[pl.ds(ROW_HALO, ROWS), own], keepdims=True)

    for fetch in fetches:
        fetch.wait()
    lane = lax.broadcasted_iota(jnp.int32, (128, LANE), 1)
    for k in range(2):
        first = NEAR + off_az[k]
        for m in range(2):
            turned = [
                pltpu.roll(sec_row_ref[k + m, :, i : i + LANE], first, axis=1)
                for i in range(0, 512, LANE)
            ]
            moved = [jnp.where(lane < first, turned[i - 1], turned[i]) for i in range(4)]
            row_mats[k, m] = jnp.concatenate(moved, axis=1)[:, : 3 * REACH].astype(BF16)
        lag = lax.broadcasted_iota(jnp.int32, (64, 2 * REACH), 0)
        cell = lax.broadcasted_iota(jnp.int32, (64, 2 * REACH), 1)
        cell = jnp.where(cell < REACH, cell, cell - REACH) + (64 - 64 * k) - first - lag
        box_mid[k] = ones_where((cell >= 0) & (cell < CHIP))
        lag = lax.broadcasted_iota(jnp.int32, (64, 2 * FAR), 0)
        cell = lax.broadcasted_iota(jnp.int32, (64, 2 * FAR), 1)
        cell = jnp.where(cell < FAR, cell, cell - FAR) + REACH * k - first - lag
        box_far[k] = ones_where((cell >= 0) & (cell < CHIP))

    def reference_lines(m, pairs):
        parts = [ref_buf[64 * m : 64 * m + 64, LANE * p : LANE * p + 256] for p in pairs]
        parts = [shifted(x, LANE - REF_HALO, LANE) - ref_mean for x in parts]
        for p, x in zip(pairs, parts):
            place = pl.ds(LANE * p, LANE)
            stats[2 * m : 2 * m + 1, place] = jnp.sum(x, axis=0, keepdims=True)
            stats[2 * m + 1 : 2 * m + 2, place] = jnp.sum(x * x, axis=0, keepdims=True)
        high, low = split(jnp.concatenate(parts, axis=1))
        return dot(ref_row_ref[m], jnp.concatenate([high, low, high], axis=0))

    def take_lines(k, spans, pairs):
        for p in pairs:
            place = slice(LANE * p, LANE * p + LANE)
            for first, count in spans:
                rows = slice(first, first + count)
                x = shifted(sec_buf[rows, LANE * p : LANE * p + 256], 64 + off_rg[k], LANE) - sec_mean
                sec_high[k, rows, place], sec_low[k, rows, place] = split(x)
                square_high[k, rows, place], square_low[k, rows, place] = split(x * x)

    def box_lines(k, first, count, p, box_ref):
        rows, place = slice(first, first + count), slice(LANE * p, LANE * p + LANE)
        stack = jnp.concatenate(
            [
                jnp.concatenate([sec_high[k, rows, place], square_high[k, rows, place]], axis=1),
                jnp.concatenate([sec_low[k, rows, place], square_low[k, rows, place]], axis=1),
            ],
            axis=0,
        )
        return dot(box_ref[k], stack)

    def window_transform(k, m, pairs):
        rows = slice(64 * (k + m), 64 * (k + m) + REACH)
        high = jnp.concatenate([sec_high[k, rows, LANE * p : LANE * p + LANE] for p in pairs], axis=1)
        low = jnp.concatenate([sec_low[k, rows, LANE * p : LANE * p + LANE] for p in pairs], axis=1)
        return dot(row_mats[k, m], jnp.concatenate([high, low, high], axis=0))

    def store(target, pairs, blocks):
        for i, p in enumerate(pairs):
            for half in range(2):
                target[2 * p + half] = blocks[2 * i + half]

    def middle_quadrants(*groups):
        rows_out = [reference_lines(1, pairs) for pairs in groups]
        for pairs, x in zip(groups, rows_out):
            store(quads.at[1], pairs, range_spectra([x], col_ref)[0])

    def middle_windows(*groups):
        rows_out = [[window_transform(k, 1 - k, pairs) for k in range(2)] for pairs in groups]
        for pairs in groups:
            for k in range(2):
                for p in pairs:
                    sums = box_lines(k, 64, REACH, p, box_mid)
                    boxes[k, :64, LANE * p : LANE * p + LANE] = sums[:, :128]
                    boxes[k, 64:, LANE * p : LANE * p + LANE] = sums[:, 128:]
        for pairs, x in zip(groups, rows_out):
            got = range_spectra(x, col_ref)
            store(windows.at[0, 1], pairs, got[0])
            store(windows.at[1, 0], pairs, got[1])

    def outer(*groups):
        for pairs in groups:
            take_lines(0, ((0, FAR),), pairs)
            take_lines(1, ((224, FAR),), pairs)
        rows_out = [
            [window_transform(k, k, pairs) for k in range(2)]
            + [reference_lines(m, pairs) for m in (0, 2)]
            for pairs in groups
        ]
        for pairs in groups:
            for k in range(2):
                for p in pairs:
                    sums = box_lines(k, 224 * k, FAR, p, box_far)
                    boxes[k, :64, LANE * p : LANE * p + LANE] += sums[:, :128]
                    boxes[k, 64:, LANE * p : LANE * p + LANE] += sums[:, 128:]
        for pairs, x in zip(groups, rows_out):
            got = range_spectra(x, col_ref)
            store(windows.at[0, 0], pairs, got[0])
            store(windows.at[1, 1], pairs, got[1])
            store(quads.at[0], pairs, got[2])
            store(quads.at[2], pairs, got[3])

    def product(k, m, n):
        q = quads[k + m, n]
        x = windows[k, m, n] + windows[k, m, n + 1]
        qr, qi, xr, xi = q[:, :128], q[:, 128:], x[:, :128], x[:, 128:]
        return jnp.concatenate([qr * xr + qi * xi, qr * xi - qi * xr], axis=0)

    def middle_strips(*numbers):
        for n in numbers:
            for k in range(2):
                strips[k, n] = product(k, 1 - k, n)

    done = {}

    def strip(k, n):
        if (k, n) not in done:
            done[k, n] = True
            strips[k, n] += product(k, k, n)
        return strips[k, n]

    def finish(*pairs):
        items = [(k, s) for s in pairs for k in range(2)]
        moments = {}
        for s in pairs:
            stat = stats[:, s * LANE : s * LANE + 256]
            place = lax.broadcasted_iota(jnp.int32, stat.shape, 1)
            a = jnp.sum(stat[:, :128], axis=1, keepdims=True)
            b = jnp.sum(jnp.where((place >= 64) & (place < 192), stat, 0.0), axis=1, keepdims=True)
            moments[s] = jnp.where(place[:, :128] < 64, a, b)
        sums = {(k, n): strip(k, n) for k, s in items for n in range(2 * s, 2 * s + 3)}
        inner = {}
        for k, s in items:
            left, middle_, right = [sums[k, 2 * s + i] for i in range(3)]
            high, low = split(jnp.concatenate([left + middle_, middle_ + right], axis=1))
            y = dot(back_row_ref[:, :256], jnp.concatenate([high, low], axis=0))
            inner[k, s] = y + dot(back_row_ref[:, 256:], high)
        for k, s in items:
            y = inner[k, s]
            corr = 0.0
            for i in range(2):
                lanes = slice(LANE * i, LANE * i + LANE)
                high, low = split(jnp.concatenate([y[:64, lanes], y[64:, lanes]], axis=1))
                wide = dot(high, back_col_ref[i])
                corr = corr + (wide[:, :128] + wide[:, 128:]) + dot(low, back_col_ref[i, :, :128])
            high, low = split(boxes[k, :, s * LANE : s * LANE + 256])
            box = dot(high, box_col_ref[...]) + dot(low, box_col_ref[...])
            first, second = box[:64], box[64:]
            both = moments[s]
            total = both[2 * k : 2 * k + 1] + both[2 * k + 2 : 2 * k + 3]
            power = both[2 * k + 1 : 2 * k + 2] + both[2 * k + 3 : 2 * k + 4]
            mean = total / AREA
            energy = power - total * mean
            centered = corr - mean * first
            var_sum = jnp.maximum(second - first * first / AREA, 0.0)
            score_ref[k, s] = (CHIP / AREA) * centered * lax.rsqrt(
                (energy / AREA) * (var_sum / AREA) + EPSILON
            )

    inside = (1, 2, 3, 4, 5)
    near_lines = ((ROW_HALO - NEAR, NEAR), (ROW_HALO + ROWS, NEAR))
    middle_quadrants((1, 2), (3, 4), (5,))
    for k in range(2):
        take_lines(k, ((ROW_HALO, ROWS),), inside)
    halo.arrive(near)
    halo.start(near_corners)
    for k in range(2):
        take_lines(k, near_lines, inside)
    middle_windows((1, 2), (3, 4), (5,))
    halo.arrive(sec_far[1])
    halo.start(sec_corners[0::2])
    halo.arrive(sec_far[6])
    halo.start(sec_corners[1::2])
    halo.arrive(beside)
    middle_quadrants((0, 6))
    halo.arrive(ref_far[1] + ref_far[6])
    halo.start(ref_corners)
    halo.arrive(near_corners)
    for k in range(2):
        take_lines(k, near_lines + ((ROW_HALO, ROWS),), (0, 6))
    middle_windows((0, 6))
    middle_strips(*range(BLOCKS - 1))
    halo.arrive(sec_far[2] + ref_far[2])
    halo.arrive(sec_far[3] + ref_far[3])
    outer((1, 2))
    halo.arrive(sec_far[4] + ref_far[4])
    outer((3,))
    finish(1, 2)
    halo.arrive(sec_corners + ref_corners)
    halo.arrive(sec_far[5] + ref_far[5])
    outer((4, 5), (0, 6))
    finish(0, 3, 4, 5)
    halo.close()


def oversample(score_ref, out_ref, staged, sem):
    def cubic(out_index, sample):
        base = out_index // 2

        def pick(step):
            return jnp.where(jnp.clip(base + step, 0, LAGS - 1) == sample, 1.0, 0.0)

        odd = (9.0 * (pick(0) + pick(1)) - (pick(-1) + pick(2))) / 16.0
        return jnp.where(out_index % 2 == 1, odd, pick(0))

    row = lax.broadcasted_iota(jnp.int32, (128, 128), 0)
    lane = lax.broadcasted_iota(jnp.int32, (128, 128), 1)
    left = cubic(row, lane % LAGS).astype(BF16)
    right = cubic(lane, row % LAGS)
    right = jnp.concatenate(
        [jnp.where(row < LAGS, right, 0.0), jnp.where(row < LAGS, 0.0, right)], axis=1
    ).astype(BF16)
    items = [(k, s) for k in range(2) for s in range(PAIRS)]
    for some in (items[:4], items[4:8], items[8:]):
        lifted = []
        for k, s in some:
            high, low = split(score_ref[k, s])
            lifted.append(dot(left, jnp.concatenate([high, low], axis=0)))
        for (k, s), value in zip(some, lifted):
            high, low = split(value)
            wide = dot(high, right) + dot(low, right)
            at = k * CHIPS + 2 * s
            staged[at] = wide[:, :128]
            staged[at + 1] = wide[:, 128:]
        for k, s in some:
            part = pl.ds(k * CHIPS + 2 * s, 2)
            pltpu.make_async_copy(staged.at[part], out_ref.at[part], sem).start()
    pltpu.make_async_copy(staged, out_ref, sem).wait()


def spread(table):
    room = np.zeros((128, REACH - 128))
    parts = [np.concatenate([table[:, i : i + 128].astype(np.float64), room], 1) for i in (0, 128, 256)]
    return np.concatenate(parts + [room], axis=1).astype(np.float32)


def body(ref_image, sec_image, off_az, off_rg):
    back_rows, back_cols = back_tables()
    tables = [
        np.stack([azimuth_table(64 * m, 64) for m in range(3)]),
        np.stack([spread(azimuth_table(64 * j, 128)) for j in range(3)]),
        column_tables(),
        back_rows,
        back_cols,
        box_table(),
    ]
    anywhere = pl.BlockSpec(memory_space=pl.ANY)
    vmem = pl.BlockSpec(memory_space=pltpu.VMEM)
    scores = pl.pallas_call(
        kernel,
        out_shape=pltpu.VMEM((2, PAIRS, LAGS, 2 * LAGS), F32),
        in_specs=[pl.BlockSpec(memory_space=pltpu.HBM)] * (4 + len(tables)),
        out_specs=vmem,
        scratch_shapes=[pltpu.VMEM(t.shape, t.dtype) for t in tables]
        + [
            pltpu.SMEM((2,), jnp.int32),
            pltpu.SMEM((2,), jnp.int32),
            pltpu.VMEM((ROWS + 2 * REF_HALO, COLS + 2 * LANE), F32),
            pltpu.VMEM((ROWS + 2 * ROW_HALO, COLS + 2 * LANE), F32),
            pltpu.VMEM((2, 2, 128, 3 * REACH), BF16),
            pltpu.VMEM((2, 64, 2 * REACH), BF16),
            pltpu.VMEM((2, 64, 2 * FAR), BF16),
        ]
        + [pltpu.VMEM((2, ROWS + 2 * ROW_HALO, WIDE), BF16)] * 4
        + [
            pltpu.VMEM((3, BLOCKS, 64, 256), F32),
            pltpu.VMEM((2, 2, BLOCKS, 64, 256), F32),
            pltpu.VMEM((2, BLOCKS - 1, 128, 128), F32),
            pltpu.VMEM((2, 128, WIDE), F32),
            pltpu.VMEM((8, WIDE), F32),
            pltpu.SemaphoreType.DMA((2,)),
            pltpu.SemaphoreType.DMA((8,)),
            pltpu.SemaphoreType.DMA((48,)),
            pltpu.SemaphoreType.DMA((48,)),
        ],
        compiler_params=pltpu.CompilerParams(
            collective_id=0, has_side_effects=True
        ),
    )(off_az, off_rg, ref_image, sec_image, *[jnp.asarray(t) for t in tables])
    out = pl.pallas_call(
        oversample,
        out_shape=jax.ShapeDtypeStruct((2 * CHIPS, 128, 128), F32),
        in_specs=[vmem],
        out_specs=anywhere,
        scratch_shapes=[pltpu.VMEM((2 * CHIPS, 128, 128), F32), pltpu.SemaphoreType.DMA],
        compiler_params=pltpu.CompilerParams(vmem_limit_bytes=8 << 20),
    )(scores)
    return out.reshape(2, CHIPS, 128, 128)


def solution(mesh):
    return jax.shard_map(
        body,
        mesh=mesh,
        in_specs=(P("az", "rg"), P("az", "rg"), P("az"), P("az")),
        out_specs=P("az", "rg", None, None),
        check_vma=False,
    )
```

```python
import functools

import jax
import jax.numpy as jnp
import numpy as np
from jax import lax
from jax.experimental import pallas as pl
from jax.experimental.pallas import tpu as pltpu
from jax.sharding import PartitionSpec as P

CHIP = 128
SPACE = 64
LAGS = 64
AREA = float(CHIP * CHIP)
EPSILON = 1e-06
ROWS = 128
COLS = 768
CHIPS = COLS // SPACE
PAIRS = CHIPS // 2
BLOCKS = CHIPS + 2
WIDE = BLOCKS * SPACE
ROW_HALO = 80
REF_HALO = 32
NEAR = 16
FAR = 64
REACH = 160
LANE = 128
MESH = pl.DeviceIdType.MESH
F32 = jnp.float32
BF16 = jnp.bfloat16


def halves(table):
    high = table.astype(jnp.bfloat16)
    low = (table - high.astype(np.float64)).astype(jnp.bfloat16)
    return high, low


def azimuth_table(first, count):
    angle = 2 * np.pi * (np.arange(64)[:, None] + 0.5) * (first + np.arange(count))[None, :] / 128
    high, low = halves(np.concatenate([np.cos(angle), -np.sin(angle)], axis=0))
    return np.concatenate([high, high, low], axis=1)


def box_table():
    cell = np.arange(256)[:, None]
    lag = np.arange(128)[None, :]
    return ((cell >= lag) & (cell < lag + 128)).astype(jnp.bfloat16)


def column_tables():
    angle = 2 * np.pi * np.arange(64)[:, None] * np.arange(128)[None, :] / 128
    c, s = np.cos(angle), np.sin(angle)
    sign = np.where(np.arange(256) % 2 == 0, 1.0, -1.0)[None, :]
    even = np.concatenate([np.concatenate([c, -s], 1), np.concatenate([s, c], 1)], 0)
    odd = np.concatenate([np.concatenate([s, c], 1), np.concatenate([c, -s], 1)], 0) * sign
    out = []
    for table in (even, odd):
        high, low = halves(table)
        out.append(np.concatenate([high, high, low], axis=0))
    return np.stack(out)


def back_tables():
    angle = 2 * np.pi * np.arange(64)[:, None] * (np.arange(64)[None, :] + 0.5) / 128
    c, s = np.cos(angle), np.sin(angle)
    high, low = halves(np.concatenate([np.concatenate([c, -s], 1), np.concatenate([s, c], 1)], 0))
    rows = np.concatenate([high, high, low], axis=1)
    angle = 2 * np.pi * np.arange(128)[:, None] * np.arange(64)[None, :] / 128
    high, low = halves(np.concatenate([np.cos(angle), -np.sin(angle)], 0) * (2.0 / AREA))
    none = np.zeros_like(high)
    first = np.concatenate([high, none, low, none], axis=1)
    second = np.concatenate([none, high, none, low], axis=1)
    return rows, np.stack([first, second])


def split(x):
    high = x.astype(BF16)
    return high, (x - high.astype(F32)).astype(BF16)


def dot(a, b):
    return jnp.dot(a, b, preferred_element_type=F32)


def shifted(x, shift, width):
    lane = lax.broadcasted_iota(jnp.int32, (x.shape[0], LANE), 1)
    turned = [
        pltpu.roll(x[:, i : i + LANE], LANE - shift, axis=1) for i in range(0, width + LANE, LANE)
    ]
    keep = lane < LANE - shift
    return jnp.concatenate(
        [jnp.where(keep, a, b) for a, b in zip(turned[:-1], turned[1:])], axis=1
    )


def range_spectra(rows_out, col_ref):
    lane = lax.broadcasted_iota(jnp.int32, (64, LANE), 1)
    low_half = lane < 64
    even, odd = [], []
    for x in rows_out:
        for i in range(0, x.shape[1], LANE):
            re = x[:64, i : i + LANE]
            im = pltpu.roll(x[64:, i : i + LANE], 64, axis=1)
            even.append(jnp.where(low_half, re, im))
            odd.append(jnp.where(low_half, im, re))
    out = []
    for parity, parts in enumerate((even, odd)):
        high, low = split(jnp.concatenate(parts, axis=0))
        got = dot(jnp.concatenate([high, low], axis=1), col_ref[parity, :256])
        got = got + dot(high, col_ref[parity, 256:])
        out.append(got)
    count = rows_out[0].shape[1] // LANE
    result = []
    for a in range(len(rows_out)):
        blocks = []
        for i in range(count):
            at = (a * count + i) * 64
            blocks += [out[0][at : at + 64], out[1][at : at + 64]]
        result.append(blocks)
    return result


def ones_where(condition):
    return jnp.where(condition, 1.0, 0.0).astype(BF16)


class Exchange:
    def __init__(self, tiles, bufs, tile_sems, send_sems, recv_sems):
        az, rg = lax.axis_index("az"), lax.axis_index("rg")
        last_az, last_rg = lax.axis_size("az") - 1, lax.axis_size("rg") - 1
        self.up = ("az", az - 1, az > 0)
        self.down = ("az", az + 1, az < last_az)
        self.left = ("rg", rg - 1, rg > 0)
        self.right = ("rg", rg + 1, rg < last_rg)
        self.sides = (self.up, self.down, self.left, self.right)
        self.bufs, self.send_sems, self.recv_sems, self.count = bufs, send_sems, recv_sems, 0
        self.all = []
        self.loads = []
        for i, (tile, (buf, halo)) in enumerate(zip(tiles, bufs)):
            own = buf.at[pl.ds(halo, ROWS), pl.ds(LANE, COLS)]
            self.loads.append(pltpu.make_async_copy(tile, own, tile_sems.at[i]))

    def greet(self):
        for load in self.loads:
            load.start()
        barrier = pltpu.get_barrier_semaphore()
        for axis, place, there in self.sides:

            @pl.when(there)
            def _(axis=axis, place=place):
                pl.semaphore_signal(barrier, inc=1, device_id={axis: place}, device_id_type=MESH)

    def clear(self):
        up, down, left, right = self.sides
        for buf, halo in self.bufs:
            for side, rows, lanes in (
                (up, slice(0, halo), slice(None)),
                (down, slice(halo + ROWS, 2 * halo + ROWS), slice(None)),
                (left, slice(None), slice(0, LANE)),
                (right, slice(None), slice(LANE + COLS, 2 * LANE + COLS)),
            ):

                @pl.when(jnp.logical_not(side[2]))
                def _(buf=buf, rows=rows, lanes=lanes):
                    shape = [n if c == slice(None) else c.stop - c.start for n, c in zip(buf.shape, (rows, lanes))]
                    buf[rows, lanes] = jnp.zeros(shape, F32)

    def meet(self):
        barrier = pltpu.get_barrier_semaphore()
        peers = sum(there.astype(jnp.int32) for _, _, there in self.sides)
        pl.semaphore_wait(barrier, peers)

    def copy(self, buf, rows, lanes, to_rows, to_lanes, side, back, have=None):
        index = self.count
        self.count += 1
        axis, place, sends = side
        comes = back[2]
        if have is not None:
            sends, comes = sends & have, comes & have
        transfer = pltpu.make_async_remote_copy(
            src_ref=buf.at[pl.ds(*rows), pl.ds(*lanes)],
            dst_ref=buf.at[pl.ds(*to_rows), pl.ds(*to_lanes)],
            send_sem=self.send_sems.at[index],
            recv_sem=self.recv_sems.at[index],
            device_id={axis: place},
            device_id_type=MESH,
        )
        entry = (transfer, sends, comes)
        self.all.append(entry)
        return entry

    def along_azimuth(self, buf, halo, near, far, lanes):
        count = far - near
        end = halo + ROWS
        return [
            self.copy(buf, (halo + near, count), lanes, (end + near, count), lanes, self.up, self.down),
            self.copy(buf, (end - far, count), lanes, (halo - far, count), lanes, self.down, self.up),
        ]

    def along_range(self, buf, rows, have=None):
        return [
            self.copy(buf, rows, (LANE, LANE), rows, (LANE + COLS, LANE), self.left, self.right, have),
            self.copy(buf, rows, (COLS, LANE), rows, (0, LANE), self.right, self.left, have),
        ]

    def corners(self, buf, halo, near, far):
        count = far - near
        return self.along_range(buf, (halo - far, count), self.up[2]) + self.along_range(
            buf, (halo + ROWS + near, count), self.down[2]
        )

    @staticmethod
    def start(entries, given=True):
        for transfer, sends, _ in entries:

            @pl.when(sends & given)
            def _(transfer=transfer):
                transfer.start()

    @staticmethod
    def arrive(entries, given=True):
        for transfer, _, comes in entries:

            @pl.when(comes & given)
            def _(transfer=transfer):
                transfer.wait_recv()

    def close(self):
        for transfer, sends, _ in self.all:

            @pl.when(sends)
            def _(transfer=transfer):
                transfer.wait_send()


def kernel(off_az_hbm, off_rg_hbm, ref_tile, sec_tile, *refs):
    table_hbm, score_ref, tables = refs[:6], refs[6], refs[7:13]
    ref_row_ref, sec_row_ref, col_ref, back_row_ref, back_col_ref, box_col_ref = tables
    off_az, off_rg, ref_buf, sec_buf, row_mats, box_mid, box_far = refs[13:20]
    sec_high, sec_low, square_high, square_low = refs[20:24]
    quads, windows, strips, boxes, stats, tile_sems, table_sems, send_sems, recv_sems = refs[24:]
    halo = Exchange(
        (ref_tile, sec_tile),
        ((ref_buf, REF_HALO), (sec_buf, ROW_HALO)),
        tile_sems,
        send_sems,
        recv_sems,
    )
    everything = (LANE, COLS)
    near = halo.along_azimuth(sec_buf, ROW_HALO, 0, NEAR, everything)
    beside = halo.along_range(sec_buf, (ROW_HALO, ROWS)) + halo.along_range(ref_buf, (REF_HALO, ROWS))
    order = (1, 6, 2, 3, 4, 5)
    sec_far, ref_far = {}, {}
    for b in order:
        lanes = (LANE * b, LANE)
        sec_far[b] = halo.along_azimuth(sec_buf, ROW_HALO, NEAR, ROW_HALO, lanes)
        ref_far[b] = halo.along_azimuth(ref_buf, REF_HALO, 0, REF_HALO, lanes)
    near_corners = halo.corners(sec_buf, ROW_HALO, 0, NEAR)
    sec_corners = halo.corners(sec_buf, ROW_HALO, NEAR, ROW_HALO)
    ref_corners = halo.corners(ref_buf, REF_HALO, 0, REF_HALO)

    corners = sec_corners + ref_corners

    def forward(step):
        for given, edges in cores:
            b = edges[step]
            halo.arrive(sec_far[b] + ref_far[b], given)
            halo.start(corners[0::2] if b == 1 else corners[1::2], given)

    halo.greet()
    fetches = [
        pltpu.make_async_copy(source, target, table_sems.at[i])
        for i, (source, target) in enumerate(
            zip((off_az_hbm, off_rg_hbm) + table_hbm, (off_az, off_rg) + tables)
        )
    ]
    for fetch in fetches:
        fetch.start()
    for load in halo.loads:
        load.wait()
    halo.meet()
    halo.start(near)
    halo.start(beside)
    second = lax.rem(lax.axis_index("rg"), 2) == 1
    cores = ((jnp.logical_not(second), (1, 6)), (second, (6, 1)))
    for given, edges in cores:
        for b in edges:
            halo.start(sec_far[b] + ref_far[b], given)
    for b in order[2:]:
        halo.start(sec_far[b] + ref_far[b])

    halo.clear()
    own = pl.ds(LANE, COLS)
    ref_mean = jnp.mean(ref_buf[pl.ds(REF_HALO, ROWS), own], keepdims=True)
    sec_mean = jnp.mean(sec_buf[pl.ds(ROW_HALO, ROWS), own], keepdims=True)

    for fetch in fetches:
        fetch.wait()
    lane = lax.broadcasted_iota(jnp.int32, (128, LANE), 1)
    for k in range(2):
        first = NEAR + off_az[k]
        for m in range(2):
            turned = [
                pltpu.roll(sec_row_ref[k + m, :, i : i + LANE], first, axis=1)
                for i in range(0, 512, LANE)
            ]
            moved = [jnp.where(lane < first, turned[i - 1], turned[i]) for i in range(4)]
            row_mats[k, m] = jnp.concatenate(moved, axis=1)[:, : 3 * REACH].astype(BF16)
        lag = lax.broadcasted_iota(jnp.int32, (64, 2 * REACH), 0)
        cell = lax.broadcasted_iota(jnp.int32, (64, 2 * REACH), 1)
        cell = jnp.where(cell < REACH, cell, cell - REACH) + (64 - 64 * k) - first - lag
        box_mid[k] = ones_where((cell >= 0) & (cell < CHIP))
        lag = lax.broadcasted_iota(jnp.int32, (64, 2 * FAR), 0)
        cell = lax.broadcasted_iota(jnp.int32, (64, 2 * FAR), 1)
        cell = jnp.where(cell < FAR, cell, cell - FAR) + REACH * k - first - lag
        box_far[k] = ones_where((cell >= 0) & (cell < CHIP))

    def reference_lines(m, pairs):
        parts = [ref_buf[64 * m : 64 * m + 64, LANE * p : LANE * p + 256] for p in pairs]
        parts = [shifted(x, LANE - REF_HALO, LANE) - ref_mean for x in parts]
        for p, x in zip(pairs, parts):
            place = pl.ds(LANE * p, LANE)
            stats[2 * m : 2 * m + 1, place] = jnp.sum(x, axis=0, keepdims=True)
            stats[2 * m + 1 : 2 * m + 2, place] = jnp.sum(x * x, axis=0, keepdims=True)
        high, low = split(jnp.concatenate(parts, axis=1))
        return dot(ref_row_ref[m], jnp.concatenate([high, low, high], axis=0))

    def take_lines(k, spans, pairs):
        for p in pairs:
            place = slice(LANE * p, LANE * p + LANE)
            for first, count in spans:
                rows = slice(first, first + count)
                x = shifted(sec_buf[rows, LANE * p : LANE * p + 256], 64 + off_rg[k], LANE) - sec_mean
                sec_high[k, rows, place], sec_low[k, rows, place] = split(x)
                square_high[k, rows, place], square_low[k, rows, place] = split(x * x)

    def box_lines(k, first, count, p, box_ref):
        rows, place = slice(first, first + count), slice(LANE * p, LANE * p + LANE)
        stack = jnp.concatenate(
            [
                jnp.concatenate([sec_high[k, rows, place], square_high[k, rows, place]], axis=1),
                jnp.concatenate([sec_low[k, rows, place], square_low[k, rows, place]], axis=1),
            ],
            axis=0,
        )
        return dot(box_ref[k], stack)

    def window_transform(k, m, pairs):
        rows = slice(64 * (k + m), 64 * (k + m) + REACH)
        high = jnp.concatenate([sec_high[k, rows, LANE * p : LANE * p + LANE] for p in pairs], axis=1)
        low = jnp.concatenate([sec_low[k, rows, LANE * p : LANE * p + LANE] for p in pairs], axis=1)
        return dot(row_mats[k, m], jnp.concatenate([high, low, high], axis=0))

    def store(target, pairs, blocks):
        for i, p in enumerate(pairs):
            for half in range(2):
                target[2 * p + half] = blocks[2 * i + half]

    def middle_quadrants(*groups):
        rows_out = [reference_lines(1, pairs) for pairs in groups]
        for pairs, x in zip(groups, rows_out):
            store(quads.at[1], pairs, range_spectra([x], col_ref)[0])

    def middle_windows(*groups):
        rows_out = [[window_transform(k, 1 - k, pairs) for k in range(2)] for pairs in groups]
        for pairs in groups:
            for k in range(2):
                for p in pairs:
                    sums = box_lines(k, 64, REACH, p, box_mid)
                    boxes[k, :64, LANE * p : LANE * p + LANE] = sums[:, :128]
                    boxes[k, 64:, LANE * p : LANE * p + LANE] = sums[:, 128:]
        for pairs, x in zip(groups, rows_out):
            got = range_spectra(x, col_ref)
            store(windows.at[0, 1], pairs, got[0])
            store(windows.at[1, 0], pairs, got[1])

    def outer(for_windows, for_quadrants):
        for pairs in for_windows:
            take_lines(0, ((0, FAR),), pairs)
            take_lines(1, ((224, FAR),), pairs)
        rows_out = {}
        for pairs in for_windows:
            rows_out[pairs] = [(windows.at[k, k], window_transform(k, k, pairs)) for k in range(2)]
        for pairs in for_quadrants:
            found = [(quads.at[m], reference_lines(m, pairs)) for m in (0, 2)]
            rows_out[pairs] = rows_out.get(pairs, []) + found
        for pairs in for_windows:
            for k in range(2):
                for p in pairs:
                    sums = box_lines(k, 224 * k, FAR, p, box_far)
                    boxes[k, :64, LANE * p : LANE * p + LANE] += sums[:, :128]
                    boxes[k, 64:, LANE * p : LANE * p + LANE] += sums[:, 128:]
        for pairs, found in rows_out.items():
            got = range_spectra([x for _, x in found], col_ref)
            for (target, _), blocks in zip(found, got):
                store(target, pairs, blocks)

    def product(k, m, n):
        q = quads[k + m, n]
        x = windows[k, m, n] + windows[k, m, n + 1]
        qr, qi, xr, xi = q[:, :128], q[:, 128:], x[:, :128], x[:, 128:]
        return jnp.concatenate([qr * xr + qi * xi, qr * xi - qi * xr], axis=0)

    def middle_strips(*numbers):
        for n in numbers:
            for k in range(2):
                strips[k, n] = product(k, 1 - k, n)

    done = {}

    def strip(k, n):
        if (k, n) not in done:
            done[k, n] = True
            value = strips[k, n] + product(k, k, n)
            strips[k, n] = value
            return value
        return strips[k, n]

    def finish(*pairs):
        items = [(k, s) for s in pairs for k in range(2)]
        moments = {}
        for s in pairs:
            stat = stats[:, s * LANE : s * LANE + 256]
            place = lax.broadcasted_iota(jnp.int32, stat.shape, 1)
            a = jnp.sum(stat[:, :128], axis=1, keepdims=True)
            b = jnp.sum(jnp.where((place >= 64) & (place < 192), stat, 0.0), axis=1, keepdims=True)
            moments[s] = jnp.where(place[:, :128] < 64, a, b)
        sums = {(k, n): strip(k, n) for k, s in items for n in range(2 * s, 2 * s + 3)}
        inner = {}
        for k, s in items:
            left, middle_, right = [sums[k, 2 * s + i] for i in range(3)]
            high, low = split(jnp.concatenate([left + middle_, middle_ + right], axis=1))
            y = dot(back_row_ref[:, :256], jnp.concatenate([high, low], axis=0))
            inner[k, s] = y + dot(back_row_ref[:, 256:], high)
        corr = 0.0
        for i in range(2):
            lanes = slice(LANE * i, LANE * i + LANE)
            parts = [split(jnp.concatenate([inner[item][:64, lanes], inner[item][64:, lanes]], axis=1)) for item in items]
            wide = dot(jnp.concatenate([high for high, _ in parts], axis=0), back_col_ref[i])
            corr = corr + (wide[:, :128] + wide[:, 128:])
            corr = corr + dot(jnp.concatenate([low for _, low in parts], axis=0), back_col_ref[i, :, :128])
        parts = [split(boxes[k, :, s * LANE : s * LANE + 256]) for k, s in items]
        box = dot(jnp.concatenate([high for high, _ in parts], axis=0), box_col_ref[...])
        box = box + dot(jnp.concatenate([low for _, low in parts], axis=0), box_col_ref[...])
        for i, (k, s) in enumerate(items):
            first, second = box[128 * i : 128 * i + 64], box[128 * i + 64 : 128 * i + 128]
            both = moments[s]
            total = both[2 * k : 2 * k + 1] + both[2 * k + 2 : 2 * k + 3]
            power = both[2 * k + 1 : 2 * k + 2] + both[2 * k + 3 : 2 * k + 4]
            mean = total / AREA
            energy = power - total * mean
            centered = corr[64 * i : 64 * i + 64] - mean * first
            var_sum = jnp.maximum(second - first * first / AREA, 0.0)
            score_ref[k, s] = (CHIP / AREA) * centered * lax.rsqrt(
                (energy / AREA) * (var_sum / AREA) + EPSILON
            )

    inside = (1, 2, 3, 4, 5)
    near_lines = ((ROW_HALO - NEAR, NEAR), (ROW_HALO + ROWS, NEAR))
    middle_quadrants((1, 2), (3, 4), (5,))
    for k in range(2):
        take_lines(k, ((ROW_HALO, ROWS),), inside)
    halo.arrive(near)
    halo.start(near_corners)
    for k in range(2):
        take_lines(k, near_lines, inside)
    middle_windows((1, 2), (3, 4), (5,))
    forward(0)
    halo.arrive(beside)
    middle_quadrants((0, 6))
    forward(1)
    halo.arrive(near_corners)
    for k in range(2):
        take_lines(k, near_lines + ((ROW_HALO, ROWS),), (0, 6))
    middle_windows((0, 6))
    middle_strips(*range(BLOCKS - 1))
    halo.arrive(sec_far[2] + ref_far[2] + sec_far[3] + ref_far[3])
    outer([(1, 2)], [(1, 2)])
    halo.arrive(sec_far[4] + ref_far[4])
    outer([(3,)], [(3,)])
    halo.arrive(corners)
    halo.arrive(sec_far[5] + ref_far[5])
    outer([(4, 5), (0, 6)], [(4, 5), (0, 6)])
    finish(0, 1, 2, 3, 4, 5)
    halo.close()


def oversample(score_ref, out_ref, staged, sem):
    def cubic(out_index, sample):
        base = out_index // 2

        def pick(step):
            return jnp.where(jnp.clip(base + step, 0, LAGS - 1) == sample, 1.0, 0.0)

        odd = (9.0 * (pick(0) + pick(1)) - (pick(-1) + pick(2))) / 16.0
        return jnp.where(out_index % 2 == 1, odd, pick(0))

    row = lax.broadcasted_iota(jnp.int32, (128, 128), 0)
    lane = lax.broadcasted_iota(jnp.int32, (128, 128), 1)
    left = cubic(row, lane % LAGS).astype(BF16)
    right = cubic(lane, row % LAGS)
    right = jnp.concatenate(
        [jnp.where(row < LAGS, right, 0.0), jnp.where(row < LAGS, 0.0, right)], axis=1
    ).astype(BF16)
    right = jnp.concatenate([right, right], axis=0)
    items = [(k, s) for k in range(2) for s in range(PAIRS)]
    for first, last in ((0, 4), (4, 8), (8, 12)):
        lifted = []
        for i in range(first, last, 2):
            parts = [split(score_ref[k, s]) for k, s in items[i : i + 2]]
            high = jnp.concatenate([high for high, _ in parts], axis=1)
            low = jnp.concatenate([low for _, low in parts], axis=1)
            both = dot(left, jnp.concatenate([high, low], axis=0))
            lifted += [both[:, :LANE], both[:, LANE:]]
        for (k, s), value in zip(items[first:last], lifted):
            wide = dot(jnp.concatenate(split(value), axis=1), right)
            at = k * CHIPS + 2 * s
            staged[at] = wide[:, :128]
            staged[at + 1] = wide[:, 128:]
        part = pl.ds(2 * first, 2 * (last - first))
        pltpu.make_async_copy(staged.at[part], out_ref.at[part], sem).start()
    pltpu.make_async_copy(staged, out_ref, sem).wait()


def spread(table):
    room = np.zeros((128, REACH - 128))
    parts = [np.concatenate([table[:, i : i + 128].astype(np.float64), room], 1) for i in (0, 128, 256)]
    return np.concatenate(parts + [room], axis=1).astype(np.float32)


def body(ref_image, sec_image, off_az, off_rg):
    back_rows, back_cols = back_tables()
    tables = [
        np.stack([azimuth_table(64 * m, 64) for m in range(3)]),
        np.stack([spread(azimuth_table(64 * j, 128)) for j in range(3)]),
        column_tables(),
        back_rows,
        back_cols,
        box_table(),
    ]
    anywhere = pl.BlockSpec(memory_space=pl.ANY)
    vmem = pl.BlockSpec(memory_space=pltpu.VMEM)
    scores = pl.pallas_call(
        kernel,
        out_shape=pltpu.VMEM((2, PAIRS, LAGS, 2 * LAGS), F32),
        in_specs=[pl.BlockSpec(memory_space=pltpu.HBM)] * (4 + len(tables)),
        out_specs=vmem,
        scratch_shapes=[pltpu.VMEM(t.shape, t.dtype) for t in tables]
        + [
            pltpu.SMEM((2,), jnp.int32),
            pltpu.SMEM((2,), jnp.int32),
            pltpu.VMEM((ROWS + 2 * REF_HALO, COLS + 2 * LANE), F32),
            pltpu.VMEM((ROWS + 2 * ROW_HALO, COLS + 2 * LANE), F32),
            pltpu.VMEM((2, 2, 128, 3 * REACH), BF16),
            pltpu.VMEM((2, 64, 2 * REACH), BF16),
            pltpu.VMEM((2, 64, 2 * FAR), BF16),
        ]
        + [pltpu.VMEM((2, ROWS + 2 * ROW_HALO, WIDE), BF16)] * 4
        + [
            pltpu.VMEM((3, BLOCKS, 64, 256), F32),
            pltpu.VMEM((2, 2, BLOCKS, 64, 256), F32),
            pltpu.VMEM((2, BLOCKS - 1, 128, 128), F32),
            pltpu.VMEM((2, 128, WIDE), F32),
            pltpu.VMEM((8, WIDE), F32),
            pltpu.SemaphoreType.DMA((2,)),
            pltpu.SemaphoreType.DMA((8,)),
            pltpu.SemaphoreType.DMA((48,)),
            pltpu.SemaphoreType.DMA((48,)),
        ],
        compiler_params=pltpu.CompilerParams(
            collective_id=0, has_side_effects=True
        ),
    )(off_az, off_rg, ref_image, sec_image, *[jnp.asarray(t) for t in tables])
    out = pl.pallas_call(
        oversample,
        out_shape=jax.ShapeDtypeStruct((2 * CHIPS, 128, 128), F32),
        in_specs=[vmem],
        out_specs=anywhere,
        scratch_shapes=[pltpu.VMEM((2 * CHIPS, 128, 128), F32), pltpu.SemaphoreType.DMA],
        compiler_params=pltpu.CompilerParams(vmem_limit_bytes=8 << 20),
    )(scores)
    return out.reshape(2, CHIPS, 128, 128)


def solution(mesh):
    return jax.shard_map(
        body,
        mesh=mesh,
        in_specs=(P("az", "rg"), P("az", "rg"), P("az"), P("az")),
        out_specs=P("az", "rg", None, None),
        check_vma=False,
    )
```

```python
import functools

import jax
import jax.numpy as jnp
import numpy as np
from jax import lax
from jax.experimental import pallas as pl
from jax.experimental.pallas import tpu as pltpu
from jax.sharding import PartitionSpec as P

CHIP = 128
SPACE = 64
LAGS = 64
AREA = float(CHIP * CHIP)
EPSILON = 1e-06
ROWS = 128
COLS = 768
CHIPS = COLS // SPACE
PAIRS = CHIPS // 2
BLOCKS = CHIPS + 2
WIDE = BLOCKS * SPACE
ROW_HALO = 80
REF_HALO = 32
NEAR = 16
FAR = 64
REACH = 160
LANE = 128
MESH = pl.DeviceIdType.MESH
F32 = jnp.float32
BF16 = jnp.bfloat16


def halves(table):
    high = table.astype(jnp.bfloat16)
    low = (table - high.astype(np.float64)).astype(jnp.bfloat16)
    return high, low


def azimuth_table(first, count):
    angle = 2 * np.pi * (np.arange(64)[:, None] + 0.5) * (first + np.arange(count))[None, :] / 128
    high, low = halves(np.concatenate([np.cos(angle), -np.sin(angle)], axis=0))
    return np.concatenate([high, high, low], axis=1)


def box_table():
    cell = np.arange(256)[:, None]
    lag = np.arange(128)[None, :]
    return ((cell >= lag) & (cell < lag + 128)).astype(jnp.bfloat16)


def column_tables():
    angle = 2 * np.pi * np.arange(64)[:, None] * np.arange(128)[None, :] / 128
    c, s = np.cos(angle), np.sin(angle)
    sign = np.where(np.arange(256) % 2 == 0, 1.0, -1.0)[None, :]
    even = np.concatenate([np.concatenate([c, -s], 1), np.concatenate([s, c], 1)], 0)
    odd = np.concatenate([np.concatenate([s, c], 1), np.concatenate([c, -s], 1)], 0) * sign
    out = []
    for table in (even, odd):
        high, low = halves(table)
        out.append(np.concatenate([high, high, low], axis=0))
    return np.stack(out)


def back_tables():
    angle = 2 * np.pi * np.arange(64)[:, None] * (np.arange(64)[None, :] + 0.5) / 128
    c, s = np.cos(angle), np.sin(angle)
    high, low = halves(np.concatenate([np.concatenate([c, -s], 1), np.concatenate([s, c], 1)], 0))
    rows = np.concatenate([high, high, low], axis=1)
    angle = 2 * np.pi * np.arange(128)[:, None] * np.arange(64)[None, :] / 128
    high, low = halves(np.concatenate([np.cos(angle), -np.sin(angle)], 0) * (2.0 / AREA))
    none = np.zeros_like(high)
    first = np.concatenate([high, none, low, none], axis=1)
    second = np.concatenate([none, high, none, low], axis=1)
    return rows, np.stack([first, second])


def split(x):
    high = x.astype(BF16)
    return high, (x - high.astype(F32)).astype(BF16)


def dot(a, b):
    return jnp.dot(a, b, preferred_element_type=F32)


def shifted(x, shift, width):
    lane = lax.broadcasted_iota(jnp.int32, (x.shape[0], LANE), 1)
    turned = [
        pltpu.roll(x[:, i : i + LANE], LANE - shift, axis=1) for i in range(0, width + LANE, LANE)
    ]
    keep = lane < LANE - shift
    return jnp.concatenate(
        [jnp.where(keep, a, b) for a, b in zip(turned[:-1], turned[1:])], axis=1
    )


def range_spectra(rows_out, col_ref):
    lane = lax.broadcasted_iota(jnp.int32, (64, LANE), 1)
    low_half = lane < 64
    even, odd = [], []
    for x in rows_out:
        for i in range(0, x.shape[1], LANE):
            re = x[:64, i : i + LANE]
            im = pltpu.roll(x[64:, i : i + LANE], 64, axis=1)
            even.append(jnp.where(low_half, re, im))
            odd.append(jnp.where(low_half, im, re))
    out = []
    for parity, parts in enumerate((even, odd)):
        high, low = split(jnp.concatenate(parts, axis=0))
        got = dot(jnp.concatenate([high, low], axis=1), col_ref[parity, :256])
        got = got + dot(high, col_ref[parity, 256:])
        out.append(got)
    count = rows_out[0].shape[1] // LANE
    result = []
    for a in range(len(rows_out)):
        blocks = []
        for i in range(count):
            at = (a * count + i) * 64
            blocks += [out[0][at : at + 64], out[1][at : at + 64]]
        result.append(blocks)
    return result


def ones_where(condition):
    return jnp.where(condition, 1.0, 0.0).astype(BF16)


class Exchange:
    def __init__(self, tiles, bufs, tile_sems, send_sems, recv_sems):
        az, rg = lax.axis_index("az"), lax.axis_index("rg")
        last_az, last_rg = lax.axis_size("az") - 1, lax.axis_size("rg") - 1
        self.up = ("az", az - 1, az > 0)
        self.down = ("az", az + 1, az < last_az)
        self.left = ("rg", rg - 1, rg > 0)
        self.right = ("rg", rg + 1, rg < last_rg)
        self.sides = (self.up, self.down, self.left, self.right)
        self.bufs, self.send_sems, self.recv_sems, self.count = bufs, send_sems, recv_sems, 0
        self.all = []
        self.loads = []
        for i, (tile, (buf, halo)) in enumerate(zip(tiles, bufs)):
            own = buf.at[pl.ds(halo, ROWS), pl.ds(LANE, COLS)]
            self.loads.append(pltpu.make_async_copy(tile, own, tile_sems.at[i]))

    def greet(self):
        for load in self.loads:
            load.start()
        barrier = pltpu.get_barrier_semaphore()
        for axis, place, there in self.sides:

            @pl.when(there)
            def _(axis=axis, place=place):
                pl.semaphore_signal(barrier, inc=1, device_id={axis: place}, device_id_type=MESH)

    def clear(self):
        up, down, left, right = self.sides
        for buf, halo in self.bufs:
            for side, rows, lanes in (
                (up, slice(0, halo), slice(None)),
                (down, slice(halo + ROWS, 2 * halo + ROWS), slice(None)),
                (left, slice(None), slice(0, LANE)),
                (right, slice(None), slice(LANE + COLS, 2 * LANE + COLS)),
            ):

                @pl.when(jnp.logical_not(side[2]))
                def _(buf=buf, rows=rows, lanes=lanes):
                    shape = [n if c == slice(None) else c.stop - c.start for n, c in zip(buf.shape, (rows, lanes))]
                    buf[rows, lanes] = jnp.zeros(shape, F32)

    def meet(self):
        barrier = pltpu.get_barrier_semaphore()
        peers = sum(there.astype(jnp.int32) for _, _, there in self.sides)
        pl.semaphore_wait(barrier, peers)

    def copy(self, buf, rows, lanes, to_rows, to_lanes, side, back, have=None):
        index = self.count
        self.count += 1
        axis, place, sends = side
        comes = back[2]
        if have is not None:
            sends, comes = sends & have, comes & have
        transfer = pltpu.make_async_remote_copy(
            src_ref=buf.at[pl.ds(*rows), pl.ds(*lanes)],
            dst_ref=buf.at[pl.ds(*to_rows), pl.ds(*to_lanes)],
            send_sem=self.send_sems.at[index],
            recv_sem=self.recv_sems.at[index],
            device_id={axis: place},
            device_id_type=MESH,
        )
        entry = (transfer, sends, comes)
        self.all.append(entry)
        return entry

    def along_azimuth(self, buf, halo, near, far, lanes):
        count = far - near
        end = halo + ROWS
        return [
            self.copy(buf, (halo + near, count), lanes, (end + near, count), lanes, self.up, self.down),
            self.copy(buf, (end - far, count), lanes, (halo - far, count), lanes, self.down, self.up),
        ]

    def along_range(self, buf, rows, have=None):
        return [
            self.copy(buf, rows, (LANE, LANE), rows, (LANE + COLS, LANE), self.left, self.right, have),
            self.copy(buf, rows, (COLS, LANE), rows, (0, LANE), self.right, self.left, have),
        ]

    def corners(self, buf, halo, near, far):
        count = far - near
        return self.along_range(buf, (halo - far, count), self.up[2]) + self.along_range(
            buf, (halo + ROWS + near, count), self.down[2]
        )

    @staticmethod
    def start(entries, given=True):
        for transfer, sends, _ in entries:

            @pl.when(sends & given)
            def _(transfer=transfer):
                transfer.start()

    @staticmethod
    def arrive(entries, given=True):
        for transfer, _, comes in entries:

            @pl.when(comes & given)
            def _(transfer=transfer):
                transfer.wait_recv()

    def close(self):
        for transfer, sends, _ in self.all:

            @pl.when(sends)
            def _(transfer=transfer):
                transfer.wait_send()


def kernel(off_az_hbm, off_rg_hbm, ref_tile, sec_tile, *refs):
    table_hbm, score_ref, tables = refs[:6], refs[6], refs[7:13]
    ref_row_ref, sec_row_ref, col_ref, back_row_ref, back_col_ref, box_col_ref = tables
    off_az, off_rg, ref_buf, sec_buf, row_mats, box_mid, box_far = refs[13:20]
    sec_high, sec_low, square_high, square_low = refs[20:24]
    quads, windows, strips, boxes, stats, tile_sems, table_sems, send_sems, recv_sems = refs[24:]
    halo = Exchange(
        (ref_tile, sec_tile),
        ((ref_buf, REF_HALO), (sec_buf, ROW_HALO)),
        tile_sems,
        send_sems,
        recv_sems,
    )
    everything = (LANE, COLS)
    near = halo.along_azimuth(sec_buf, ROW_HALO, 0, NEAR, everything)
    beside = halo.along_range(sec_buf, (ROW_HALO, ROWS)) + halo.along_range(ref_buf, (REF_HALO, ROWS))
    order = (1, 6, 2, 3, 4, 5)
    sec_far, ref_far = {}, {}
    for b in order:
        lanes = (LANE * b, LANE)
        sec_far[b] = halo.along_azimuth(sec_buf, ROW_HALO, NEAR, ROW_HALO, lanes)
        ref_far[b] = halo.along_azimuth(ref_buf, REF_HALO, 0, REF_HALO, lanes)
    near_corners = halo.corners(sec_buf, ROW_HALO, 0, NEAR)
    sec_corners = halo.corners(sec_buf, ROW_HALO, NEAR, ROW_HALO)
    ref_corners = halo.corners(ref_buf, REF_HALO, 0, REF_HALO)

    corners = sec_corners + ref_corners

    def forward(step):
        for given, edges in cores:
            b = edges[step]
            halo.arrive(sec_far[b] + ref_far[b], given)
            halo.start(corners[0::2] if b == 1 else corners[1::2], given)

    halo.greet()
    fetches = [
        pltpu.make_async_copy(source, target, table_sems.at[i])
        for i, (source, target) in enumerate(
            zip((off_az_hbm, off_rg_hbm) + table_hbm, (off_az, off_rg) + tables)
        )
    ]
    for fetch in fetches:
        fetch.start()
    for load in halo.loads:
        load.wait()
    halo.meet()
    halo.start(near)
    halo.start(beside)
    second = lax.rem(lax.axis_index("rg"), 2) == 1
    cores = ((jnp.logical_not(second), (1, 6)), (second, (6, 1)))
    for given, edges in cores:
        for b in edges:
            halo.start(sec_far[b] + ref_far[b], given)
    late = (4, 5)
    for b in order[2:]:
        halo.start(sec_far[b] + ref_far[b], jnp.logical_not(second) if b in late else True)

    halo.clear()
    own = pl.ds(LANE, COLS)
    ref_mean = jnp.mean(ref_buf[pl.ds(REF_HALO, ROWS), own], keepdims=True)
    sec_mean = jnp.mean(sec_buf[pl.ds(ROW_HALO, ROWS), own], keepdims=True)

    for fetch in fetches:
        fetch.wait()
    lane = lax.broadcasted_iota(jnp.int32, (128, LANE), 1)
    for k in range(2):
        first = NEAR + off_az[k]
        for m in range(2):
            turned = [
                pltpu.roll(sec_row_ref[k + m, :, i : i + LANE], first, axis=1)
                for i in range(0, 512, LANE)
            ]
            moved = [jnp.where(lane < first, turned[i - 1], turned[i]) for i in range(4)]
            row_mats[k, m] = jnp.concatenate(moved, axis=1)[:, : 3 * REACH].astype(BF16)
        lag = lax.broadcasted_iota(jnp.int32, (64, 2 * REACH), 0)
        cell = lax.broadcasted_iota(jnp.int32, (64, 2 * REACH), 1)
        cell = jnp.where(cell < REACH, cell, cell - REACH) + (64 - 64 * k) - first - lag
        box_mid[k] = ones_where((cell >= 0) & (cell < CHIP))
        lag = lax.broadcasted_iota(jnp.int32, (64, 2 * FAR), 0)
        cell = lax.broadcasted_iota(jnp.int32, (64, 2 * FAR), 1)
        cell = jnp.where(cell < FAR, cell, cell - FAR) + REACH * k - first - lag
        box_far[k] = ones_where((cell >= 0) & (cell < CHIP))

    def reference_lines(m, pairs):
        parts = [ref_buf[64 * m : 64 * m + 64, LANE * p : LANE * p + 256] for p in pairs]
        parts = [shifted(x, LANE - REF_HALO, LANE) - ref_mean for x in parts]
        for p, x in zip(pairs, parts):
            place = pl.ds(LANE * p, LANE)
            stats[2 * m : 2 * m + 1, place] = jnp.sum(x, axis=0, keepdims=True)
            stats[2 * m + 1 : 2 * m + 2, place] = jnp.sum(x * x, axis=0, keepdims=True)
        high, low = split(jnp.concatenate(parts, axis=1))
        return dot(ref_row_ref[m], jnp.concatenate([high, low, high], axis=0))

    def take_lines(k, spans, pairs):
        for p in pairs:
            place = slice(LANE * p, LANE * p + LANE)
            for first, count in spans:
                rows = slice(first, first + count)
                x = shifted(sec_buf[rows, LANE * p : LANE * p + 256], 64 + off_rg[k], LANE) - sec_mean
                sec_high[k, rows, place], sec_low[k, rows, place] = split(x)
                square_high[k, rows, place], square_low[k, rows, place] = split(x * x)

    def box_lines(k, first, count, p, box_ref):
        rows, place = slice(first, first + count), slice(LANE * p, LANE * p + LANE)
        stack = jnp.concatenate(
            [
                jnp.concatenate([sec_high[k, rows, place], square_high[k, rows, place]], axis=1),
                jnp.concatenate([sec_low[k, rows, place], square_low[k, rows, place]], axis=1),
            ],
            axis=0,
        )
        return dot(box_ref[k], stack)

    def window_transform(k, m, pairs):
        rows = slice(64 * (k + m), 64 * (k + m) + REACH)
        high = jnp.concatenate([sec_high[k, rows, LANE * p : LANE * p + LANE] for p in pairs], axis=1)
        low = jnp.concatenate([sec_low[k, rows, LANE * p : LANE * p + LANE] for p in pairs], axis=1)
        return dot(row_mats[k, m], jnp.concatenate([high, low, high], axis=0))

    def store(target, pairs, blocks):
        for i, p in enumerate(pairs):
            for half in range(2):
                target[2 * p + half] = blocks[2 * i + half]

    def middle_quadrants(*groups):
        rows_out = [reference_lines(1, pairs) for pairs in groups]
        for pairs, x in zip(groups, rows_out):
            store(quads.at[1], pairs, range_spectra([x], col_ref)[0])

    def middle_windows(*groups):
        rows_out = [[window_transform(k, 1 - k, pairs) for k in range(2)] for pairs in groups]
        for pairs in groups:
            for k in range(2):
                for p in pairs:
                    sums = box_lines(k, 64, REACH, p, box_mid)
                    boxes[k, :64, LANE * p : LANE * p + LANE] = sums[:, :128]
                    boxes[k, 64:, LANE * p : LANE * p + LANE] = sums[:, 128:]
        for pairs, x in zip(groups, rows_out):
            got = range_spectra(x, col_ref)
            store(windows.at[0, 1], pairs, got[0])
            store(windows.at[1, 0], pairs, got[1])

    def outer(for_windows, for_quadrants):
        for pairs in for_windows:
            take_lines(0, ((0, FAR),), pairs)
            take_lines(1, ((224, FAR),), pairs)
        rows_out = {}
        for pairs in for_windows:
            rows_out[pairs] = [(windows.at[k, k], window_transform(k, k, pairs)) for k in range(2)]
        for pairs in for_quadrants:
            found = [(quads.at[m], reference_lines(m, pairs)) for m in (0, 2)]
            rows_out[pairs] = rows_out.get(pairs, []) + found
        for pairs in for_windows:
            for k in range(2):
                for p in pairs:
                    sums = box_lines(k, 224 * k, FAR, p, box_far)
                    boxes[k, :64, LANE * p : LANE * p + LANE] += sums[:, :128]
                    boxes[k, 64:, LANE * p : LANE * p + LANE] += sums[:, 128:]
        for pairs, found in rows_out.items():
            got = range_spectra([x for _, x in found], col_ref)
            for (target, _), blocks in zip(found, got):
                store(target, pairs, blocks)

    def product(k, m, n):
        q = quads[k + m, n]
        x = windows[k, m, n] + windows[k, m, n + 1]
        qr, qi, xr, xi = q[:, :128], q[:, 128:], x[:, :128], x[:, 128:]
        return jnp.concatenate([qr * xr + qi * xi, qr * xi - qi * xr], axis=0)

    def middle_strips(*numbers):
        for n in numbers:
            for k in range(2):
                strips[k, n] = product(k, 1 - k, n)

    done = {}

    def strip(k, n):
        if (k, n) not in done:
            done[k, n] = True
            value = strips[k, n] + product(k, k, n)
            strips[k, n] = value
            return value
        return strips[k, n]

    def finish(*pairs):
        items = [(k, s) for s in pairs for k in range(2)]
        moments = {}
        for s in pairs:
            stat = stats[:, s * LANE : s * LANE + 256]
            place = lax.broadcasted_iota(jnp.int32, stat.shape, 1)
            a = jnp.sum(stat[:, :128], axis=1, keepdims=True)
            b = jnp.sum(jnp.where((place >= 64) & (place < 192), stat, 0.0), axis=1, keepdims=True)
            moments[s] = jnp.where(place[:, :128] < 64, a, b)
        sums = {(k, n): strip(k, n) for k, s in items for n in range(2 * s, 2 * s + 3)}
        inner = {}
        for k, s in items:
            left, middle_, right = [sums[k, 2 * s + i] for i in range(3)]
            high, low = split(jnp.concatenate([left + middle_, middle_ + right], axis=1))
            y = dot(back_row_ref[:, :256], jnp.concatenate([high, low], axis=0))
            inner[k, s] = y + dot(back_row_ref[:, 256:], high)
        corr = 0.0
        for i in range(2):
            lanes = slice(LANE * i, LANE * i + LANE)
            parts = [split(jnp.concatenate([inner[item][:64, lanes], inner[item][64:, lanes]], axis=1)) for item in items]
            wide = dot(jnp.concatenate([high for high, _ in parts], axis=0), back_col_ref[i])
            corr = corr + (wide[:, :128] + wide[:, 128:])
            corr = corr + dot(jnp.concatenate([low for _, low in parts], axis=0), back_col_ref[i, :, :128])
        parts = [split(boxes[k, :, s * LANE : s * LANE + 256]) for k, s in items]
        box = dot(jnp.concatenate([high for high, _ in parts], axis=0), box_col_ref[...])
        box = box + dot(jnp.concatenate([low for _, low in parts], axis=0), box_col_ref[...])
        for i, (k, s) in enumerate(items):
            first, second = box[128 * i : 128 * i + 64], box[128 * i + 64 : 128 * i + 128]
            both = moments[s]
            total = both[2 * k : 2 * k + 1] + both[2 * k + 2 : 2 * k + 3]
            power = both[2 * k + 1 : 2 * k + 2] + both[2 * k + 3 : 2 * k + 4]
            mean = total / AREA
            energy = power - total * mean
            centered = corr[64 * i : 64 * i + 64] - mean * first
            var_sum = jnp.maximum(second - first * first / AREA, 0.0)
            score_ref[k, s] = (CHIP / AREA) * centered * lax.rsqrt(
                (energy / AREA) * (var_sum / AREA) + EPSILON
            )

    inside = (1, 2, 3, 4, 5)
    near_lines = ((ROW_HALO - NEAR, NEAR), (ROW_HALO + ROWS, NEAR))
    middle_quadrants((1, 2), (3, 4), (5,))
    for k in range(2):
        take_lines(k, ((ROW_HALO, ROWS),), inside)
    halo.arrive(near)
    halo.start(near_corners)
    for k in range(2):
        take_lines(k, near_lines, inside)
    middle_windows((1, 2), (3, 4), (5,))
    for b in late:
        halo.start(sec_far[b] + ref_far[b], second)
    forward(0)
    halo.arrive(beside)
    middle_quadrants((0, 6))
    middle_strips(*range(2, 11))
    forward(1)
    halo.arrive(near_corners)
    for k in range(2):
        take_lines(k, near_lines + ((ROW_HALO, ROWS),), (0, 6))
    middle_windows((0, 6))
    middle_strips(0, 1, 11, 12)
    halo.arrive(sec_far[2] + ref_far[2] + sec_far[3] + ref_far[3])
    outer([(1, 2)], [(1, 2)])
    halo.arrive(sec_far[4] + ref_far[4])
    outer([(3,)], [(3,)])
    halo.arrive(corners)
    halo.arrive(sec_far[5] + ref_far[5])
    outer([(4, 5), (0, 6)], [(4, 5), (0, 6)])
    finish(0, 1, 2, 3, 4, 5)
    halo.close()


def oversample(score_ref, out_ref, staged, sem):
    def cubic(out_index, sample):
        base = out_index // 2

        def pick(step):
            return jnp.where(jnp.clip(base + step, 0, LAGS - 1) == sample, 1.0, 0.0)

        odd = (9.0 * (pick(0) + pick(1)) - (pick(-1) + pick(2))) / 16.0
        return jnp.where(out_index % 2 == 1, odd, pick(0))

    row = lax.broadcasted_iota(jnp.int32, (128, 128), 0)
    lane = lax.broadcasted_iota(jnp.int32, (128, 128), 1)
    left = cubic(row, lane % LAGS).astype(BF16)
    right = cubic(lane, row % LAGS)
    right = jnp.concatenate(
        [jnp.where(row < LAGS, right, 0.0), jnp.where(row < LAGS, 0.0, right)], axis=1
    ).astype(BF16)
    right = jnp.concatenate([right, right], axis=0)
    items = [(k, s) for k in range(2) for s in range(PAIRS)]
    for first, last in ((0, 4), (4, 8), (8, 12)):
        lifted = []
        for i in range(first, last, 2):
            parts = [split(score_ref[k, s]) for k, s in items[i : i + 2]]
            high = jnp.concatenate([high for high, _ in parts], axis=1)
            low = jnp.concatenate([low for _, low in parts], axis=1)
            both = dot(left, jnp.concatenate([high, low], axis=0))
            lifted += [both[:, :LANE], both[:, LANE:]]
        for (k, s), value in zip(items[first:last], lifted):
            wide = dot(jnp.concatenate(split(value), axis=1), right)
            at = k * CHIPS + 2 * s
            staged[at] = wide[:, :128]
            staged[at + 1] = wide[:, 128:]
        part = pl.ds(2 * first, 2 * (last - first))
        pltpu.make_async_copy(staged.at[part], out_ref.at[part], sem).start()
    pltpu.make_async_copy(staged, out_ref, sem).wait()


def spread(table):
    room = np.zeros((128, REACH - 128))
    parts = [np.concatenate([table[:, i : i + 128].astype(np.float64), room], 1) for i in (0, 128, 256)]
    return np.concatenate(parts + [room], axis=1).astype(np.float32)


def body(ref_image, sec_image, off_az, off_rg):
    back_rows, back_cols = back_tables()
    tables = [
        np.stack([azimuth_table(64 * m, 64) for m in range(3)]),
        np.stack([spread(azimuth_table(64 * j, 128)) for j in range(3)]),
        column_tables(),
        back_rows,
        back_cols,
        box_table(),
    ]
    anywhere = pl.BlockSpec(memory_space=pl.ANY)
    vmem = pl.BlockSpec(memory_space=pltpu.VMEM)
    scores = pl.pallas_call(
        kernel,
        out_shape=pltpu.VMEM((2, PAIRS, LAGS, 2 * LAGS), F32),
        in_specs=[pl.BlockSpec(memory_space=pltpu.HBM)] * (4 + len(tables)),
        out_specs=vmem,
        scratch_shapes=[pltpu.VMEM(t.shape, t.dtype) for t in tables]
        + [
            pltpu.SMEM((2,), jnp.int32),
            pltpu.SMEM((2,), jnp.int32),
            pltpu.VMEM((ROWS + 2 * REF_HALO, COLS + 2 * LANE), F32),
            pltpu.VMEM((ROWS + 2 * ROW_HALO, COLS + 2 * LANE), F32),
            pltpu.VMEM((2, 2, 128, 3 * REACH), BF16),
            pltpu.VMEM((2, 64, 2 * REACH), BF16),
            pltpu.VMEM((2, 64, 2 * FAR), BF16),
        ]
        + [pltpu.VMEM((2, ROWS + 2 * ROW_HALO, WIDE), BF16)] * 4
        + [
            pltpu.VMEM((3, BLOCKS, 64, 256), F32),
            pltpu.VMEM((2, 2, BLOCKS, 64, 256), F32),
            pltpu.VMEM((2, BLOCKS - 1, 128, 128), F32),
            pltpu.VMEM((2, 128, WIDE), F32),
            pltpu.VMEM((8, WIDE), F32),
            pltpu.SemaphoreType.DMA((2,)),
            pltpu.SemaphoreType.DMA((8,)),
            pltpu.SemaphoreType.DMA((48,)),
            pltpu.SemaphoreType.DMA((48,)),
        ],
        compiler_params=pltpu.CompilerParams(
            collective_id=0, has_side_effects=True
        ),
    )(off_az, off_rg, ref_image, sec_image, *[jnp.asarray(t) for t in tables])
    out = pl.pallas_call(
        oversample,
        out_shape=jax.ShapeDtypeStruct((2 * CHIPS, 128, 128), F32),
        in_specs=[vmem],
        out_specs=anywhere,
        scratch_shapes=[pltpu.VMEM((2 * CHIPS, 128, 128), F32), pltpu.SemaphoreType.DMA],
        compiler_params=pltpu.CompilerParams(vmem_limit_bytes=8 << 20),
    )(scores)
    return out.reshape(2, CHIPS, 128, 128)


def solution(mesh):
    return jax.shard_map(
        body,
        mesh=mesh,
        in_specs=(P("az", "rg"), P("az", "rg"), P("az"), P("az")),
        out_specs=P("az", "rg", None, None),
        check_vma=False,
    )
```

```python
import functools

import jax
import jax.numpy as jnp
import numpy as np
from jax import lax
from jax.experimental import pallas as pl
from jax.experimental.pallas import tpu as pltpu
from jax.sharding import PartitionSpec as P

CHIP = 128
SPACE = 64
LAGS = 64
AREA = float(CHIP * CHIP)
EPSILON = 1e-06
ROWS = 128
COLS = 768
CHIPS = COLS // SPACE
PAIRS = CHIPS // 2
BLOCKS = CHIPS + 2
WIDE = BLOCKS * SPACE
ROW_HALO = 80
REF_HALO = 32
NEAR = 16
FAR = 64
REACH = 160
LANE = 128
MESH = pl.DeviceIdType.MESH
F32 = jnp.float32
BF16 = jnp.bfloat16


def halves(table):
    high = table.astype(jnp.bfloat16)
    low = (table - high.astype(np.float64)).astype(jnp.bfloat16)
    return high, low


def azimuth_table(first, count):
    angle = 2 * np.pi * (np.arange(64)[:, None] + 0.5) * (first + np.arange(count))[None, :] / 128
    high, low = halves(np.concatenate([np.cos(angle), -np.sin(angle)], axis=0))
    return np.concatenate([high, high, low], axis=1)


def box_table():
    cell = np.arange(256)[:, None]
    lag = np.arange(128)[None, :]
    return ((cell >= lag) & (cell < lag + 128)).astype(jnp.bfloat16)


def column_tables():
    angle = 2 * np.pi * np.arange(64)[:, None] * np.arange(128)[None, :] / 128
    c, s = np.cos(angle), np.sin(angle)
    sign = np.where(np.arange(256) % 2 == 0, 1.0, -1.0)[None, :]
    even = np.concatenate([np.concatenate([c, -s], 1), np.concatenate([s, c], 1)], 0)
    odd = np.concatenate([np.concatenate([s, c], 1), np.concatenate([c, -s], 1)], 0) * sign
    out = []
    for table in (even, odd):
        high, low = halves(table)
        out.append(np.concatenate([high, high, low], axis=0))
    return np.stack(out)


def back_tables():
    angle = 2 * np.pi * np.arange(64)[:, None] * (np.arange(64)[None, :] + 0.5) / 128
    c, s = np.cos(angle), np.sin(angle)
    high, low = halves(np.concatenate([np.concatenate([c, -s], 1), np.concatenate([s, c], 1)], 0))
    rows = np.concatenate([high, high, low], axis=1)
    angle = 2 * np.pi * np.arange(128)[:, None] * np.arange(64)[None, :] / 128
    high, low = halves(np.concatenate([np.cos(angle), -np.sin(angle)], 0) * (2.0 / AREA))
    none = np.zeros_like(high)
    first = np.concatenate([high, none, low, none], axis=1)
    second = np.concatenate([none, high, none, low], axis=1)
    return rows, np.stack([first, second])


def split(x):
    high = x.astype(BF16)
    return high, (x - high.astype(F32)).astype(BF16)


def dot(a, b):
    return jnp.dot(a, b, preferred_element_type=F32)


def shifted(x, shift, width):
    lane = lax.broadcasted_iota(jnp.int32, (x.shape[0], LANE), 1)
    turned = [
        pltpu.roll(x[:, i : i + LANE], LANE - shift, axis=1) for i in range(0, width + LANE, LANE)
    ]
    keep = lane < LANE - shift
    return jnp.concatenate(
        [jnp.where(keep, a, b) for a, b in zip(turned[:-1], turned[1:])], axis=1
    )


def range_spectra(rows_out, col_ref):
    lane = lax.broadcasted_iota(jnp.int32, (64, LANE), 1)
    low_half = lane < 64
    even, odd = [], []
    for x in rows_out:
        for i in range(0, x.shape[1], LANE):
            re = x[:64, i : i + LANE]
            im = pltpu.roll(x[64:, i : i + LANE], 64, axis=1)
            even.append(jnp.where(low_half, re, im))
            odd.append(jnp.where(low_half, im, re))
    out = []
    for parity, parts in enumerate((even, odd)):
        high, low = split(jnp.concatenate(parts, axis=0))
        got = dot(jnp.concatenate([high, low], axis=1), col_ref[parity, :256])
        got = got + dot(high, col_ref[parity, 256:])
        out.append(got)
    count = rows_out[0].shape[1] // LANE
    result = []
    for a in range(len(rows_out)):
        blocks = []
        for i in range(count):
            at = (a * count + i) * 64
            blocks += [out[0][at : at + 64], out[1][at : at + 64]]
        result.append(blocks)
    return result


def ones_where(condition):
    return jnp.where(condition, 1.0, 0.0).astype(BF16)


class Exchange:
    def __init__(self, tiles, bufs, tile_sems, send_sems, recv_sems):
        az, rg = lax.axis_index("az"), lax.axis_index("rg")
        last_az, last_rg = lax.axis_size("az") - 1, lax.axis_size("rg") - 1
        self.up = ("az", az - 1, az > 0)
        self.down = ("az", az + 1, az < last_az)
        self.left = ("rg", rg - 1, rg > 0)
        self.right = ("rg", rg + 1, rg < last_rg)
        self.sides = (self.up, self.down, self.left, self.right)
        self.bufs, self.send_sems, self.recv_sems, self.count = bufs, send_sems, recv_sems, 0
        self.all = []
        self.loads = []
        for i, (tile, (buf, halo)) in enumerate(zip(tiles, bufs)):
            own = buf.at[pl.ds(halo, ROWS), pl.ds(LANE, COLS)]
            self.loads.append(pltpu.make_async_copy(tile, own, tile_sems.at[i]))

    def greet(self):
        for load in self.loads:
            load.start()
        barrier = pltpu.get_barrier_semaphore()
        for axis, place, there in self.sides:

            @pl.when(there)
            def _(axis=axis, place=place):
                pl.semaphore_signal(barrier, inc=1, device_id={axis: place}, device_id_type=MESH)

    def clear(self):
        up, down, left, right = self.sides
        for buf, halo in self.bufs:
            for side, rows, lanes in (
                (up, slice(0, halo), slice(None)),
                (down, slice(halo + ROWS, 2 * halo + ROWS), slice(None)),
                (left, slice(None), slice(0, LANE)),
                (right, slice(None), slice(LANE + COLS, 2 * LANE + COLS)),
            ):

                @pl.when(jnp.logical_not(side[2]))
                def _(buf=buf, rows=rows, lanes=lanes):
                    shape = [n if c == slice(None) else c.stop - c.start for n, c in zip(buf.shape, (rows, lanes))]
                    buf[rows, lanes] = jnp.zeros(shape, F32)

    def meet(self):
        barrier = pltpu.get_barrier_semaphore()
        peers = sum(there.astype(jnp.int32) for _, _, there in self.sides)
        pl.semaphore_wait(barrier, peers)

    def copy(self, buf, rows, lanes, to_rows, to_lanes, side, back, have=None):
        index = self.count
        self.count += 1
        axis, place, sends = side
        comes = back[2]
        if have is not None:
            sends, comes = sends & have, comes & have
        transfer = pltpu.make_async_remote_copy(
            src_ref=buf.at[pl.ds(*rows), pl.ds(*lanes)],
            dst_ref=buf.at[pl.ds(*to_rows), pl.ds(*to_lanes)],
            send_sem=self.send_sems.at[index],
            recv_sem=self.recv_sems.at[index],
            device_id={axis: place},
            device_id_type=MESH,
        )
        entry = (transfer, sends, comes)
        self.all.append(entry)
        return entry

    def along_azimuth(self, buf, halo, near, far, lanes):
        count = far - near
        end = halo + ROWS
        return [
            self.copy(buf, (halo + near, count), lanes, (end + near, count), lanes, self.up, self.down),
            self.copy(buf, (end - far, count), lanes, (halo - far, count), lanes, self.down, self.up),
        ]

    def along_range(self, buf, rows, have=None):
        return [
            self.copy(buf, rows, (LANE, LANE), rows, (LANE + COLS, LANE), self.left, self.right, have),
            self.copy(buf, rows, (COLS, LANE), rows, (0, LANE), self.right, self.left, have),
        ]

    def corners(self, buf, halo, near, far):
        count = far - near
        return self.along_range(buf, (halo - far, count), self.up[2]) + self.along_range(
            buf, (halo + ROWS + near, count), self.down[2]
        )

    @staticmethod
    def start(entries, given=True):
        for transfer, sends, _ in entries:

            @pl.when(sends & given)
            def _(transfer=transfer):
                transfer.start()

    @staticmethod
    def arrive(entries, given=True):
        for transfer, _, comes in entries:

            @pl.when(comes & given)
            def _(transfer=transfer):
                transfer.wait_recv()

    def close(self):
        for transfer, sends, _ in self.all:

            @pl.when(sends)
            def _(transfer=transfer):
                transfer.wait_send()


def kernel(off_az_hbm, off_rg_hbm, ref_tile, sec_tile, *refs):
    table_hbm, score_ref, tables = refs[:6], refs[6], refs[7:13]
    ref_row_ref, sec_row_ref, col_ref, back_row_ref, back_col_ref, box_col_ref = tables
    off_az, off_rg, ref_buf, sec_buf, row_mats, box_mid, box_far = refs[13:20]
    sec_high, sec_low, square_high, square_low = refs[20:24]
    quads, windows, strips, boxes, stats, tile_sems, table_sems, send_sems, recv_sems = refs[24:]
    halo = Exchange(
        (ref_tile, sec_tile),
        ((ref_buf, REF_HALO), (sec_buf, ROW_HALO)),
        tile_sems,
        send_sems,
        recv_sems,
    )
    everything = (LANE, COLS)
    near = halo.along_azimuth(sec_buf, ROW_HALO, 0, NEAR, everything)
    beside = halo.along_range(sec_buf, (ROW_HALO, ROWS)) + halo.along_range(ref_buf, (REF_HALO, ROWS))
    order = (1, 6, 2, 3, 4, 5)
    sec_far, ref_far = {}, {}
    for b in order:
        lanes = (LANE * b, LANE)
        sec_far[b] = halo.along_azimuth(sec_buf, ROW_HALO, NEAR, ROW_HALO, lanes)
        ref_far[b] = halo.along_azimuth(ref_buf, REF_HALO, 0, REF_HALO, lanes)
    near_corners = halo.corners(sec_buf, ROW_HALO, 0, NEAR)
    sec_corners = halo.corners(sec_buf, ROW_HALO, NEAR, ROW_HALO)
    ref_corners = halo.corners(ref_buf, REF_HALO, 0, REF_HALO)

    corners = sec_corners + ref_corners

    def forward(step):
        for given, edges in cores:
            b = edges[step]
            halo.arrive(sec_far[b] + ref_far[b], given)
            halo.start(corners[0::2] if b == 1 else corners[1::2], given)

    halo.greet()
    fetches = [
        pltpu.make_async_copy(source, target, table_sems.at[i])
        for i, (source, target) in enumerate(
            zip((off_az_hbm, off_rg_hbm) + table_hbm, (off_az, off_rg) + tables)
        )
    ]
    for fetch in fetches:
        fetch.start()
    for load in halo.loads:
        load.wait()
    halo.meet()
    halo.start(near)
    halo.start(beside)
    second = lax.rem(lax.axis_index("rg"), 2) == 1
    cores = ((jnp.logical_not(second), (1, 6)), (second, (6, 1)))
    for given, edges in cores:
        for b in edges:
            halo.start(sec_far[b] + ref_far[b], given)
    for b in order[2:]:
        halo.start(sec_far[b] + ref_far[b])

    halo.clear()
    own = pl.ds(LANE, COLS)
    ref_mean = jnp.mean(ref_buf[pl.ds(REF_HALO, ROWS), own], keepdims=True)
    sec_mean = jnp.mean(sec_buf[pl.ds(ROW_HALO, ROWS), own], keepdims=True)

    for fetch in fetches:
        fetch.wait()
    lane = lax.broadcasted_iota(jnp.int32, (128, LANE), 1)
    for k in range(2):
        first = NEAR + off_az[k]
        for m in range(2):
            turned = [
                pltpu.roll(sec_row_ref[k + m, :, i : i + LANE], first, axis=1)
                for i in range(0, 512, LANE)
            ]
            moved = [jnp.where(lane < first, turned[i - 1], turned[i]) for i in range(4)]
            row_mats[k, m] = jnp.concatenate(moved, axis=1)[:, : 3 * REACH].astype(BF16)
        lag = lax.broadcasted_iota(jnp.int32, (64, 2 * REACH), 0)
        cell = lax.broadcasted_iota(jnp.int32, (64, 2 * REACH), 1)
        cell = jnp.where(cell < REACH, cell, cell - REACH) + (64 - 64 * k) - first - lag
        box_mid[k] = ones_where((cell >= 0) & (cell < CHIP))
        lag = lax.broadcasted_iota(jnp.int32, (64, 2 * FAR), 0)
        cell = lax.broadcasted_iota(jnp.int32, (64, 2 * FAR), 1)
        cell = jnp.where(cell < FAR, cell, cell - FAR) + REACH * k - first - lag
        box_far[k] = ones_where((cell >= 0) & (cell < CHIP))

    def reference_lines(m, pairs):
        parts = [ref_buf[64 * m : 64 * m + 64, LANE * p : LANE * p + 256] for p in pairs]
        parts = [shifted(x, LANE - REF_HALO, LANE) - ref_mean for x in parts]
        for p, x in zip(pairs, parts):
            place = pl.ds(LANE * p, LANE)
            stats[2 * m : 2 * m + 1, place] = jnp.sum(x, axis=0, keepdims=True)
            stats[2 * m + 1 : 2 * m + 2, place] = jnp.sum(x * x, axis=0, keepdims=True)
        high, low = split(jnp.concatenate(parts, axis=1))
        return dot(ref_row_ref[m], jnp.concatenate([high, low, high], axis=0))

    def take_lines(k, spans, pairs):
        for p in pairs:
            place = slice(LANE * p, LANE * p + LANE)
            for first, count in spans:
                rows = slice(first, first + count)
                x = shifted(sec_buf[rows, LANE * p : LANE * p + 256], 64 + off_rg[k], LANE) - sec_mean
                sec_high[k, rows, place], sec_low[k, rows, place] = split(x)
                square_high[k, rows, place], square_low[k, rows, place] = split(x * x)

    def box_lines(k, first, count, p, box_ref):
        rows, place = slice(first, first + count), slice(LANE * p, LANE * p + LANE)
        stack = jnp.concatenate(
            [
                jnp.concatenate([sec_high[k, rows, place], square_high[k, rows, place]], axis=1),
                jnp.concatenate([sec_low[k, rows, place], square_low[k, rows, place]], axis=1),
            ],
            axis=0,
        )
        return dot(box_ref[k], stack)

    def window_transform(k, m, pairs):
        rows = slice(64 * (k + m), 64 * (k + m) + REACH)
        high = jnp.concatenate([sec_high[k, rows, LANE * p : LANE * p + LANE] for p in pairs], axis=1)
        low = jnp.concatenate([sec_low[k, rows, LANE * p : LANE * p + LANE] for p in pairs], axis=1)
        return dot(row_mats[k, m], jnp.concatenate([high, low, high], axis=0))

    def store(target, pairs, blocks):
        for i, p in enumerate(pairs):
            for half in range(2):
                target[2 * p + half] = blocks[2 * i + half]

    def middle_quadrants(*groups):
        rows_out = [reference_lines(1, pairs) for pairs in groups]
        for pairs, x in zip(groups, rows_out):
            store(quads.at[1], pairs, range_spectra([x], col_ref)[0])

    def middle_windows(*groups):
        rows_out = [[window_transform(k, 1 - k, pairs) for k in range(2)] for pairs in groups]
        for pairs in groups:
            for k in range(2):
                for p in pairs:
                    sums = box_lines(k, 64, REACH, p, box_mid)
                    boxes[k, :64, LANE * p : LANE * p + LANE] = sums[:, :128]
                    boxes[k, 64:, LANE * p : LANE * p + LANE] = sums[:, 128:]
        for pairs, x in zip(groups, rows_out):
            got = range_spectra(x, col_ref)
            store(windows.at[0, 1], pairs, got[0])
            store(windows.at[1, 0], pairs, got[1])

    def outer(for_windows, for_quadrants):
        for pairs in for_windows:
            take_lines(0, ((0, FAR),), pairs)
            take_lines(1, ((224, FAR),), pairs)
        rows_out = {}
        for pairs in for_windows:
            rows_out[pairs] = [(windows.at[k, k], window_transform(k, k, pairs)) for k in range(2)]
        for pairs in for_quadrants:
            found = [(quads.at[m], reference_lines(m, pairs)) for m in (0, 2)]
            rows_out[pairs] = rows_out.get(pairs, []) + found
        for pairs in for_windows:
            for k in range(2):
                for p in pairs:
                    sums = box_lines(k, 224 * k, FAR, p, box_far)
                    boxes[k, :64, LANE * p : LANE * p + LANE] += sums[:, :128]
                    boxes[k, 64:, LANE * p : LANE * p + LANE] += sums[:, 128:]
        for pairs, found in rows_out.items():
            got = range_spectra([x for _, x in found], col_ref)
            for (target, _), blocks in zip(found, got):
                store(target, pairs, blocks)

    def product(k, m, n):
        q = quads[k + m, n]
        x = windows[k, m, n] + windows[k, m, n + 1]
        qr, qi, xr, xi = q[:, :128], q[:, 128:], x[:, :128], x[:, 128:]
        return jnp.concatenate([qr * xr + qi * xi, qr * xi - qi * xr], axis=0)

    def middle_strips(*numbers):
        for n in numbers:
            for k in range(2):
                strips[k, n] = product(k, 1 - k, n)

    done = {}

    def strip(k, n):
        if (k, n) not in done:
            done[k, n] = True
            value = strips[k, n] + product(k, k, n)
            strips[k, n] = value
            return value
        return strips[k, n]

    def finish(*pairs):
        items = [(k, s) for s in pairs for k in range(2)]
        moments = {}
        for s in pairs:
            stat = stats[:, s * LANE : s * LANE + 256]
            place = lax.broadcasted_iota(jnp.int32, stat.shape, 1)
            a = jnp.sum(stat[:, :128], axis=1, keepdims=True)
            b = jnp.sum(jnp.where((place >= 64) & (place < 192), stat, 0.0), axis=1, keepdims=True)
            moments[s] = jnp.where(place[:, :128] < 64, a, b)
        sums = {(k, n): strip(k, n) for k, s in items for n in range(2 * s, 2 * s + 3)}
        inner = {}
        for k, s in items:
            left, middle_, right = [sums[k, 2 * s + i] for i in range(3)]
            high, low = split(jnp.concatenate([left + middle_, middle_ + right], axis=1))
            y = dot(back_row_ref[:, :256], jnp.concatenate([high, low], axis=0))
            inner[k, s] = y + dot(back_row_ref[:, 256:], high)
        corr = 0.0
        for i in range(2):
            lanes = slice(LANE * i, LANE * i + LANE)
            parts = [split(jnp.concatenate([inner[item][:64, lanes], inner[item][64:, lanes]], axis=1)) for item in items]
            wide = dot(jnp.concatenate([high for high, _ in parts], axis=0), back_col_ref[i])
            corr = corr + (wide[:, :128] + wide[:, 128:])
            corr = corr + dot(jnp.concatenate([low for _, low in parts], axis=0), back_col_ref[i, :, :128])
        parts = [split(boxes[k, :, s * LANE : s * LANE + 256]) for k, s in items]
        box = dot(jnp.concatenate([high for high, _ in parts], axis=0), box_col_ref[...])
        box = box + dot(jnp.concatenate([low for _, low in parts], axis=0), box_col_ref[...])
        for i, (k, s) in enumerate(items):
            first, second = box[128 * i : 128 * i + 64], box[128 * i + 64 : 128 * i + 128]
            both = moments[s]
            total = both[2 * k : 2 * k + 1] + both[2 * k + 2 : 2 * k + 3]
            power = both[2 * k + 1 : 2 * k + 2] + both[2 * k + 3 : 2 * k + 4]
            mean = total / AREA
            energy = power - total * mean
            centered = corr[64 * i : 64 * i + 64] - mean * first
            var_sum = jnp.maximum(second - first * first / AREA, 0.0)
            score_ref[k, s] = (CHIP / AREA) * centered * lax.rsqrt(
                (energy / AREA) * (var_sum / AREA) + EPSILON
            )

    inside = (1, 2, 3, 4, 5)
    near_lines = ((ROW_HALO - NEAR, NEAR), (ROW_HALO + ROWS, NEAR))
    middle_quadrants((1, 2), (3, 4), (5,))
    for k in range(2):
        take_lines(k, ((ROW_HALO, ROWS),), inside)
    halo.arrive(near)
    halo.start(near_corners)
    for k in range(2):
        take_lines(k, near_lines, inside)
    middle_windows((1, 2), (3, 4), (5,))
    forward(0)
    halo.arrive(beside)
    middle_quadrants((0, 6))
    middle_strips(*range(2, 11))
    forward(1)
    halo.arrive(near_corners)
    for k in range(2):
        take_lines(k, near_lines + ((ROW_HALO, ROWS),), (0, 6))
    middle_windows((0, 6))
    middle_strips(0, 1, 11, 12)
    halo.arrive(sec_far[2] + ref_far[2] + sec_far[3] + ref_far[3])
    outer([(1, 2)], [(1, 2)])
    halo.arrive(sec_far[4] + ref_far[4])
    outer([(3,)], [(3,)])
    halo.arrive(corners)
    halo.arrive(sec_far[5] + ref_far[5])
    outer([(4, 5), (0, 6)], [(4, 5), (0, 6)])
    finish(0, 1, 2, 3, 4, 5)
    halo.close()


def oversample(score_ref, out_ref, staged, sem):
    def cubic(out_index, sample):
        base = out_index // 2

        def pick(step):
            return jnp.where(jnp.clip(base + step, 0, LAGS - 1) == sample, 1.0, 0.0)

        odd = (9.0 * (pick(0) + pick(1)) - (pick(-1) + pick(2))) / 16.0
        return jnp.where(out_index % 2 == 1, odd, pick(0))

    row = lax.broadcasted_iota(jnp.int32, (128, 128), 0)
    lane = lax.broadcasted_iota(jnp.int32, (128, 128), 1)
    left = cubic(row, lane % LAGS).astype(BF16)
    right = cubic(lane, row % LAGS)
    right = jnp.concatenate(
        [jnp.where(row < LAGS, right, 0.0), jnp.where(row < LAGS, 0.0, right)], axis=1
    ).astype(BF16)
    right = jnp.concatenate([right, right], axis=0)
    items = [(k, s) for k in range(2) for s in range(PAIRS)]
    for first, last in ((0, 6), (6, 12)):
        lifted = []
        for i in range(first, last, 2):
            parts = [split(score_ref[k, s]) for k, s in items[i : i + 2]]
            high = jnp.concatenate([high for high, _ in parts], axis=1)
            low = jnp.concatenate([low for _, low in parts], axis=1)
            both = dot(left, jnp.concatenate([high, low], axis=0))
            lifted += [both[:, :LANE], both[:, LANE:]]
        for (k, s), value in zip(items[first:last], lifted):
            wide = dot(jnp.concatenate(split(value), axis=1), right)
            at = k * CHIPS + 2 * s
            staged[at] = wide[:, :128]
            staged[at + 1] = wide[:, 128:]
        part = pl.ds(2 * first, 2 * (last - first))
        pltpu.make_async_copy(staged.at[part], out_ref.at[part], sem).start()
    pltpu.make_async_copy(staged, out_ref, sem).wait()


def spread(table):
    room = np.zeros((128, REACH - 128))
    parts = [np.concatenate([table[:, i : i + 128].astype(np.float64), room], 1) for i in (0, 128, 256)]
    return np.concatenate(parts + [room], axis=1).astype(np.float32)


def body(ref_image, sec_image, off_az, off_rg):
    back_rows, back_cols = back_tables()
    tables = [
        np.stack([azimuth_table(64 * m, 64) for m in range(3)]),
        np.stack([spread(azimuth_table(64 * j, 128)) for j in range(3)]),
        column_tables(),
        back_rows,
        back_cols,
        box_table(),
    ]
    anywhere = pl.BlockSpec(memory_space=pl.ANY)
    vmem = pl.BlockSpec(memory_space=pltpu.VMEM)
    scores = pl.pallas_call(
        kernel,
        out_shape=pltpu.VMEM((2, PAIRS, LAGS, 2 * LAGS), F32),
        in_specs=[pl.BlockSpec(memory_space=pltpu.HBM)] * (4 + len(tables)),
        out_specs=vmem,
        scratch_shapes=[pltpu.VMEM(t.shape, t.dtype) for t in tables]
        + [
            pltpu.SMEM((2,), jnp.int32),
            pltpu.SMEM((2,), jnp.int32),
            pltpu.VMEM((ROWS + 2 * REF_HALO, COLS + 2 * LANE), F32),
            pltpu.VMEM((ROWS + 2 * ROW_HALO, COLS + 2 * LANE), F32),
            pltpu.VMEM((2, 2, 128, 3 * REACH), BF16),
            pltpu.VMEM((2, 64, 2 * REACH), BF16),
            pltpu.VMEM((2, 64, 2 * FAR), BF16),
        ]
        + [pltpu.VMEM((2, ROWS + 2 * ROW_HALO, WIDE), BF16)] * 4
        + [
            pltpu.VMEM((3, BLOCKS, 64, 256), F32),
            pltpu.VMEM((2, 2, BLOCKS, 64, 256), F32),
            pltpu.VMEM((2, BLOCKS - 1, 128, 128), F32),
            pltpu.VMEM((2, 128, WIDE), F32),
            pltpu.VMEM((8, WIDE), F32),
            pltpu.SemaphoreType.DMA((2,)),
            pltpu.SemaphoreType.DMA((8,)),
            pltpu.SemaphoreType.DMA((48,)),
            pltpu.SemaphoreType.DMA((48,)),
        ],
        compiler_params=pltpu.CompilerParams(
            collective_id=0, has_side_effects=True
        ),
    )(off_az, off_rg, ref_image, sec_image, *[jnp.asarray(t) for t in tables])
    out = pl.pallas_call(
        oversample,
        out_shape=jax.ShapeDtypeStruct((2 * CHIPS, 128, 128), F32),
        in_specs=[vmem],
        out_specs=anywhere,
        scratch_shapes=[pltpu.VMEM((2 * CHIPS, 128, 128), F32), pltpu.SemaphoreType.DMA],
        compiler_params=pltpu.CompilerParams(vmem_limit_bytes=8 << 20),
    )(scores)
    return out.reshape(2, CHIPS, 128, 128)


def solution(mesh):
    return jax.shard_map(
        body,
        mesh=mesh,
        in_specs=(P("az", "rg"), P("az", "rg"), P("az"), P("az")),
        out_specs=P("az", "rg", None, None),
        check_vma=False,
    )
```

```python
import functools

import jax
import jax.numpy as jnp
import numpy as np
from jax import lax
from jax.experimental import pallas as pl
from jax.experimental.pallas import tpu as pltpu
from jax.sharding import PartitionSpec as P

CHIP = 128
SPACE = 64
LAGS = 64
AREA = float(CHIP * CHIP)
EPSILON = 1e-06
ROWS = 128
COLS = 768
CHIPS = COLS // SPACE
PAIRS = CHIPS // 2
BLOCKS = CHIPS + 2
WIDE = BLOCKS * SPACE
ROW_HALO = 80
REF_HALO = 32
NEAR = 16
FAR = 64
REACH = 160
LANE = 128
MESH = pl.DeviceIdType.MESH
F32 = jnp.float32
BF16 = jnp.bfloat16


def halves(table):
    high = table.astype(jnp.bfloat16)
    low = (table - high.astype(np.float64)).astype(jnp.bfloat16)
    return high, low


def azimuth_table(first, count):
    angle = 2 * np.pi * (np.arange(64)[:, None] + 0.5) * (first + np.arange(count))[None, :] / 128
    high, low = halves(np.concatenate([np.cos(angle), -np.sin(angle)], axis=0))
    return np.concatenate([high, high, low], axis=1)


def box_table():
    cell = np.arange(256)[:, None]
    lag = np.arange(128)[None, :]
    return ((cell >= lag) & (cell < lag + 128)).astype(jnp.bfloat16)


def column_tables():
    angle = 2 * np.pi * np.arange(64)[:, None] * np.arange(128)[None, :] / 128
    c, s = np.cos(angle), np.sin(angle)
    sign = np.where(np.arange(256) % 2 == 0, 1.0, -1.0)[None, :]
    even = np.concatenate([np.concatenate([c, -s], 1), np.concatenate([s, c], 1)], 0)
    odd = np.concatenate([np.concatenate([s, c], 1), np.concatenate([c, -s], 1)], 0) * sign
    out = []
    for table in (even, odd):
        high, low = halves(table)
        out.append(np.concatenate([high, high, low], axis=0))
    return np.stack(out)


def back_tables():
    angle = 2 * np.pi * np.arange(64)[:, None] * (np.arange(64)[None, :] + 0.5) / 128
    c, s = np.cos(angle), np.sin(angle)
    high, low = halves(np.concatenate([np.concatenate([c, -s], 1), np.concatenate([s, c], 1)], 0))
    rows = np.concatenate([high, high, low], axis=1)
    angle = 2 * np.pi * np.arange(128)[:, None] * np.arange(64)[None, :] / 128
    high, low = halves(np.concatenate([np.cos(angle), -np.sin(angle)], 0) * (2.0 / AREA))
    none = np.zeros_like(high)
    first = np.concatenate([high, none, low, none], axis=1)
    second = np.concatenate([none, high, none, low], axis=1)
    return rows, np.stack([first, second])


def split(x):
    high = x.astype(BF16)
    return high, (x - high.astype(F32)).astype(BF16)


def dot(a, b):
    return jnp.dot(a, b, preferred_element_type=F32)


def shifted(x, shift, width):
    lane = lax.broadcasted_iota(jnp.int32, (x.shape[0], LANE), 1)
    turned = [
        pltpu.roll(x[:, i : i + LANE], LANE - shift, axis=1) for i in range(0, width + LANE, LANE)
    ]
    keep = lane < LANE - shift
    return jnp.concatenate(
        [jnp.where(keep, a, b) for a, b in zip(turned[:-1], turned[1:])], axis=1
    )


def range_spectra(rows_out, col_ref):
    lane = lax.broadcasted_iota(jnp.int32, (64, LANE), 1)
    low_half = lane < 64
    even, odd = [], []
    for x in rows_out:
        for i in range(0, x.shape[1], LANE):
            re = x[:64, i : i + LANE]
            im = pltpu.roll(x[64:, i : i + LANE], 64, axis=1)
            even.append(jnp.where(low_half, re, im))
            odd.append(jnp.where(low_half, im, re))
    out = []
    for parity, parts in enumerate((even, odd)):
        high, low = split(jnp.concatenate(parts, axis=0))
        got = dot(jnp.concatenate([high, low], axis=1), col_ref[parity, :256])
        got = got + dot(high, col_ref[parity, 256:])
        out.append(got)
    count = rows_out[0].shape[1] // LANE
    result = []
    for a in range(len(rows_out)):
        blocks = []
        for i in range(count):
            at = (a * count + i) * 64
            blocks += [out[0][at : at + 64], out[1][at : at + 64]]
        result.append(blocks)
    return result


def ones_where(condition):
    return jnp.where(condition, 1.0, 0.0).astype(BF16)


class Exchange:
    def __init__(self, tiles, bufs, tile_sems, send_sems, recv_sems):
        az, rg = lax.axis_index("az"), lax.axis_index("rg")
        last_az, last_rg = lax.axis_size("az") - 1, lax.axis_size("rg") - 1
        self.place = {"az": az, "rg": rg}
        self.up = ("az", -1, az > 0)
        self.down = ("az", 1, az < last_az)
        self.left = ("rg", -1, rg > 0)
        self.right = ("rg", 1, rg < last_rg)
        self.sides = (self.up, self.down, self.left, self.right)
        self.bufs, self.send_sems, self.recv_sems, self.count = bufs, send_sems, recv_sems, 0
        self.all = []
        self.loads = []
        for i, (tile, (buf, halo)) in enumerate(zip(tiles, bufs)):
            own = buf.at[pl.ds(halo, ROWS), pl.ds(LANE, COLS)]
            self.loads.append(pltpu.make_async_copy(tile, own, tile_sems.at[i]))

    def greet(self):
        for load in self.loads:
            load.start()
        barrier = pltpu.get_barrier_semaphore()
        for axis, step, there in self.sides:

            @pl.when(there)
            def _(axis=axis, step=step):
                peer = {axis: self.place[axis] + step}
                pl.semaphore_signal(barrier, inc=1, device_id=peer, device_id_type=MESH)

    def clear(self):
        up, down, left, right = self.sides
        for buf, halo in self.bufs:
            for side, rows, lanes in (
                (up, slice(0, halo), slice(None)),
                (down, slice(halo + ROWS, 2 * halo + ROWS), slice(None)),
                (left, slice(None), slice(0, LANE)),
                (right, slice(None), slice(LANE + COLS, 2 * LANE + COLS)),
            ):

                @pl.when(jnp.logical_not(side[2]))
                def _(buf=buf, rows=rows, lanes=lanes):
                    shape = [n if c == slice(None) else c.stop - c.start for n, c in zip(buf.shape, (rows, lanes))]
                    buf[rows, lanes] = jnp.zeros(shape, F32)

    def meet(self):
        barrier = pltpu.get_barrier_semaphore()
        peers = sum(there.astype(jnp.int32) for _, _, there in self.sides)
        pl.semaphore_wait(barrier, peers)

    def copy(self, buf, rows, lanes, to_rows, to_lanes, side, back, have=None):
        index = self.count
        self.count += 1
        axis, step, sends = side
        comes, name = back[2], None
        if have is not None:
            name = have[1]
            sends, comes = sends & have[2], comes & have[2]
        transfer = pltpu.make_async_remote_copy(
            src_ref=buf.at[pl.ds(*rows), pl.ds(*lanes)],
            dst_ref=buf.at[pl.ds(*to_rows), pl.ds(*to_lanes)],
            send_sem=self.send_sems.at[index],
            recv_sem=self.recv_sems.at[index],
            device_id={axis: self.place[axis] + step},
            device_id_type=MESH,
        )
        self.all.append((transfer, sends, comes, (axis, step, name), (axis, -step, name)))
        return self.all[-1]

    def along_azimuth(self, buf, halo, near, far, lanes):
        count = far - near
        end = halo + ROWS
        return [
            self.copy(buf, (halo + near, count), lanes, (end + near, count), lanes, self.up, self.down),
            self.copy(buf, (end - far, count), lanes, (halo - far, count), lanes, self.down, self.up),
        ]

    def along_range(self, buf, rows, have=None):
        return [
            self.copy(buf, rows, (LANE, LANE), rows, (LANE + COLS, LANE), self.left, self.right, have),
            self.copy(buf, rows, (COLS, LANE), rows, (0, LANE), self.right, self.left, have),
        ]

    def corners(self, buf, halo, near, far):
        count = far - near
        return self.along_range(buf, (halo - far, count), self.up) + self.along_range(
            buf, (halo + ROWS + near, count), self.down
        )

    @staticmethod
    def each(entries, act, coming, given=True):
        together = {}
        for entry in entries:
            together.setdefault(entry[4 if coming else 3], []).append(entry)
        for some in together.values():

            @pl.when(some[0][2 if coming else 1] & given)
            def _(some=some):
                for entry in some:
                    act(entry[0])

    def start(self, entries, given=True):
        self.each(entries, lambda transfer: transfer.start(), False, given)

    def arrive(self, entries, given=True):
        self.each(entries, lambda transfer: transfer.wait_recv(), True, given)

    def close(self):
        self.each(self.all, lambda transfer: transfer.wait_send(), False)


def kernel(off_az_hbm, off_rg_hbm, ref_tile, sec_tile, *refs):
    table_hbm, score_ref, tables = refs[:6], refs[6], refs[7:13]
    ref_row_ref, sec_row_ref, col_ref, back_row_ref, back_col_ref, box_col_ref = tables
    off_az, off_rg, ref_buf, sec_buf, row_mats, box_mid, box_far = refs[13:20]
    sec_high, sec_low, square_high, square_low = refs[20:24]
    quads, windows, strips, boxes, stats, tile_sems, table_sems, send_sems, recv_sems = refs[24:]
    halo = Exchange(
        (ref_tile, sec_tile),
        ((ref_buf, REF_HALO), (sec_buf, ROW_HALO)),
        tile_sems,
        send_sems,
        recv_sems,
    )
    everything = (LANE, COLS)
    near = halo.along_azimuth(sec_buf, ROW_HALO, 0, NEAR, everything)
    beside = halo.along_range(sec_buf, (ROW_HALO, ROWS)) + halo.along_range(ref_buf, (REF_HALO, ROWS))
    order = (1, 6, 2, 3, 4, 5)
    sec_far, ref_far = {}, {}
    for b in order:
        lanes = (LANE * b, LANE)
        sec_far[b] = halo.along_azimuth(sec_buf, ROW_HALO, NEAR, ROW_HALO, lanes)
        ref_far[b] = halo.along_azimuth(ref_buf, REF_HALO, 0, REF_HALO, lanes)
    near_corners = halo.corners(sec_buf, ROW_HALO, 0, NEAR)
    sec_corners = halo.corners(sec_buf, ROW_HALO, NEAR, ROW_HALO)
    ref_corners = halo.corners(ref_buf, REF_HALO, 0, REF_HALO)

    second = lax.rem(lax.axis_index("rg"), 2) == 1
    cores = ((jnp.logical_not(second), (1, 6)), (second, (6, 1)))
    corners = sec_corners + ref_corners

    def forward(step):
        for given, edges in cores:
            b = edges[step]
            halo.arrive(sec_far[b] + ref_far[b], given)
            halo.start(corners[0::2] if b == 1 else corners[1::2], given)

    halo.greet()
    fetches = [
        pltpu.make_async_copy(source, target, table_sems.at[i])
        for i, (source, target) in enumerate(
            zip((off_az_hbm, off_rg_hbm) + table_hbm, (off_az, off_rg) + tables)
        )
    ]
    for fetch in fetches:
        fetch.start()
    for load in halo.loads:
        load.wait()
    halo.meet()
    halo.start(beside)
    rest = [entry for b in order[2:] for entry in sec_far[b] + ref_far[b]]
    for given, (b, c) in cores:
        edges = sec_far[b] + ref_far[b] + sec_far[c] + ref_far[c]
        halo.start(near + edges + rest, given)

    halo.clear()
    own = pl.ds(LANE, COLS)
    ref_mean = jnp.mean(ref_buf[pl.ds(REF_HALO, ROWS), own], keepdims=True)
    sec_mean = jnp.mean(sec_buf[pl.ds(ROW_HALO, ROWS), own], keepdims=True)

    for fetch in fetches:
        fetch.wait()
    lane = lax.broadcasted_iota(jnp.int32, (128, LANE), 1)
    for k in range(2):
        first = NEAR + off_az[k]
        for m in range(2):
            turned = [
                pltpu.roll(sec_row_ref[k + m, :, i : i + LANE], first, axis=1)
                for i in range(0, 512, LANE)
            ]
            moved = [jnp.where(lane < first, turned[i - 1], turned[i]) for i in range(4)]
            row_mats[k, m] = jnp.concatenate(moved, axis=1)[:, : 3 * REACH].astype(BF16)
        lag = lax.broadcasted_iota(jnp.int32, (64, 2 * REACH), 0)
        cell = lax.broadcasted_iota(jnp.int32, (64, 2 * REACH), 1)
        cell = jnp.where(cell < REACH, cell, cell - REACH) + (64 - 64 * k) - first - lag
        box_mid[k] = ones_where((cell >= 0) & (cell < CHIP))
        lag = lax.broadcasted_iota(jnp.int32, (64, 2 * FAR), 0)
        cell = lax.broadcasted_iota(jnp.int32, (64, 2 * FAR), 1)
        cell = jnp.where(cell < FAR, cell, cell - FAR) + REACH * k - first - lag
        box_far[k] = ones_where((cell >= 0) & (cell < CHIP))

    def reference_lines(m, pairs):
        parts = [ref_buf[64 * m : 64 * m + 64, LANE * p : LANE * p + 256] for p in pairs]
        parts = [shifted(x, LANE - REF_HALO, LANE) - ref_mean for x in parts]
        for p, x in zip(pairs, parts):
            place = pl.ds(LANE * p, LANE)
            stats[2 * m : 2 * m + 1, place] = jnp.sum(x, axis=0, keepdims=True)
            stats[2 * m + 1 : 2 * m + 2, place] = jnp.sum(x * x, axis=0, keepdims=True)
        high, low = split(jnp.concatenate(parts, axis=1))
        return dot(ref_row_ref[m], jnp.concatenate([high, low, high], axis=0))

    def take_lines(k, spans, pairs):
        for p in pairs:
            place = slice(LANE * p, LANE * p + LANE)
            for first, count in spans:
                rows = slice(first, first + count)
                x = shifted(sec_buf[rows, LANE * p : LANE * p + 256], 64 + off_rg[k], LANE) - sec_mean
                sec_high[k, rows, place], sec_low[k, rows, place] = split(x)
                square_high[k, rows, place], square_low[k, rows, place] = split(x * x)

    def box_lines(k, first, count, p, box_ref):
        rows, place = slice(first, first + count), slice(LANE * p, LANE * p + LANE)
        stack = jnp.concatenate(
            [
                jnp.concatenate([sec_high[k, rows, place], square_high[k, rows, place]], axis=1),
                jnp.concatenate([sec_low[k, rows, place], square_low[k, rows, place]], axis=1),
            ],
            axis=0,
        )
        return dot(box_ref[k], stack)

    def window_transform(k, m, pairs):
        rows = slice(64 * (k + m), 64 * (k + m) + REACH)
        high = jnp.concatenate([sec_high[k, rows, LANE * p : LANE * p + LANE] for p in pairs], axis=1)
        low = jnp.concatenate([sec_low[k, rows, LANE * p : LANE * p + LANE] for p in pairs], axis=1)
        return dot(row_mats[k, m], jnp.concatenate([high, low, high], axis=0))

    def store(target, pairs, blocks):
        for i, p in enumerate(pairs):
            for half in range(2):
                target[2 * p + half] = blocks[2 * i + half]

    def middle_quadrants(*groups):
        rows_out = [reference_lines(1, pairs) for pairs in groups]
        for pairs, x in zip(groups, rows_out):
            store(quads.at[1], pairs, range_spectra([x], col_ref)[0])

    def middle_windows(*groups):
        rows_out = [[window_transform(k, 1 - k, pairs) for k in range(2)] for pairs in groups]
        for pairs in groups:
            for k in range(2):
                for p in pairs:
                    sums = box_lines(k, 64, REACH, p, box_mid)
                    boxes[k, :64, LANE * p : LANE * p + LANE] = sums[:, :128]
                    boxes[k, 64:, LANE * p : LANE * p + LANE] = sums[:, 128:]
        for pairs, x in zip(groups, rows_out):
            got = range_spectra(x, col_ref)
            store(windows.at[0, 1], pairs, got[0])
            store(windows.at[1, 0], pairs, got[1])

    def outer(for_windows, for_quadrants):
        for pairs in for_windows:
            take_lines(0, ((0, FAR),), pairs)
            take_lines(1, ((224, FAR),), pairs)
        rows_out = {}
        for pairs in for_windows:
            rows_out[pairs] = [(windows.at[k, k], window_transform(k, k, pairs)) for k in range(2)]
        for pairs in for_quadrants:
            found = [(quads.at[m], reference_lines(m, pairs)) for m in (0, 2)]
            rows_out[pairs] = rows_out.get(pairs, []) + found
        for pairs in for_windows:
            for k in range(2):
                for p in pairs:
                    sums = box_lines(k, 224 * k, FAR, p, box_far)
                    boxes[k, :64, LANE * p : LANE * p + LANE] += sums[:, :128]
                    boxes[k, 64:, LANE * p : LANE * p + LANE] += sums[:, 128:]
        for pairs, found in rows_out.items():
            got = range_spectra([x for _, x in found], col_ref)
            for (target, _), blocks in zip(found, got):
                store(target, pairs, blocks)

    def product(k, m, n):
        q = quads[k + m, n]
        x = windows[k, m, n] + windows[k, m, n + 1]
        qr, qi, xr, xi = q[:, :128], q[:, 128:], x[:, :128], x[:, 128:]
        return jnp.concatenate([qr * xr + qi * xi, qr * xi - qi * xr], axis=0)

    def middle_strips(*numbers):
        for n in numbers:
            for k in range(2):
                strips[k, n] = product(k, 1 - k, n)

    done = {}

    def strip(k, n):
        if (k, n) not in done:
            done[k, n] = True
            value = strips[k, n] + product(k, k, n)
            strips[k, n] = value
            return value
        return strips[k, n]

    def finish(*pairs):
        items = [(k, s) for s in pairs for k in range(2)]
        moments = {}
        for s in pairs:
            stat = stats[:, s * LANE : s * LANE + 256]
            place = lax.broadcasted_iota(jnp.int32, stat.shape, 1)
            a = jnp.sum(stat[:, :128], axis=1, keepdims=True)
            b = jnp.sum(jnp.where((place >= 64) & (place < 192), stat, 0.0), axis=1, keepdims=True)
            moments[s] = jnp.where(place[:, :128] < 64, a, b)
        sums = {(k, n): strip(k, n) for k, s in items for n in range(2 * s, 2 * s + 3)}
        inner = {}
        for k, s in items:
            left, middle_, right = [sums[k, 2 * s + i] for i in range(3)]
            high, low = split(jnp.concatenate([left + middle_, middle_ + right], axis=1))
            y = dot(back_row_ref[:, :256], jnp.concatenate([high, low], axis=0))
            inner[k, s] = y + dot(back_row_ref[:, 256:], high)
        corr = 0.0
        for i in range(2):
            lanes = slice(LANE * i, LANE * i + LANE)
            parts = [split(jnp.concatenate([inner[item][:64, lanes], inner[item][64:, lanes]], axis=1)) for item in items]
            wide = dot(jnp.concatenate([high for high, _ in parts], axis=0), back_col_ref[i])
            corr = corr + (wide[:, :128] + wide[:, 128:])
            corr = corr + dot(jnp.concatenate([low for _, low in parts], axis=0), back_col_ref[i, :, :128])
        parts = [split(boxes[k, :, s * LANE : s * LANE + 256]) for k, s in items]
        box = dot(jnp.concatenate([high for high, _ in parts], axis=0), box_col_ref[...])
        box = box + dot(jnp.concatenate([low for _, low in parts], axis=0), box_col_ref[...])
        for i, (k, s) in enumerate(items):
            first, second = box[128 * i : 128 * i + 64], box[128 * i + 64 : 128 * i + 128]
            both = moments[s]
            total = both[2 * k : 2 * k + 1] + both[2 * k + 2 : 2 * k + 3]
            power = both[2 * k + 1 : 2 * k + 2] + both[2 * k + 3 : 2 * k + 4]
            mean = total / AREA
            energy = power - total * mean
            centered = corr[64 * i : 64 * i + 64] - mean * first
            var_sum = jnp.maximum(second - first * first / AREA, 0.0)
            score_ref[k, s] = (CHIP / AREA) * centered * lax.rsqrt(
                (energy / AREA) * (var_sum / AREA) + EPSILON
            )

    inside = (1, 2, 3, 4, 5)
    near_lines = ((ROW_HALO - NEAR, NEAR), (ROW_HALO + ROWS, NEAR))
    middle_quadrants((1, 2), (3, 4), (5,))
    for k in range(2):
        take_lines(k, ((ROW_HALO, ROWS),), inside)
    halo.arrive(near)
    halo.start(near_corners)
    for k in range(2):
        take_lines(k, near_lines, inside)
    middle_windows((1, 2), (3, 4), (5,))
    forward(0)
    halo.arrive(beside)
    middle_quadrants((0, 6))
    middle_strips(*range(2, 11))
    forward(1)
    halo.arrive(near_corners)
    for k in range(2):
        take_lines(k, near_lines + ((ROW_HALO, ROWS),), (0, 6))
    middle_windows((0, 6))
    middle_strips(0, 1, 11, 12)
    halo.arrive(sec_far[2] + ref_far[2] + sec_far[3] + ref_far[3])
    outer([(1, 2)], [(1, 2)])
    halo.arrive(sec_far[4] + ref_far[4])
    outer([(3,)], [(3,)])
    halo.arrive(corners)
    halo.arrive(sec_far[5] + ref_far[5])
    outer([(4, 5), (0, 6)], [(4, 5), (0, 6)])
    finish(0, 1, 2, 3, 4, 5)
    halo.close()


def oversample(score_ref, out_ref, staged, sem):
    def cubic(out_index, sample):
        base = out_index // 2

        def pick(step):
            return jnp.where(jnp.clip(base + step, 0, LAGS - 1) == sample, 1.0, 0.0)

        odd = (9.0 * (pick(0) + pick(1)) - (pick(-1) + pick(2))) / 16.0
        return jnp.where(out_index % 2 == 1, odd, pick(0))

    row = lax.broadcasted_iota(jnp.int32, (128, 128), 0)
    lane = lax.broadcasted_iota(jnp.int32, (128, 128), 1)
    left = cubic(row, lane % LAGS).astype(BF16)
    right = cubic(lane, row % LAGS)
    right = jnp.concatenate(
        [jnp.where(row < LAGS, right, 0.0), jnp.where(row < LAGS, 0.0, right)], axis=1
    ).astype(BF16)
    right = jnp.concatenate([right, right], axis=0)
    items = [(k, s) for k in range(2) for s in range(PAIRS)]
    for first, last in ((0, 6), (6, 12)):
        lifted = []
        for i in range(first, last, 2):
            parts = [split(score_ref[k, s]) for k, s in items[i : i + 2]]
            high = jnp.concatenate([high for high, _ in parts], axis=1)
            low = jnp.concatenate([low for _, low in parts], axis=1)
            both = dot(left, jnp.concatenate([high, low], axis=0))
            lifted += [both[:, :LANE], both[:, LANE:]]
        for (k, s), value in zip(items[first:last], lifted):
            wide = dot(jnp.concatenate(split(value), axis=1), right)
            at = k * CHIPS + 2 * s
            staged[at] = wide[:, :128]
            staged[at + 1] = wide[:, 128:]
        part = pl.ds(2 * first, 2 * (last - first))
        pltpu.make_async_copy(staged.at[part], out_ref.at[part], sem).start()
    pltpu.make_async_copy(staged, out_ref, sem).wait()


def spread(table):
    room = np.zeros((128, REACH - 128))
    parts = [np.concatenate([table[:, i : i + 128].astype(np.float64), room], 1) for i in (0, 128, 256)]
    return np.concatenate(parts + [room], axis=1).astype(np.float32)


def body(ref_image, sec_image, off_az, off_rg):
    back_rows, back_cols = back_tables()
    tables = [
        np.stack([azimuth_table(64 * m, 64) for m in range(3)]),
        np.stack([spread(azimuth_table(64 * j, 128)) for j in range(3)]),
        column_tables(),
        back_rows,
        back_cols,
        box_table(),
    ]
    anywhere = pl.BlockSpec(memory_space=pl.ANY)
    vmem = pl.BlockSpec(memory_space=pltpu.VMEM)
    scores = pl.pallas_call(
        kernel,
        out_shape=pltpu.VMEM((2, PAIRS, LAGS, 2 * LAGS), F32),
        in_specs=[pl.BlockSpec(memory_space=pltpu.HBM)] * (4 + len(tables)),
        out_specs=vmem,
        scratch_shapes=[pltpu.VMEM(t.shape, t.dtype) for t in tables]
        + [
            pltpu.SMEM((2,), jnp.int32),
            pltpu.SMEM((2,), jnp.int32),
            pltpu.VMEM((ROWS + 2 * REF_HALO, COLS + 2 * LANE), F32),
            pltpu.VMEM((ROWS + 2 * ROW_HALO, COLS + 2 * LANE), F32),
            pltpu.VMEM((2, 2, 128, 3 * REACH), BF16),
            pltpu.VMEM((2, 64, 2 * REACH), BF16),
            pltpu.VMEM((2, 64, 2 * FAR), BF16),
        ]
        + [pltpu.VMEM((2, ROWS + 2 * ROW_HALO, WIDE), BF16)] * 4
        + [
            pltpu.VMEM((3, BLOCKS, 64, 256), F32),
            pltpu.VMEM((2, 2, BLOCKS, 64, 256), F32),
            pltpu.VMEM((2, BLOCKS - 1, 128, 128), F32),
            pltpu.VMEM((2, 128, WIDE), F32),
            pltpu.VMEM((8, WIDE), F32),
            pltpu.SemaphoreType.DMA((2,)),
            pltpu.SemaphoreType.DMA((8,)),
            pltpu.SemaphoreType.DMA((48,)),
            pltpu.SemaphoreType.DMA((48,)),
        ],
        compiler_params=pltpu.CompilerParams(
            collective_id=0, has_side_effects=True
        ),
    )(off_az, off_rg, ref_image, sec_image, *[jnp.asarray(t) for t in tables])
    out = pl.pallas_call(
        oversample,
        out_shape=jax.ShapeDtypeStruct((2 * CHIPS, 128, 128), F32),
        in_specs=[vmem],
        out_specs=anywhere,
        scratch_shapes=[pltpu.VMEM((2 * CHIPS, 128, 128), F32), pltpu.SemaphoreType.DMA],
        compiler_params=pltpu.CompilerParams(vmem_limit_bytes=8 << 20),
    )(scores)
    return out.reshape(2, CHIPS, 128, 128)


def solution(mesh):
    return jax.shard_map(
        body,
        mesh=mesh,
        in_specs=(P("az", "rg"), P("az", "rg"), P("az"), P("az")),
        out_specs=P("az", "rg", None, None),
        check_vma=False,
    )
```

```python
import functools

import jax
import jax.numpy as jnp
import numpy as np
from jax import lax
from jax.experimental import pallas as pl
from jax.experimental.pallas import tpu as pltpu
from jax.sharding import PartitionSpec as P

CHIP = 128
SPACE = 64
LAGS = 64
AREA = float(CHIP * CHIP)
EPSILON = 1e-06
ROWS = 128
COLS = 768
CHIPS = COLS // SPACE
PAIRS = CHIPS // 2
BLOCKS = CHIPS + 2
WIDE = BLOCKS * SPACE
ROW_HALO = 80
REF_HALO = 32
NEAR = 16
FAR = 64
REACH = 160
LANE = 128
MESH = pl.DeviceIdType.MESH
F32 = jnp.float32
BF16 = jnp.bfloat16


def halves(table):
    high = table.astype(jnp.bfloat16)
    low = (table - high.astype(np.float64)).astype(jnp.bfloat16)
    return high, low


def azimuth_table(first, count):
    angle = 2 * np.pi * (np.arange(64)[:, None] + 0.5) * (first + np.arange(count))[None, :] / 128
    high, low = halves(np.concatenate([np.cos(angle), -np.sin(angle)], axis=0))
    return np.concatenate([high, high, low], axis=1)


def box_table():
    cell = np.arange(256)[:, None]
    lag = np.arange(128)[None, :]
    return ((cell >= lag) & (cell < lag + 128)).astype(jnp.bfloat16)


def column_tables():
    angle = 2 * np.pi * np.arange(64)[:, None] * np.arange(128)[None, :] / 128
    c, s = np.cos(angle), np.sin(angle)
    sign = np.where(np.arange(256) % 2 == 0, 1.0, -1.0)[None, :]
    even = np.concatenate([np.concatenate([c, -s], 1), np.concatenate([s, c], 1)], 0)
    odd = np.concatenate([np.concatenate([s, c], 1), np.concatenate([c, -s], 1)], 0) * sign
    out = []
    for table in (even, odd):
        high, low = halves(table)
        out.append(np.concatenate([high, high, low], axis=0))
    return np.stack(out)


def back_tables():
    angle = 2 * np.pi * np.arange(64)[:, None] * (np.arange(64)[None, :] + 0.5) / 128
    c, s = np.cos(angle), np.sin(angle)
    high, low = halves(np.concatenate([np.concatenate([c, -s], 1), np.concatenate([s, c], 1)], 0))
    rows = np.concatenate([high, high, low], axis=1)
    angle = 2 * np.pi * np.arange(128)[:, None] * np.arange(64)[None, :] / 128
    high, low = halves(np.concatenate([np.cos(angle), -np.sin(angle)], 0) * (2.0 / AREA))
    none = np.zeros_like(high)
    first = np.concatenate([high, none, low, none], axis=1)
    second = np.concatenate([none, high, none, low], axis=1)
    return rows, np.stack([first, second])


def split(x):
    high = x.astype(BF16)
    return high, (x - high.astype(F32)).astype(BF16)


def dot(a, b):
    return jnp.dot(a, b, preferred_element_type=F32)


def shifted(x, shift, width):
    lane = lax.broadcasted_iota(jnp.int32, (x.shape[0], LANE), 1)
    turned = [
        pltpu.roll(x[:, i : i + LANE], LANE - shift, axis=1) for i in range(0, width + LANE, LANE)
    ]
    keep = lane < LANE - shift
    return jnp.concatenate(
        [jnp.where(keep, a, b) for a, b in zip(turned[:-1], turned[1:])], axis=1
    )


def range_spectra(rows_out, col_ref):
    lane = lax.broadcasted_iota(jnp.int32, (64, LANE), 1)
    low_half = lane < 64
    even, odd = [], []
    for x in rows_out:
        for i in range(0, x.shape[1], LANE):
            re = x[:64, i : i + LANE]
            im = pltpu.roll(x[64:, i : i + LANE], 64, axis=1)
            even.append(jnp.where(low_half, re, im))
            odd.append(jnp.where(low_half, im, re))
    out = []
    for parity, parts in enumerate((even, odd)):
        high, low = split(jnp.concatenate(parts, axis=0))
        got = dot(jnp.concatenate([high, low], axis=1), col_ref[parity, :256])
        got = got + dot(high, col_ref[parity, 256:])
        out.append(got)
    count = rows_out[0].shape[1] // LANE
    result = []
    for a in range(len(rows_out)):
        blocks = []
        for i in range(count):
            at = (a * count + i) * 64
            blocks += [out[0][at : at + 64], out[1][at : at + 64]]
        result.append(blocks)
    return result


def ones_where(condition):
    return jnp.where(condition, 1.0, 0.0).astype(BF16)


class Exchange:
    def __init__(self, tiles, bufs, tile_sems, send_sems, recv_sems):
        az, rg = lax.axis_index("az"), lax.axis_index("rg")
        last_az, last_rg = lax.axis_size("az") - 1, lax.axis_size("rg") - 1
        self.up = ("az", az - 1, az > 0)
        self.down = ("az", az + 1, az < last_az)
        self.left = ("rg", rg - 1, rg > 0)
        self.right = ("rg", rg + 1, rg < last_rg)
        self.sides = (self.up, self.down, self.left, self.right)
        self.bufs, self.send_sems, self.recv_sems, self.count = bufs, send_sems, recv_sems, 0
        self.all = []
        self.loads = []
        for i, (tile, (buf, halo)) in enumerate(zip(tiles, bufs)):
            own = buf.at[pl.ds(halo, ROWS), pl.ds(LANE, COLS)]
            self.loads.append(pltpu.make_async_copy(tile, own, tile_sems.at[i]))

    def greet(self):
        for load in self.loads:
            load.start()
        barrier = pltpu.get_barrier_semaphore()
        for axis, place, there in self.sides:

            @pl.when(there)
            def _(axis=axis, place=place):
                pl.semaphore_signal(barrier, inc=1, device_id={axis: place}, device_id_type=MESH)

    def clear(self):
        up, down, left, right = self.sides
        for buf, halo in self.bufs:
            for side, rows, lanes in (
                (up, slice(0, halo), slice(None)),
                (down, slice(halo + ROWS, 2 * halo + ROWS), slice(None)),
                (left, slice(None), slice(0, LANE)),
                (right, slice(None), slice(LANE + COLS, 2 * LANE + COLS)),
            ):

                @pl.when(jnp.logical_not(side[2]))
                def _(buf=buf, rows=rows, lanes=lanes):
                    shape = [n if c == slice(None) else c.stop - c.start for n, c in zip(buf.shape, (rows, lanes))]
                    buf[rows, lanes] = jnp.zeros(shape, F32)

    def meet(self):
        barrier = pltpu.get_barrier_semaphore()
        peers = sum(there.astype(jnp.int32) for _, _, there in self.sides)
        pl.semaphore_wait(barrier, peers)

    def copy(self, buf, rows, lanes, to_rows, to_lanes, side, back, have=None):
        index = self.count
        self.count += 1
        axis, place, sends = side
        comes = back[2]
        if have is not None:
            sends, comes = sends & have, comes & have
        transfer = pltpu.make_async_remote_copy(
            src_ref=buf.at[pl.ds(*rows), pl.ds(*lanes)],
            dst_ref=buf.at[pl.ds(*to_rows), pl.ds(*to_lanes)],
            send_sem=self.send_sems.at[index],
            recv_sem=self.recv_sems.at[index],
            device_id={axis: place},
            device_id_type=MESH,
        )
        entry = (transfer, sends, comes)
        self.all.append(entry)
        return entry

    def along_azimuth(self, buf, halo, near, far, lanes):
        count = far - near
        end = halo + ROWS
        return [
            self.copy(buf, (halo + near, count), lanes, (end + near, count), lanes, self.up, self.down),
            self.copy(buf, (end - far, count), lanes, (halo - far, count), lanes, self.down, self.up),
        ]

    def along_range(self, buf, rows, have=None):
        return [
            self.copy(buf, rows, (LANE, LANE), rows, (LANE + COLS, LANE), self.left, self.right, have),
            self.copy(buf, rows, (COLS, LANE), rows, (0, LANE), self.right, self.left, have),
        ]

    def corners(self, buf, halo, near, far):
        count = far - near
        return self.along_range(buf, (halo - far, count), self.up[2]) + self.along_range(
            buf, (halo + ROWS + near, count), self.down[2]
        )

    @staticmethod
    def start(entries, given=True):
        for transfer, sends, _ in entries:

            @pl.when(sends & given)
            def _(transfer=transfer):
                transfer.start()

    @staticmethod
    def arrive(entries, given=True):
        for transfer, _, comes in entries:

            @pl.when(comes & given)
            def _(transfer=transfer):
                transfer.wait_recv()

    def close(self):
        for transfer, sends, _ in self.all:

            @pl.when(sends)
            def _(transfer=transfer):
                transfer.wait_send()


def kernel(off_az_hbm, off_rg_hbm, ref_tile, sec_tile, *refs):
    table_hbm, score_ref, tables = refs[:6], refs[6], refs[7:13]
    ref_row_ref, sec_row_ref, col_ref, back_row_ref, back_col_ref, box_col_ref = tables
    off_az, off_rg, ref_buf, sec_buf, row_mats, box_mid, box_far = refs[13:20]
    sec_high, sec_low, square_high, square_low = refs[20:24]
    quads, windows, strips, boxes, stats, tile_sems, table_sems, send_sems, recv_sems = refs[24:]
    halo = Exchange(
        (ref_tile, sec_tile),
        ((ref_buf, REF_HALO), (sec_buf, ROW_HALO)),
        tile_sems,
        send_sems,
        recv_sems,
    )
    everything = (LANE, COLS)
    near = halo.along_azimuth(sec_buf, ROW_HALO, 0, NEAR, everything)
    beside = halo.along_range(sec_buf, (ROW_HALO, ROWS)) + halo.along_range(ref_buf, (REF_HALO, ROWS))
    order = (1, 6, 2, 3, 4, 5)
    sec_far, ref_far = {}, {}
    for b in order:
        lanes = (LANE * b, LANE)
        sec_far[b] = halo.along_azimuth(sec_buf, ROW_HALO, NEAR, ROW_HALO, lanes)
        ref_far[b] = halo.along_azimuth(ref_buf, REF_HALO, 0, REF_HALO, lanes)
    near_corners = halo.corners(sec_buf, ROW_HALO, 0, NEAR)
    sec_corners = halo.corners(sec_buf, ROW_HALO, NEAR, ROW_HALO)
    ref_corners = halo.corners(ref_buf, REF_HALO, 0, REF_HALO)

    corners = sec_corners + ref_corners

    def forward(step):
        for given, edges in cores:
            b = edges[step]
            halo.arrive(sec_far[b] + ref_far[b], given)
            halo.start(corners[0::2] if b == 1 else corners[1::2], given)

    halo.greet()
    fetches = [
        pltpu.make_async_copy(source, target, table_sems.at[i])
        for i, (source, target) in enumerate(
            zip((off_az_hbm, off_rg_hbm) + table_hbm, (off_az, off_rg) + tables)
        )
    ]
    for fetch in fetches:
        fetch.start()
    for load in halo.loads:
        load.wait()
    halo.meet()
    halo.start(near)
    halo.start(beside)
    second = lax.rem(lax.axis_index("rg"), 2) == 1
    cores = ((jnp.logical_not(second), (1, 6)), (second, (6, 1)))
    for given, edges in cores:
        for b in edges:
            halo.start(sec_far[b] + ref_far[b], given)
    for b in order[2:]:
        halo.start(sec_far[b] + ref_far[b])

    halo.clear()
    own = pl.ds(LANE, COLS)
    ref_mean = jnp.mean(ref_buf[pl.ds(REF_HALO, ROWS), own], keepdims=True)
    sec_mean = jnp.mean(sec_buf[pl.ds(ROW_HALO, ROWS), own], keepdims=True)

    for fetch in fetches:
        fetch.wait()
    lane = lax.broadcasted_iota(jnp.int32, (128, LANE), 1)
    for k in range(2):
        first = NEAR + off_az[k]
        for m in range(2):
            turned = [
                pltpu.roll(sec_row_ref[k + m, :, i : i + LANE], first, axis=1)
                for i in range(0, 512, LANE)
            ]
            moved = [jnp.where(lane < first, turned[i - 1], turned[i]) for i in range(4)]
            row_mats[k, m] = jnp.concatenate(moved, axis=1)[:, : 3 * REACH].astype(BF16)
        lag = lax.broadcasted_iota(jnp.int32, (64, 2 * REACH), 0)
        cell = lax.broadcasted_iota(jnp.int32, (64, 2 * REACH), 1)
        cell = jnp.where(cell < REACH, cell, cell - REACH) + (64 - 64 * k) - first - lag
        box_mid[k] = ones_where((cell >= 0) & (cell < CHIP))
        lag = lax.broadcasted_iota(jnp.int32, (64, 2 * FAR), 0)
        cell = lax.broadcasted_iota(jnp.int32, (64, 2 * FAR), 1)
        cell = jnp.where(cell < FAR, cell, cell - FAR) + REACH * k - first - lag
        box_far[k] = ones_where((cell >= 0) & (cell < CHIP))

    def reference_lines(m, pairs):
        parts = [ref_buf[64 * m : 64 * m + 64, LANE * p : LANE * p + 256] for p in pairs]
        parts = [shifted(x, LANE - REF_HALO, LANE) - ref_mean for x in parts]
        for p, x in zip(pairs, parts):
            place = pl.ds(LANE * p, LANE)
            stats[2 * m : 2 * m + 1, place] = jnp.sum(x, axis=0, keepdims=True)
            stats[2 * m + 1 : 2 * m + 2, place] = jnp.sum(x * x, axis=0, keepdims=True)
        high, low = split(jnp.concatenate(parts, axis=1))
        return dot(ref_row_ref[m], jnp.concatenate([high, low, high], axis=0))

    def take_lines(k, spans, pairs):
        for p in pairs:
            place = slice(LANE * p, LANE * p + LANE)
            for first, count in spans:
                rows = slice(first, first + count)
                x = shifted(sec_buf[rows, LANE * p : LANE * p + 256], 64 + off_rg[k], LANE) - sec_mean
                sec_high[k, rows, place], sec_low[k, rows, place] = split(x)
                square_high[k, rows, place], square_low[k, rows, place] = split(x * x)

    def box_lines(k, first, count, p, box_ref):
        rows, place = slice(first, first + count), slice(LANE * p, LANE * p + LANE)
        stack = jnp.concatenate(
            [
                jnp.concatenate([sec_high[k, rows, place], square_high[k, rows, place]], axis=1),
                jnp.concatenate([sec_low[k, rows, place], square_low[k, rows, place]], axis=1),
            ],
            axis=0,
        )
        return dot(box_ref[k], stack)

    def window_transform(k, m, pairs):
        rows = slice(64 * (k + m), 64 * (k + m) + REACH)
        high = jnp.concatenate([sec_high[k, rows, LANE * p : LANE * p + LANE] for p in pairs], axis=1)
        low = jnp.concatenate([sec_low[k, rows, LANE * p : LANE * p + LANE] for p in pairs], axis=1)
        return dot(row_mats[k, m], jnp.concatenate([high, low, high], axis=0))

    def store(target, pairs, blocks):
        for i, p in enumerate(pairs):
            for half in range(2):
                target[2 * p + half] = blocks[2 * i + half]

    def middle_quadrants(*groups):
        rows_out = [reference_lines(1, pairs) for pairs in groups]
        for pairs, x in zip(groups, rows_out):
            store(quads.at[1], pairs, range_spectra([x], col_ref)[0])

    def middle_windows(*groups):
        rows_out = [[window_transform(k, 1 - k, pairs) for k in range(2)] for pairs in groups]
        for pairs in groups:
            for k in range(2):
                for p in pairs:
                    sums = box_lines(k, 64, REACH, p, box_mid)
                    boxes[k, :64, LANE * p : LANE * p + LANE] = sums[:, :128]
                    boxes[k, 64:, LANE * p : LANE * p + LANE] = sums[:, 128:]
        for pairs, x in zip(groups, rows_out):
            got = range_spectra(x, col_ref)
            store(windows.at[0, 1], pairs, got[0])
            store(windows.at[1, 0], pairs, got[1])

    def outer(for_windows, for_quadrants):
        for pairs in for_windows:
            take_lines(0, ((0, FAR),), pairs)
            take_lines(1, ((224, FAR),), pairs)
        rows_out = {}
        for pairs in for_windows:
            rows_out[pairs] = [(windows.at[k, k], window_transform(k, k, pairs)) for k in range(2)]
        for pairs in for_quadrants:
            found = [(quads.at[m], reference_lines(m, pairs)) for m in (0, 2)]
            rows_out[pairs] = rows_out.get(pairs, []) + found
        for pairs in for_windows:
            for k in range(2):
                for p in pairs:
                    sums = box_lines(k, 224 * k, FAR, p, box_far)
                    boxes[k, :64, LANE * p : LANE * p + LANE] += sums[:, :128]
                    boxes[k, 64:, LANE * p : LANE * p + LANE] += sums[:, 128:]
        for pairs, found in rows_out.items():
            got = range_spectra([x for _, x in found], col_ref)
            for (target, _), blocks in zip(found, got):
                store(target, pairs, blocks)

    def product(k, m, n):
        q = quads[k + m, n]
        x = windows[k, m, n] + windows[k, m, n + 1]
        qr, qi, xr, xi = q[:, :128], q[:, 128:], x[:, :128], x[:, 128:]
        return jnp.concatenate([qr * xr + qi * xi, qr * xi - qi * xr], axis=0)

    def middle_strips(*numbers):
        for n in numbers:
            for k in range(2):
                strips[k, n] = product(k, 1 - k, n)

    done = {}

    def strip(k, n):
        if (k, n) not in done:
            done[k, n] = True
            value = strips[k, n] + product(k, k, n)
            strips[k, n] = value
            return value
        return strips[k, n]

    def finish(*pairs):
        items = [(k, s) for s in pairs for k in range(2)]
        moments = {}
        for s in pairs:
            stat = stats[:, s * LANE : s * LANE + 256]
            place = lax.broadcasted_iota(jnp.int32, stat.shape, 1)
            a = jnp.sum(stat[:, :128], axis=1, keepdims=True)
            b = jnp.sum(jnp.where((place >= 64) & (place < 192), stat, 0.0), axis=1, keepdims=True)
            moments[s] = jnp.where(place[:, :128] < 64, a, b)
        sums = {(k, n): strip(k, n) for k, s in items for n in range(2 * s, 2 * s + 3)}
        inner = {}
        for k, s in items:
            left, middle_, right = [sums[k, 2 * s + i] for i in range(3)]
            high, low = split(jnp.concatenate([left + middle_, middle_ + right], axis=1))
            y = dot(back_row_ref[:, :256], jnp.concatenate([high, low], axis=0))
            inner[k, s] = y + dot(back_row_ref[:, 256:], high)
        corr = 0.0
        for i in range(2):
            lanes = slice(LANE * i, LANE * i + LANE)
            parts = [split(jnp.concatenate([inner[item][:64, lanes], inner[item][64:, lanes]], axis=1)) for item in items]
            wide = dot(jnp.concatenate([high for high, _ in parts], axis=0), back_col_ref[i])
            corr = corr + (wide[:, :128] + wide[:, 128:])
            corr = corr + dot(jnp.concatenate([low for _, low in parts], axis=0), back_col_ref[i, :, :128])
        parts = [split(boxes[k, :, s * LANE : s * LANE + 256]) for k, s in items]
        box = dot(jnp.concatenate([high for high, _ in parts], axis=0), box_col_ref[...])
        box = box + dot(jnp.concatenate([low for _, low in parts], axis=0), box_col_ref[...])
        for i, (k, s) in enumerate(items):
            first, second = box[128 * i : 128 * i + 64], box[128 * i + 64 : 128 * i + 128]
            both = moments[s]
            total = both[2 * k : 2 * k + 1] + both[2 * k + 2 : 2 * k + 3]
            power = both[2 * k + 1 : 2 * k + 2] + both[2 * k + 3 : 2 * k + 4]
            mean = total / AREA
            energy = power - total * mean
            centered = corr[64 * i : 64 * i + 64] - mean * first
            var_sum = jnp.maximum(second - first * first / AREA, 0.0)
            score_ref[k, s] = (CHIP / AREA) * centered * lax.rsqrt(
                (energy / AREA) * (var_sum / AREA) + EPSILON
            )

    inside = (1, 2, 3, 4, 5)
    near_lines = ((ROW_HALO - NEAR, NEAR), (ROW_HALO + ROWS, NEAR))
    middle_quadrants((1, 2), (3, 4), (5,))
    for k in range(2):
        take_lines(k, ((ROW_HALO, ROWS),), inside)
    halo.arrive(near)
    halo.start(near_corners)
    for k in range(2):
        take_lines(k, near_lines, inside)
    middle_windows((1, 2), (3, 4), (5,))
    forward(0)
    halo.arrive(beside)
    middle_quadrants((0, 6))
    middle_strips(*range(2, 11))
    forward(1)
    halo.arrive(near_corners)
    for k in range(2):
        take_lines(k, near_lines + ((ROW_HALO, ROWS),), (0, 6))
    middle_windows((0, 6))
    middle_strips(0, 1, 11, 12)
    halo.arrive(sec_far[2] + ref_far[2] + sec_far[3] + ref_far[3])
    outer([(1, 2)], [(1, 2)])
    halo.arrive(sec_far[4] + ref_far[4])
    outer([(3,)], [(3,)])
    halo.arrive(corners)
    halo.arrive(sec_far[5] + ref_far[5])
    outer([(4, 5), (0, 6)], [(4, 5), (0, 6)])
    finish(0, 1, 2, 3, 4, 5)
    halo.close()


def oversample(score_ref, out_ref, staged, sem):
    def cubic(out_index, sample):
        base = out_index // 2

        def pick(step):
            return jnp.where(jnp.clip(base + step, 0, LAGS - 1) == sample, 1.0, 0.0)

        odd = (9.0 * (pick(0) + pick(1)) - (pick(-1) + pick(2))) / 16.0
        return jnp.where(out_index % 2 == 1, odd, pick(0))

    row = lax.broadcasted_iota(jnp.int32, (128, 128), 0)
    lane = lax.broadcasted_iota(jnp.int32, (128, 128), 1)
    left = cubic(row, lane % LAGS).astype(BF16)
    right = cubic(lane, row % LAGS)
    right = jnp.concatenate(
        [jnp.where(row < LAGS, right, 0.0), jnp.where(row < LAGS, 0.0, right)], axis=1
    ).astype(BF16)
    right = jnp.concatenate([right, right], axis=0)
    items = [(k, s) for k in range(2) for s in range(PAIRS)]
    for first, last in ((0, 4), (4, 12)):
        lifted = []
        for i in range(first, last, 2):
            parts = [split(score_ref[k, s]) for k, s in items[i : i + 2]]
            high = jnp.concatenate([high for high, _ in parts], axis=1)
            low = jnp.concatenate([low for _, low in parts], axis=1)
            both = dot(left, jnp.concatenate([high, low], axis=0))
            lifted += [both[:, :LANE], both[:, LANE:]]
        for (k, s), value in zip(items[first:last], lifted):
            wide = dot(jnp.concatenate(split(value), axis=1), right)
            at = k * CHIPS + 2 * s
            staged[at] = wide[:, :128]
            staged[at + 1] = wide[:, 128:]
        part = pl.ds(2 * first, 2 * (last - first))
        pltpu.make_async_copy(staged.at[part], out_ref.at[part], sem).start()
    pltpu.make_async_copy(staged, out_ref, sem).wait()


def spread(table):
    room = np.zeros((128, REACH - 128))
    parts = [np.concatenate([table[:, i : i + 128].astype(np.float64), room], 1) for i in (0, 128, 256)]
    return np.concatenate(parts + [room], axis=1).astype(np.float32)


def body(ref_image, sec_image, off_az, off_rg):
    back_rows, back_cols = back_tables()
    tables = [
        np.stack([azimuth_table(64 * m, 64) for m in range(3)]),
        np.stack([spread(azimuth_table(64 * j, 128)) for j in range(3)]),
        column_tables(),
        back_rows,
        back_cols,
        box_table(),
    ]
    anywhere = pl.BlockSpec(memory_space=pl.ANY)
    vmem = pl.BlockSpec(memory_space=pltpu.VMEM)
    scores = pl.pallas_call(
        kernel,
        out_shape=pltpu.VMEM((2, PAIRS, LAGS, 2 * LAGS), F32),
        in_specs=[pl.BlockSpec(memory_space=pltpu.HBM)] * (4 + len(tables)),
        out_specs=vmem,
        scratch_shapes=[pltpu.VMEM(t.shape, t.dtype) for t in tables]
        + [
            pltpu.SMEM((2,), jnp.int32),
            pltpu.SMEM((2,), jnp.int32),
            pltpu.VMEM((ROWS + 2 * REF_HALO, COLS + 2 * LANE), F32),
            pltpu.VMEM((ROWS + 2 * ROW_HALO, COLS + 2 * LANE), F32),
            pltpu.VMEM((2, 2, 128, 3 * REACH), BF16),
            pltpu.VMEM((2, 64, 2 * REACH), BF16),
            pltpu.VMEM((2, 64, 2 * FAR), BF16),
        ]
        + [pltpu.VMEM((2, ROWS + 2 * ROW_HALO, WIDE), BF16)] * 4
        + [
            pltpu.VMEM((3, BLOCKS, 64, 256), F32),
            pltpu.VMEM((2, 2, BLOCKS, 64, 256), F32),
            pltpu.VMEM((2, BLOCKS - 1, 128, 128), F32),
            pltpu.VMEM((2, 128, WIDE), F32),
            pltpu.VMEM((8, WIDE), F32),
            pltpu.SemaphoreType.DMA((2,)),
            pltpu.SemaphoreType.DMA((8,)),
            pltpu.SemaphoreType.DMA((48,)),
            pltpu.SemaphoreType.DMA((48,)),
        ],
        compiler_params=pltpu.CompilerParams(
            collective_id=0, has_side_effects=True
        ),
    )(off_az, off_rg, ref_image, sec_image, *[jnp.asarray(t) for t in tables])
    out = pl.pallas_call(
        oversample,
        out_shape=jax.ShapeDtypeStruct((2 * CHIPS, 128, 128), F32),
        in_specs=[vmem],
        out_specs=anywhere,
        scratch_shapes=[pltpu.VMEM((2 * CHIPS, 128, 128), F32), pltpu.SemaphoreType.DMA],
        compiler_params=pltpu.CompilerParams(vmem_limit_bytes=8 << 20),
    )(scores)
    return out.reshape(2, CHIPS, 128, 128)


def solution(mesh):
    return jax.shard_map(
        body,
        mesh=mesh,
        in_specs=(P("az", "rg"), P("az", "rg"), P("az"), P("az")),
        out_specs=P("az", "rg", None, None),
        check_vma=False,
    )
```
